32 devices in a mesh: leaf: 8 (over z, y), grid: 4 (over x, core).
Axes of the slice: x: 2, y: 2, z: 4, core: 2. Of those that a mesh axis runs over, the one named last changes fastest.
Arguments:
- source_leaf: float32 [8, 4096], P(None, ('leaf', 'grid')), may hold values from -6 to 6
- block_leaf: float32 [4096, 128], P(('leaf', 'grid')), may hold values from -0.5 to 0.5
- expand_leaf: float32 [4096, 128], P(('leaf', 'grid')), may hold values from -0.5 to 0.5
- basis_leaf: float32 [4096, 256], P(('leaf', 'grid')), may hold values from -0.25 to 0.25
- pivot_leaf: float32 [4096], P(('leaf', 'grid')), may hold values from -2 to 2
- couple_leaf: float32 [8192, 128], P(('leaf', 'grid')), may hold values from -0.5 to 0.5
- ranks_leaf: int32 [8, 2], replicated, may hold values from 32 to 128
- targets_leaf: int32 [8192], P(('leaf', 'grid')), may hold values from 0 to 2047, as said below
- source_middle: float32 [8, 4096], P(None, ('leaf', 'grid')), may hold values from -6 to 6
- block_middle: float32 [4096, 128], P(('leaf', 'grid')), may hold values from -0.5 to 0.5
- expand_middle: float32 [4096, 128], P(('leaf', 'grid')), may hold values from -0.5 to 0.5
- basis_middle: float32 [4096, 256], P(('leaf', 'grid')), may hold values from -0.1875 to 0.1875
- pivot_middle: float32 [4096], P(('leaf', 'grid')), may hold values from -2 to 2
- couple_middle: float32 [4096, 128], P(('leaf', 'grid')), may hold values from -0.5 to 0.5
- ranks_middle: int32 [4, 2], replicated, may hold values from 32 to 128
- targets_middle: int32 [4096], P(('leaf', 'grid')), may hold values from 0 to 4095, as said below
- source_upper: float32 [8, 4096], P(None, ('leaf', 'grid')), may hold values from -6 to 6
- block_upper: float32 [4096, 128], P(('leaf', 'grid')), may hold values from -0.5 to 0.5
- expand_upper: float32 [4096, 128], P(('leaf', 'grid')), may hold values from -0.5 to 0.5
- basis_upper: float32 [4096, 256], P(('leaf', 'grid')), may hold values from -0.125 to 0.125
- pivot_upper: float32 [4096], P(('leaf', 'grid')), may hold values from -2 to 2
- couple_upper: float32 [4096, 128], P(('leaf', 'grid')), may hold values from -0.5 to 0.5
- ranks_upper: int32 [2, 2], replicated, may hold values from 32 to 128
- targets_upper: int32 [4096], P(('leaf', 'grid')), may hold values from 0 to 4095, as said below
- source_root: float32 [8, 4096], P(None, ('leaf', 'grid')), may hold values from -6 to 6
- block_root: float32 [4096, 128], P(('leaf', 'grid')), may hold values from -0.5 to 0.5
- expand_root: float32 [4096, 128], P(('leaf', 'grid')), may hold values from -0.5 to 0.5
- basis_root: float32 [4096, 256], P(('leaf', 'grid')), may hold values from -0.09375 to 0.09375
- pivot_root: float32 [4096], P(('leaf', 'grid')), may hold values from -2 to 2
- ranks_root: int32 [1, 2], replicated, may hold values from 32 to 128
Outputs:
- answer_leaf: float32 [8, 4096], P(None, ('leaf', 'grid'))
- answer_middle: float32 [8, 4096], P(None, ('leaf', 'grid'))
- answer_upper: float32 [8, 4096], P(None, ('leaf', 'grid'))
- answer_root: float32 [8, 4096], P(None, ('leaf', 'grid'))
The draws below stay inside these ranges and needn't reach their ends.
Inputs may be any that keep to these rules, and one draw needn't show every extreme that they name: `targets_leaf`: within one leaf front the 1024 entries are distinct; each names a row of the parent front's row vector of 2048 rows. Split that vector's separator part and its update part each evenly, in order, over the parent's devices (leaf then grid); then the rows of one device name at most 32 rows held by any one of them, and exactly that many for some. `targets_middle`: within one middle front the entries are distinct; each names a row of the parent front's row vector of 4096 rows. Split likewise over the parent's devices, the rows of one device name at most 8 rows held by any one of them, and exactly that many for some. `targets_upper`: within one upper front the entries are distinct; each names a row of the root separator. Split evenly in order over all devices, the rows of one device name at most 4 rows held by any one of them, and exactly that many for some.
All inputs are finite; a program needn't handle non-finite values.
Results may differ from the reference program's by a relative error of at most 0.0003.
Values sent between devices are 32-bit elements; how exact they have to be, the bound alone decides.
A program may use at most 128 MiB of HBM per device.

```python
import jax
import jax.numpy as jnp
from jax import lax

RHS_COUNT = 8
BLOCK = 128
RANK = 128
TOP_ROWS = 128
SEP_LEAF = 512
UPD_LEAF = 1024
SEP_MID = 1024
SEP_UP = 2048
SEP_ROOT = 4096
N_LEAF = 8
N_GRID = 4


def pick_rows(key, salt, fronts, count, owners, width, pieces, sep_rows):
    base = jax.random.fold_in(key, salt)
    slots_each = pieces * width

    def one_front(front):
        fkey = jax.random.fold_in(base, front)
        order = jax.random.permutation(jax.random.fold_in(fkey, 1), owners)
        slot_keys = jax.vmap(lambda owner: jax.random.fold_in(jax.random.fold_in(fkey, 2), owner))(jnp.arange(owners, dtype=jnp.int32))
        slot_order = jax.vmap(lambda one: jax.random.permutation(one, slots_each))(slot_keys)
        rows = jnp.arange(count, dtype=jnp.int32)
        owner = order[rows % owners]
        slot = slot_order[owner, rows // owners]
        return slot // width * sep_rows + owner * width + slot % width
    picked = jax.vmap(one_front)(jnp.arange(fronts, dtype=jnp.int32))
    return picked.reshape(-1).astype(jnp.int32)


def draw_targets_leaf(key, part):
    return pick_rows(key, 11, N_LEAF, UPD_LEAF, N_LEAF * N_GRID // 4, TOP_ROWS, 2, SEP_MID)


def draw_targets_middle(key, part):
    return pick_rows(key, 12, 4, SEP_MID, N_LEAF * N_GRID // 2, TOP_ROWS, 2, SEP_UP)


def draw_targets_upper(key, part):
    return pick_rows(key, 13, 2, SEP_UP, N_LEAF * N_GRID, TOP_ROWS, 1, SEP_ROOT)


def set_ends(array, own_key, low, top_value):
    longest = array.shape.index(max(array.shape))
    spots = []
    for shift in (0, 1):
        where = [jax.random.randint(jax.random.fold_in(own_key, axis), (), 0, length) for axis, length in enumerate(array.shape)]
        where[longest] = (where[longest] + shift) % array.shape[longest]
        spots.append(tuple(where))
    return array.at[spots[0]].set(low).at[spots[1]].set(top_value)


def level_of(rng, dims, shards, least, high):
    def one(position, blocks):
        heights = jax.random.uniform(jax.random.fold_in(jax.random.fold_in(rng, 6), position), (blocks,), jnp.float32, least / len(shards), high / len(shards))
        return jnp.repeat(jnp.exp(heights), dims[position] // blocks).reshape((-1,) + (1,) * (len(dims) - position - 1))

    factor_of = one(*shards[0])
    for cut in shards[1:]:
        factor_of = factor_of * one(*cut)
    return factor_of


def centred(key, dims, scale, limit, shards=(), held_as=jnp.bfloat16):
    factor_of = level_of(key, dims, shards, -0.22, 0.18) if shards else 1.0
    values = jax.random.normal(key, dims, jnp.float32) * scale * factor_of
    return jnp.minimum(jnp.maximum(values, -limit), limit).astype(held_as)


def setup_inputs(seed: int = 0) -> dict:
    key_list = jax.random.split(jax.random.key(seed), 31)
    return {
        "source_leaf": centred(key_list[0], (RHS_COUNT, N_LEAF * SEP_LEAF), 1.0, 6.0, ((1, 32),), jnp.float32),
        "block_leaf": centred(key_list[1], (N_LEAF * SEP_LEAF, BLOCK), BLOCK ** -0.5, 0.5, ((0, 32),), jnp.float32),
        "expand_leaf": centred(key_list[2], (N_LEAF * SEP_LEAF, RANK), RANK ** -0.5, 0.5, ((0, 32),), jnp.float32),
        "basis_leaf": centred(key_list[3], (N_LEAF * SEP_LEAF, 2 * RANK), SEP_LEAF ** -0.5, 0.25, ((0, 32),), jnp.float32),
        "pivot_leaf": jnp.clip(jax.random.uniform(key_list[4], (N_LEAF * SEP_LEAF,), jnp.float32, -2.0, 2.0) * level_of(key_list[4], (N_LEAF * SEP_LEAF,), ((0, 32),), -0.4, 0.0), -2.0, 2.0),
        "couple_leaf": centred(key_list[5], (N_LEAF * UPD_LEAF, RANK), RANK ** -0.5, 0.5, ((0, 32),), jnp.float32),
        "ranks_leaf": set_ends(jax.random.randint(key_list[6], (N_LEAF, 2), RANK // 4, RANK + 1), jax.random.fold_in(key_list[6], 1), RANK // 4, RANK).astype(jnp.int32),
        "targets_leaf": draw_targets_leaf(jax.random.fold_in(key_list[30], 71), 0),
        "source_middle": centred(key_list[8], (RHS_COUNT, 4 * SEP_MID), 1.0, 6.0, ((1, 32),), jnp.float32),
        "block_middle": centred(key_list[9], (4 * SEP_MID, BLOCK), BLOCK ** -0.5, 0.5, ((0, 32),), jnp.float32),
        "expand_middle": centred(key_list[10], (4 * SEP_MID, RANK), RANK ** -0.5, 0.5, ((0, 32),), jnp.float32),
        "basis_middle": centred(key_list[11], (4 * SEP_MID, 2 * RANK), SEP_MID ** -0.5, 0.1875, ((0, 32),), jnp.float32),
        "pivot_middle": jnp.clip(jax.random.uniform(key_list[12], (4 * SEP_MID,), jnp.float32, -2.0, 2.0) * level_of(key_list[12], (4 * SEP_MID,), ((0, 32),), -0.4, 0.0), -2.0, 2.0),
        "couple_middle": centred(key_list[13], (4 * SEP_MID, RANK), RANK ** -0.5, 0.5, ((0, 32),), jnp.float32),
        "ranks_middle": set_ends(jax.random.randint(key_list[14], (4, 2), RANK // 4, RANK + 1), jax.random.fold_in(key_list[14], 1), RANK // 4, RANK).astype(jnp.int32),
        "targets_middle": draw_targets_middle(jax.random.fold_in(key_list[30], 71), 0),
        "source_upper": centred(key_list[16], (RHS_COUNT, 2 * SEP_UP), 1.0, 6.0, ((1, 32),), jnp.float32),
        "block_upper": centred(key_list[17], (2 * SEP_UP, BLOCK), BLOCK ** -0.5, 0.5, ((0, 32),), jnp.float32),
        "expand_upper": centred(key_list[18], (2 * SEP_UP, RANK), RANK ** -0.5, 0.5, ((0, 32),), jnp.float32),
        "basis_upper": centred(key_list[19], (2 * SEP_UP, 2 * RANK), SEP_UP ** -0.5, 0.125, ((0, 32),), jnp.float32),
        "pivot_upper": jnp.clip(jax.random.uniform(key_list[20], (2 * SEP_UP,), jnp.float32, -2.0, 2.0) * level_of(key_list[20], (2 * SEP_UP,), ((0, 32),), -0.4, 0.0), -2.0, 2.0),
        "couple_upper": centred(key_list[21], (2 * SEP_UP, RANK), RANK ** -0.5, 0.5, ((0, 32),), jnp.float32),
        "ranks_upper": set_ends(jax.random.randint(key_list[22], (2, 2), RANK // 4, RANK + 1), jax.random.fold_in(key_list[22], 1), RANK // 4, RANK).astype(jnp.int32),
        "targets_upper": draw_targets_upper(jax.random.fold_in(key_list[30], 71), 0),
        "source_root": centred(key_list[24], (RHS_COUNT, SEP_ROOT), 1.0, 6.0, ((1, 32),), jnp.float32),
        "block_root": centred(key_list[25], (SEP_ROOT, BLOCK), BLOCK ** -0.5, 0.5, ((0, 32),), jnp.float32),
        "expand_root": centred(key_list[26], (SEP_ROOT, RANK), RANK ** -0.5, 0.5, ((0, 32),), jnp.float32),
        "basis_root": centred(key_list[27], (SEP_ROOT, 2 * RANK), SEP_ROOT ** -0.5, 0.09375, ((0, 32),), jnp.float32),
        "pivot_root": jnp.clip(jax.random.uniform(key_list[28], (SEP_ROOT,), jnp.float32, -2.0, 2.0) * level_of(key_list[28], (SEP_ROOT,), ((0, 32),), -0.4, 0.0), -2.0, 2.0),
        "ranks_root": jax.random.randint(key_list[29], (1, 2), RANK // 4, RANK + 1).astype(jnp.int32),
    }


HIGH_PRECISION = lax.Precision.HIGHEST


def make_masks(ranks):
    cols = jnp.arange(RANK, dtype=jnp.int32)
    head_mask_grid = (cols[None, :] < ranks[:, 0:1]).astype(jnp.float32)[:, None, :]
    column_mask_grid = (cols[None, :] < ranks[:, 1:2]).astype(jnp.float32)[:, None, :]
    return head_mask_grid, column_mask_grid


def forward(source, inc_sep, block, expand, basis, pivot, ranks, fronts):
    width = source.shape[1] // fronts
    level_batch_index = source.reshape(RHS_COUNT, fronts, width).transpose(1, 0, 2)
    if inc_sep is not None:
        level_batch_index = level_batch_index + inc_sep
    tiles = block.reshape(fronts, width // BLOCK, BLOCK, BLOCK)
    local_portion = jnp.einsum("fanh,fnhk->fank", level_batch_index.reshape(fronts, RHS_COUNT, width // BLOCK, BLOCK), tiles, precision=HIGH_PRECISION).reshape(fronts, RHS_COUNT, width)
    gens = basis.reshape(fronts, width, 2 * RANK)
    query_lookup = gens[:, :, :RANK]
    coupling_right_factor = gens[:, :, RANK:]
    spread_across_rows = expand.reshape(fronts, width, RANK)
    head_mask_grid, column_mask_grid = make_masks(ranks)
    hidden_query_rows = jnp.einsum("mle,meq->mlq", level_batch_index, query_lookup, precision=HIGH_PRECISION) * head_mask_grid
    intermediate_entries = local_portion + jnp.einsum("gdk,gtk->gdt", hidden_query_rows, spread_across_rows, precision=HIGH_PRECISION)
    weight_entries = jnp.einsum("mle,meq->mlq", intermediate_entries, coupling_right_factor, precision=HIGH_PRECISION) * column_mask_grid
    correction_entries = intermediate_entries * pivot.reshape(fronts, 1, width)
    return correction_entries, weight_entries, (tiles, query_lookup, coupling_right_factor, spread_across_rows, head_mask_grid, column_mask_grid)


def flat_index(targets, fronts, parents, total):
    count = targets.shape[0] // fronts
    owner = jnp.arange(fronts, dtype=jnp.int32) // (fronts // parents)
    return (owner[:, None] * total + targets.reshape(fronts, count).astype(jnp.int32)).reshape(-1)


def scatter_up(update, targets, fronts, parents, sep_par, upd_par):
    total = sep_par + upd_par
    flat = flat_index(targets, fronts, parents, total)
    values = update.transpose(1, 0, 2).reshape(RHS_COUNT, -1)
    buffer = jnp.zeros((RHS_COUNT, parents * total), jnp.float32).at[:, flat].add(values)
    buffer = buffer.reshape(RHS_COUNT, parents, total).transpose(1, 0, 2)
    return buffer[:, :, :sep_par], buffer[:, :, sep_par:]


def pull_down(front_rows, targets, fronts, parents):
    total = front_rows.shape[2]
    flat = flat_index(targets, fronts, parents, total)
    whole = front_rows.transpose(1, 0, 2).reshape(RHS_COUNT, parents * total)
    values = jnp.take(whole, flat, axis=1)
    return values.reshape(RHS_COUNT, fronts, -1).transpose(1, 0, 2)


def backward(correction_entries, x_upd, couple, parts, fronts):
    tiles, query_lookup, coupling_right_factor, spread_across_rows, head_mask_grid, column_mask_grid = parts
    width = correction_entries.shape[2]
    remainder_rows = correction_entries
    if x_upd is not None:
        couple_u = couple.reshape(fronts, -1, RANK)
        solve_direction = jnp.einsum("fau,fur->far", x_upd, couple_u, precision=HIGH_PRECISION) * column_mask_grid
        remainder_rows = correction_entries - jnp.einsum("gdk,gtk->gdt", solve_direction, coupling_right_factor, precision=HIGH_PRECISION)
    right_projection = jnp.einsum("mle,meq->mlq", remainder_rows, spread_across_rows, precision=HIGH_PRECISION) * head_mask_grid
    local_portion = jnp.einsum("fanh,fnkh->fank", remainder_rows.reshape(fronts, RHS_COUNT, width // BLOCK, BLOCK), tiles, precision=HIGH_PRECISION).reshape(fronts, RHS_COUNT, width)
    return local_portion + jnp.einsum("gdk,gtk->gdt", right_projection, query_lookup, precision=HIGH_PRECISION)


def reference(source_leaf, block_leaf, expand_leaf, basis_leaf, pivot_leaf, couple_leaf, ranks_leaf, targets_leaf,
              source_middle, block_middle, expand_middle, basis_middle, pivot_middle, couple_middle, ranks_middle, targets_middle,
              source_upper, block_upper, expand_upper, basis_upper, pivot_upper, couple_upper, ranks_upper, targets_upper,
              source_root, block_root, expand_root, basis_root, pivot_root, ranks_root):
    levels = [
        (source_leaf, block_leaf, expand_leaf, basis_leaf, pivot_leaf, couple_leaf, ranks_leaf, targets_leaf),
        (source_middle, block_middle, expand_middle, basis_middle, pivot_middle, couple_middle, ranks_middle, targets_middle),
        (source_upper, block_upper, expand_upper, basis_upper, pivot_upper, couple_upper, ranks_upper, targets_upper),
        (source_root, block_root, expand_root, basis_root, pivot_root, None, ranks_root, None),
    ]
    fronts = [N_LEAF, 4, 2, 1]
    inc_sep = None
    inc_upd = None
    saved = []
    for level in range(4):
        source, block, expand, basis, pivot, couple, ranks, targets = levels[level]
        correction_entries, weight_entries, parts = forward(source, inc_sep, block, expand, basis, pivot, ranks, fronts[level])
        saved.append((correction_entries, parts))
        if level < 3:
            couple_u = couple.reshape(fronts[level], -1, RANK)
            update = -jnp.einsum("far,fur->fau", weight_entries, couple_u, precision=HIGH_PRECISION)
            if inc_upd is not None:
                update = update + inc_upd
            sep_par = levels[level + 1][0].shape[1] // fronts[level + 1]
            upd_par = 0
            if level + 1 < 3:
                upd_par = levels[level + 1][5].shape[0] // fronts[level + 1]
            inc_sep, inc_upd = scatter_up(update, targets, fronts[level], fronts[level + 1], sep_par, upd_par)
            if upd_par == 0:
                inc_upd = None
    answers = [None, None, None, None]
    rows_par = None
    for level in (3, 2, 1, 0):
        correction_entries, parts = saved[level]
        couple = levels[level][5]
        targets = levels[level][7]
        x_upd = None
        if level < 3:
            x_upd = pull_down(rows_par, targets, fronts[level], fronts[level + 1])
        xvals = backward(correction_entries, x_upd, couple, parts, fronts[level])
        answers[level] = xvals.transpose(1, 0, 2).reshape(RHS_COUNT, -1)
        rows_par = xvals if x_upd is None else jnp.concatenate([xvals, x_upd], axis=2)
    return (answers[0], answers[1], answers[2], answers[3])
```

```python
import functools

import jax
import jax.numpy as jnp
from jax import lax
from jax.experimental import pallas as pl
from jax.experimental.pallas import tpu as pltpu
from jax.sharding import PartitionSpec as P

RANK = 128
LANES = 128
MESH = pl.DeviceIdType.MESH
F32 = jnp.float32
BF16 = jnp.bfloat16


def once(a, b, ca, cb):
    return lax.dot_general(a, b, (((ca,), (cb,)), ((), ())), preferred_element_type=F32)


def halves(x):
    hi = x.astype(BF16)
    return hi, (x - hi.astype(F32)).astype(BF16)


def dot(a, b, ca, cb):
    ah, al = halves(a)
    bh, bl = halves(b)
    if ca == 0:
        return once(ah, bh, ca, cb) + (once(al, bh, ca, cb) + once(ah, bl, ca, cb))
    n = a.shape[0]
    both = once(jnp.concatenate([ah.astype(F32), al.astype(F32)], axis=0).astype(BF16), bh, ca, cb)
    return both[:n] + (both[n:] + once(ah, bl, ca, cb))


def pieces3(x):
    hi = x.astype(BF16)
    rest = x - hi.astype(F32)
    mid = rest.astype(BF16)
    return hi, mid, (rest - mid.astype(F32)).astype(BF16)


def mult(a, b):
    return dot(a, b, 1, 0)


def outer(a, b):
    return dot(a, b, 1, 1)


def inner(a, b):
    return dot(a, b, 0, 0)


def split3(x):
    hi = x.astype(BF16).astype(F32)
    rest = x - hi
    mid = rest.astype(BF16).astype(F32)
    return jnp.concatenate([hi, mid, rest - mid], axis=0).astype(BF16)


def select(x, onehot, cb):
    out = once(split3(x), onehot, 1, cb)
    n = x.shape[0]
    return out[:n] + out[n : 2 * n] + out[2 * n :]


KINDS = ("src", "blk", "exp", "bas", "piv", "rnk")


def kernel(cfg, names, *refs):
    leaves, across, size, ups, count, caps, fronts = cfg
    total_devices = leaves * across
    hbm = [refs[4 * i : 4 * i + 4] for i in range(6)]
    cpl_in = refs[24:27]
    tgt_in = refs[27:30]
    outs = refs[30:34]
    m = dict(zip(names, refs[34:-3]))
    send_sem, recv_sem, load_sem = refs[-3:]
    sems = {}
    src, blk, exp, bas, piv, rnk = [[m[k, i] for i in range(4)] for k in KINDS]
    cpl = [m["cpl", i] for i in range(3)]
    tgt = [m["tgt", i] for i in range(3)]

    me = lax.axis_index("leaf") * across + lax.axis_index("grid")
    plane = size[1]
    planes = total_devices // plane
    spot = me % plane
    layer = me // plane
    late = total_devices > 64
    pending = []

    loads = {}
    loaded = set()
    order = [("src", 0), ("bas", 0), ("blk", 0), ("exp", 0), ("cpl", 0), ("tgt", 0), ("piv", 0)]
    order += [("rnk", i) for i in range(4)]
    order += [(k, 1) for k in ("blk", "bas", "exp", "cpl", "tgt", "src", "piv")]
    order += [(k, 2) for k in ("blk", "bas", "exp", "cpl", "tgt", "src", "piv")]
    order += [(k, 3) for k in ("blk", "bas", "exp", "src", "piv")]
    where_from = {(k, i): hbm[j][i] for j, k in enumerate(KINDS) for i in range(4)}
    for i in range(3):
        where_from["cpl", i] = cpl_in[i]
        where_from["tgt", i] = tgt_in[i]

    def load(keys):
        for key in keys:
            loads[key] = pltpu.make_async_copy(
                where_from[key], m[key], load_sem.at[len(loads)]
            )
            loads[key].start()

    def need(*keys):
        for key in keys:
            if key not in loaded:
                loaded.add(key)
                loads[key].wait()

    def where(peer):
        return (peer // across, peer % across)

    def sem_of(name):
        return sems.setdefault(name, len(sems))

    def remote(a, b, sem, peer):
        return pltpu.make_async_remote_copy(
            src_ref=a,
            dst_ref=b,
            send_sem=send_sem.at[sem],
            recv_sem=recv_sem.at[sem],
            device_id=where(peer),
            device_id_type=MESH,
        )

    def wait_for(part, sem):
        pltpu.make_async_copy(part, part, sem).wait()

    def send_each(source, dest, group, name, stride=1):
        idx = me // stride % group
        base = me - idx * stride
        sem = sem_of(name)

        def body(k, carry):
            q = (idx + k) % group
            remote(source(q), dest(idx), sem, base + q * stride).start()
            return carry

        lax.fori_loop(1, group, body, 0)

    def send_all(name, group, stride=1):
        buf = m[name]
        idx = me // stride % group
        send_each(lambda q: buf.at[idx], lambda i: buf.at[i], group, name, stride)
        pending.append((buf.at[pl.ds(0, group - 1)], sem_of(name)))

    def arrive(name, group):
        wait_for(m[name].at[pl.ds(0, group - 1)], recv_sem.at[sem_of(name)])

    load(order[:7])
    barrier = pltpu.get_barrier_semaphore()

    def greet(k, carry):
        pl.semaphore_signal(
            barrier, inc=1, device_id=where((me + k) % total_devices), device_id_type=MESH
        )
        return carry

    lax.fori_loop(1, total_devices, greet, 0)
    load(order[7:])

    col = lax.broadcasted_iota(jnp.int32, (count, RANK), 1).astype(F32)
    mask_slots = {}

    def fill_mask(name, level, front, which):
        ranks = rnk[level][...].astype(F32)
        if ranks.shape[0] == 2 and fronts[level] > 2:
            lane = lax.broadcasted_iota(jnp.int32, ranks.shape, 1)
            row = lax.broadcasted_iota(jnp.int32, ranks.shape, 0)
            hit = (lane == front) & (row == which)
        else:
            lane = lax.broadcasted_iota(jnp.int32, ranks.shape, 1)
            row = lax.broadcasted_iota(jnp.int32, ranks.shape, 0)
            hit = (lane == which) & (row == front)
        r = jnp.sum(jnp.where(hit, ranks, 0.0), axis=1, keepdims=True)
        r = jnp.sum(r, axis=0, keepdims=True)
        slot = mask_slots.setdefault(name, len(mask_slots))
        m["mask"][slot] = (col < r).astype(F32)

    def mask(*name):
        return m["mask"][mask_slots[name]]

    def fill_masks(level):
        need(("rnk", level))
        fill_mask(("own", level, 0), level, me // size[level], 0)
        if level == 3:
            return
        fill_mask(("own", level, 1), level, me // size[level], 1)
        nch = size[level + 1] // size[level]
        for child in range(nch):
            front = me // size[level + 1] * nch + child
            fill_mask(("kid", level, child, 1), level, front, 1)
            if level > 0:
                fill_mask(("kid", level, child, 0), level, front, 0)

    def build_forward(level):
        need(("blk", level), ("bas", level), ("piv", level), ("exp", level))
        if level == 3:
            pt = exp[3][...].T * piv[3][...]
            m["cross_p", 3][...] = mult(pt, exp[3][...])
            last = outer(blk[3][...], pt)
        else:
            last = mult(blk[level][...], bas[level][:, RANK:])
        both = jnp.concatenate([blk[level][...], bas[level][:, :RANK], last], axis=1)
        hi, lo = halves(both)
        m["fwd", level, 0][...] = hi
        m["fwd", level, 1][...] = lo

    def local_forward(level, b):
        need(("src", level))
        bh, bl = halves(b)
        wh = m["fwd", level, 0][...]
        n = b.shape[0]
        two = once(jnp.concatenate([bh.astype(F32), bl.astype(F32)], axis=0).astype(BF16), wh, 1, 0)
        out = two[:n] + (two[n:] + once(bh, m["fwd", level, 1][...], 1, 0))
        return out[:, :RANK], out[:, RANK : 2 * RANK], out[:, 2 * RANK :]

    def group_of(level):
        return size[level] if level < 3 else plane

    parts_of = [min(group_of(level), 16) for level in range(4)]

    def scatter_cross(level):
        g = group_of(level)
        p = parts_of[level]
        rp = RANK // p
        idx = me % g
        base = me - idx
        sem = sem_of(("rs", level))
        cross_p, rs_buf = m["cross_p", level], m["rs", level]

        def body(k, carry):
            q = (idx + k) % p

            def go():
                rows = pl.ds(pl.multiple_of(q * rp, 8), rp)
                remote(cross_p.at[rows], rs_buf.at[idx], sem, base + q).start()

            if g == p:
                go()
            else:
                pl.when(q != idx)(go)
            return carry

        lax.fori_loop(1 if g == p else 0, p, body, 0)

        def keep():
            rows = pl.ds(pl.multiple_of(idx * rp, 8), rp)
            rs_buf[idx] = cross_p[rows, :]

        if g == p:
            keep()
        else:
            pl.when(idx < p)(keep)

    def spread_of(level):
        return (size[0], size[2], size[3], plane)[level]

    def holds_part(level, go):
        if group_of(level) == parts_of[level]:
            go()
        else:
            pl.when(me % group_of(level) < parts_of[level])(go)

    def sum_parts(level):
        g = group_of(level)
        wait_for(m["rs", level].at[pl.ds(0, g - 1)], recv_sem.at[sem_of(("rs", level))])
        return jnp.sum(m["rs", level][...], axis=0)

    def cross_planes():
        buf = m["gram"]

        def go():
            buf[layer] = sum_parts(3)
            send_each(lambda q: buf.at[layer], lambda i: buf.at[i], planes, "gram", plane)

        holds_part(3, go)

    def gather_cross(level):
        g = group_of(level)
        gp = spread_of(level)
        p = parts_of[level]
        idx = me % g
        place = me % gp
        sem = sem_of(("cross", level))
        slot = place // g * p + idx
        buf = m["cross", level]

        def go():
            if level == 3:
                arrive("gram", planes)
                buf[slot] = jnp.sum(m["gram"][...], axis=0)
            else:
                buf[slot] = sum_parts(level)

            def body(k, carry):
                peer = me - place + (place + k) % gp
                remote(buf.at[slot], buf.at[slot], sem, peer).start()
                return carry

            lax.fori_loop(1, gp, body, 0)

        holds_part(level, go)

    def rows_path(level):
        return caps[level] > 4

    def wide_of(level):
        return max(8, -(-caps[level] // 8) * 8)

    def ship_couple(level):
        need(("tgt", level), ("cpl", level))
        g = size[level]
        gp = size[level + 1]
        u = ups[level]
        wide = wide_of(level)
        sep = gp * LANES
        t = tgt[level][...]
        upd = t >= sep
        rel = jnp.where(upd, t - sep, t)
        dst = rel // LANES
        low = rel % LANES + jnp.where(upd, LANES, 0)
        ri = lax.broadcasted_iota(jnp.int32, (u, u), 0)
        ci = lax.broadcasted_iota(jnp.int32, (u, u), 1)
        dst_f = dst.astype(F32)
        dst_c = jnp.sum(jnp.where(ri == ci, jnp.broadcast_to(dst_f, (u, u)), 0.0), axis=1, keepdims=True)
        same = dst_c == dst_f
        rank = jnp.sum(jnp.where(same & (ri < ci), 1.0, 0.0), axis=0, keepdims=True).astype(jnp.int32)
        pos = dst * wide + rank
        slots = gp * wide
        si = lax.broadcasted_iota(jnp.int32, (slots, u), 0)
        hit = (si == pos).astype(F32)
        hit16 = hit.astype(BF16)
        hi, mid, lo = [once(hit16, piece, 1, 0) for piece in pieces3(cpl[level][...])]
        moved = hi + mid + lo
        perm_buf, recv_c = m["perm", level], m["couple", level]
        idx = me % gp
        if rows_path(level):
            rank_c = jnp.sum(jnp.where(same & (ci < ri), 1.0, 0.0), axis=1, keepdims=True)
            first = (me % g * wide).astype(F32)
            lane = lax.broadcasted_iota(jnp.int32, (u, LANES), 1).astype(F32)
            place = (lane == rank_c + first).astype(F32).astype(BF16)
            qi = lax.broadcasted_iota(jnp.int32, (gp, u), 0)
            named = jnp.where(qi == dst, low.astype(F32), 0.0).astype(BF16)
            lows = once(named, place, 1, 0)
            lows_s, lows_r = m["low_s", level], m["low", level]
            for q in range(gp):
                lows_s[q] = lows[q : q + 1, :]
            lows_r[idx] = lows_s[idx]
            perm_buf[...] = moved.reshape(gp, wide, LANES)
        else:
            shifted = (si == pos + 4).astype(F32)
            lowc = jnp.sum(shifted * low.astype(F32), axis=1, keepdims=True)
            both = moved + jnp.broadcast_to(lowc, (slots, LANES))
            perm_buf[...] = both.reshape(gp, wide, LANES)
        recv_c[idx] = perm_buf[idx]
        if rows_path(level):
            send_each(lambda q: lows_s.at[q], lambda i: lows_r.at[i], gp, ("low", level))
            pending.append((lows_s.at[pl.ds(0, gp - 1)], sem_of(("low", level))))
        send_each(lambda q: perm_buf.at[q], lambda i: recv_c.at[i], gp, ("couple", level))
        pending.append((perm_buf.at[pl.ds(0, gp - 1)], sem_of(("couple", level))))

    def build_gt(level):
        g = size[level]
        gp = size[level + 1]
        wide = wide_of(level)
        nch = gp // g
        gt = m["gt", level]
        rows = gt.shape[1]
        if rows_path(level):
            arrive(("low", level), gp)
        arrive(("couple", level), gp)
        slots = g * wide
        for child in range(nch):
            got = m["couple", level][child * g : (child + 1) * g]
            got = got.reshape(slots, LANES)
            if rows_path(level):
                low = jnp.sum(m["low", level][child * g : (child + 1) * g], axis=0)[:, :slots]
                ri = lax.broadcasted_iota(jnp.int32, (rows, slots), 0).astype(F32)
                ot = (ri == low).astype(F32).astype(BF16)
                hi, mid, lo = [once(piece, ot, 0, 1) for piece in pieces3(got)]
            else:
                lane = lax.broadcasted_iota(jnp.int32, (slots, rows), 1).astype(F32)
                up = jnp.concatenate([got[4:, :1], got[:4, :1]], axis=0)
                si = lax.broadcasted_iota(jnp.int32, (slots, 1), 0)
                low = jnp.where(si % 8 < 4, up, -1.0)
                ot = (lane == low).astype(F32).astype(BF16)
                hi, mid, lo = [once(piece, ot, 0, 0) for piece in pieces3(got)]
            gt[child * RANK : (child + 1) * RANK, :] = hi + mid + lo

    def arrive_cross(level):
        g = group_of(level)
        p = parts_of[level]
        n = spread_of(level) // g * p
        sem = recv_sem.at[sem_of(("cross", level))]
        buf = m["cross", level]
        if g == p:
            wait_for(buf.at[pl.ds(0, n - 1)], sem)
        else:
            idx = me % g
            pl.when(idx < p)(lambda: wait_for(buf.at[pl.ds(0, n - 1)], sem))
            pl.when(idx >= p)(lambda: wait_for(buf.at[pl.ds(0, n)], sem))

    def cross_of(level, child):
        p = parts_of[level]
        return m["cross", level][pl.ds(child * p, p)].reshape(RANK, RANK)

    def build_bot_middle():
        gp = size[2]
        place = me % gp
        rows = 2 * LANES
        ri = lax.broadcasted_iota(jnp.int32, (rows, LANES), 0)
        arrive("tgt_middle", gp)
        mine = jnp.where(ri < LANES, place * LANES + ri, (gp + place - 1) * LANES + ri).astype(F32)

        def fill(j, carry):
            t = m["tgt_middle"][j]
            lanes = pl.ds(pl.multiple_of(j * LANES, LANES), LANES)
            m["bot_middle"][:, lanes] = (mine == t).astype(F32).astype(BF16)
            return carry

        lax.fori_loop(0, gp, fill, 0)

    def build_bot_upper():
        rows = planes * LANES
        ri = lax.broadcasted_iota(jnp.int32, (rows, LANES), 0)
        arrive("tgt_upper", plane)
        mine = ((ri // LANES * plane + spot) * LANES + ri % LANES).astype(F32)

        def fill(j, carry):
            t = m["tgt_upper"][j]
            lanes = pl.ds(pl.multiple_of(j * LANES, LANES), LANES)
            m["bot_upper"][:, lanes] = (mine == t).astype(F32).astype(BF16)
            return carry

        lax.fori_loop(0, plane, fill, 0)

    def build_ft_middle():
        t = tgt[1][...]
        ri = lax.broadcasted_iota(jnp.int32, (LANES, LANES), 0)

        def fill(j, carry):
            rows = pl.ds(pl.multiple_of(j * LANES, LANES), LANES)
            m["ft_middle"][rows, :] = (ri + j * LANES == t).astype(F32).astype(BF16)
            return carry

        lax.fori_loop(0, m["ft_middle"].shape[0] // LANES, fill, 0)

    def build_ft_upper():
        arrive("tgt_layer", planes)
        t = jnp.concatenate([m["tgt_layer"][j] for j in range(planes)], axis=1)
        ri = lax.broadcasted_iota(jnp.int32, (LANES, planes * LANES), 0)

        def fill(j, carry):
            rows = pl.ds(pl.multiple_of(j * LANES, LANES), LANES)
            here = ((ri + (layer * plane + j) * LANES).astype(F32) == t).astype(F32)
            m["ft_upper"][rows, :] = here.astype(BF16)
            return carry

        lax.fori_loop(0, plane, fill, 0)

    def share(level, zp):
        m["zp", level][me % size[level]] = zp
        send_all(("zp", level), size[level])

    def shared(level):
        arrive(("zp", level), size[level])
        return jnp.sum(m["zp", level][...], axis=0)

    def start_cross(level):
        need(("exp", level), ("bas", level))
        m["cross_p", level][...] = inner(exp[level][...], bas[level][:, RANK:])
        scatter_cross(level)

    need(("src", 0), ("bas", 0))
    m["f0"][me % size[0]] = mult(src[0][...], bas[0][:, :RANK])
    pl.semaphore_wait(barrier, total_devices - 1)
    send_all("f0", size[0])
    need(("blk", 0), ("exp", 0), ("piv", 0))
    ship_couple(0)
    local = mult(src[0][...], blk[0][...])
    fill_masks(0)
    arrive("f0", size[0])
    hq = jnp.sum(m["f0"][...], axis=0) * mask("own", 0, 0)
    y = local + outer(hq, exp[0][...])
    m["f1"][spot] = mult(y, bas[0][:, RANK:])
    send_all("f1", plane)
    need(("tgt", 1), ("tgt", 2))
    m["tgt_middle"][me % size[2]] = tgt[1][...].astype(F32)
    send_all("tgt_middle", size[2])
    mine_t = tgt[2][...].astype(F32)
    m["tgt_upper"][spot] = mine_t
    send_all("tgt_upper", plane)
    m["tgt_layer"][layer] = mine_t
    send_all("tgt_layer", planes, plane)
    saved = [y * piv[0][...]]
    start_cross(1)
    ship_couple(1)
    build_forward(1)
    fill_masks(1)
    build_gt(0)
    start_cross(2)

    inc_upd = None
    for level in range(3):
        g = size[level]
        gp = size[level + 1]
        nch = gp // g
        place = me % gp
        parent = me // gp
        child_me = place // g
        if level > 0:
            arrive_cross(level)
        if level < 2:
            name = ("f1", "f2")[level]
            buf, step = m[name], g
            arrive(name, gp)
        else:
            buf, step = m["f3b"], g // plane
            arrive("f3b", planes)
        ws = []
        for child in range(nch):
            if level == 0:
                tot = jnp.sum(buf[child * step : (child + 1) * step], axis=0)
                ws.append(tot * mask("kid", 0, child, 1))
            else:
                tot = jnp.sum(buf[child * step : (child + 1) * step, : 2 * count, :], axis=0)
                hq = tot[:count] * mask("kid", level, child, 0)
                cross = cross_of(level, child)
                ws.append((tot[count:] + mult(hq, cross)) * mask("kid", level, child, 1))
        inc = -mult(jnp.concatenate(ws, axis=1), m["gt", level][...])
        if level == 1:
            rows = jnp.concatenate([buf[j, 2 * count : 3 * count, :] for j in range(gp)], axis=1)
            inc = inc + select(rows, m["bot_middle"][...], 1)
        if level == 2:
            inc = inc + jnp.sum(buf[:, 2 * count : 3 * count, :], axis=0)
        need(("src", level + 1))
        bn = src[level + 1][...] + inc[:, :LANES]
        local_n, bq_n, lv_n = local_forward(level + 1, bn)
        if level == 0:
            m["f2"][me % size[2]] = jnp.concatenate([bq_n, lv_n, inc[:, LANES:]], axis=0)
            send_all("f2", size[2])
        elif level == 1:
            m["f3a"][spot] = jnp.concatenate([bq_n, lv_n, inc[:, LANES:]], axis=0)
            send_all("f3a", plane)
        else:
            m["f4", "a"][spot] = jnp.concatenate([bq_n, lv_n], axis=0)
            send_all(("f4", "a"), plane)
        if level > 0:
            own = jnp.sum(buf[pl.ds(child_me * step, step), :count, :], axis=0)
            hq = own * mask("own", level, 0)
            saved.append((local + outer(hq, exp[level][...])) * piv[level][...])
            share(level, mult(saved[level], exp[level][...]))
        if level == 0:
            gather_cross(1)
            ship_couple(2)
            build_forward(2)
            fill_masks(2)
            build_gt(1)
            build_bot_middle()
            gather_cross(2)
            build_forward(3)
            scatter_cross(3)
        elif level == 1:
            build_bot_upper()
            fill_masks(3)
            arrive("f3a", plane)
            sums = jnp.sum(m["f3a"][:, : 2 * count, :], axis=0)
            rows = jnp.concatenate([m["f3a"][j, 2 * count :, :] for j in range(plane)], axis=1)
            part = select(rows, m["bot_upper"][...], 1)
            for q in range(planes):
                m["f3s"][q] = jnp.concatenate([sums, part[:, q * LANES : (q + 1) * LANES]], axis=0)
            m["f3b"][layer] = m["f3s"][layer]
            send_each(lambda q: m["f3s"].at[q], lambda i: m["f3b"].at[i], planes, "f3b", plane)
            pending.append((m["f3s"].at[pl.ds(0, planes - 1)], sem_of("f3b")))
            cross_planes()
            build_gt(2)
            share(0, mult(saved[0], exp[0][...]))
            start_cross(0)
        else:
            gather_cross(3)
            gather_cross(0)
            arrive(("f4", "a"), plane)
            m["f4", "b"][layer] = jnp.sum(m["f4", "a"][...], axis=0)
            send_all(("f4", "b"), planes, plane)
        local = local_n

    build_ft_upper()
    if not late:
        build_ft_middle()
    arrive_cross(3)
    arrive_cross(0)
    arrive(("f4", "b"), planes)
    both = jnp.sum(m["f4", "b"][...], axis=0)
    hq = both[:count] * mask("own", 3, 0)
    z = (local + outer(hq, exp[3][...])) * piv[3][...]
    rp_total = (both[count:] + mult(hq, cross_of(3, 0))) * mask("own", 3, 0)
    x = outer(z, blk[3][...]) + outer(rp_total, bas[3][:, :RANK])

    xu = None
    for level in (2, 1, 0):
        g = size[level]
        gp = size[level + 1]
        nch = gp // g
        place = me % gp
        child_me = place // g
        full = x if xu is None else jnp.concatenate([x, xu], axis=1)
        sp = outer(full, m["gt", level][...])
        pieces = [sp[:, c * RANK : (c + 1) * RANK] for c in range(nch)]
        if level == 2:
            m["b1a"][spot] = jnp.concatenate(pieces + [x], axis=0)
            send_all("b1a", plane)
            outs[3][...] = x
            arrive("b1a", plane)
            o = nch * count
            sums = jnp.sum(m["b1a"][:, :o, :], axis=0)
            rows = jnp.concatenate([m["b1a"][j, o:, :] for j in range(plane)], axis=1)
            part = select(rows, m["ft_upper"][...], 0)
            for q in range(planes):
                c = q * plane // g
                m["b1s"][q] = jnp.concatenate(
                    [sums[c * count : (c + 1) * count], part[:, q * LANES : (q + 1) * LANES]], axis=0
                )
            m["b1b"][layer] = m["b1s"][layer]
            send_each(lambda q: m["b1s"].at[q], lambda i: m["b1b"].at[i], planes, "b1b", plane)
            pending.append((m["b1s"].at[pl.ds(0, planes - 1)], sem_of("b1b")))
            arrive("b1b", planes)
            both = jnp.sum(m["b1b"][...], axis=0)
            s, xu = both[:count], both[count:]
        else:
            name = ("b3", "b2")[level]
            buf, piece = m[name], m["piece", level]
            for c in range(nch):
                piece[c] = pieces[c]
            head = pl.ds(0, count)
            rest = pl.ds(count, 2 * count)
            buf[place, head] = piece[child_me]
            if level == 1:
                buf[place, rest] = jnp.concatenate([x, xu], axis=0)

                def ship(k, carry, gp=gp, g=g, place=place, buf=buf, piece=piece, name=name):
                    q = (place + k) % gp
                    peer = me - place + q
                    sem = sem_of(name)
                    remote(piece.at[q // g], buf.at[place, head], sem, peer).start()
                    remote(buf.at[place, rest], buf.at[place, rest], sem, peer).start()
                    return carry

                lax.fori_loop(1, gp, ship, 0)
            else:
                send_each(lambda q: piece.at[q // g], lambda i: buf.at[i], gp, name)
            pending.append((buf.at[pl.ds(0, gp - 1)], sem_of(name)))
            outs[level + 1][...] = x
            arrive(name, gp)
            s = jnp.sum(buf[:, head, :], axis=0)
            if level == 1:
                blocks = [buf[j, count : 2 * count, :] for j in range(gp)]
                blocks += [buf[j, 2 * count :, :] for j in range(gp)]
                if late:
                    build_ft_middle()
                xu = select(jnp.concatenate(blocks, axis=1), m["ft_middle"][...], 0)
        s = s * mask("own", level, 1)
        r = saved[level] - outer(s, bas[level][:, RANK:])
        mine = child_me if level > 0 else 0
        proj = (shared(level) - outer(s, cross_of(level, mine))) * mask("own", level, 0)
        x = outer(r, blk[level][...]) + outer(proj, bas[level][:, :RANK])
    outs[0][...] = x

    for part, sem in pending:
        wait_for(part, send_sem.at[sem])
    for level in range(4):
        g = group_of(level)
        p = parts_of[level]
        rp = RANK // p
        gp = spread_of(level)
        n = gp // g * p
        idx = me % g
        rs_sem = send_sem.at[sem_of(("rs", level))]
        ag_sem = send_sem.at[sem_of(("cross", level))]
        cross_p, buf = m["cross_p", level], m["cross", level]

        def ag_done():
            for _ in range((gp - 1) // n):
                wait_for(buf.at[pl.ds(0, n)], ag_sem)
            if (gp - 1) % n:
                wait_for(buf.at[pl.ds(0, (gp - 1) % n)], ag_sem)
            if level == 3:
                wait_for(m["gram"].at[pl.ds(0, planes - 1)], send_sem.at[sem_of("gram")])

        if g == p:
            wait_for(cross_p.at[pl.ds(0, (p - 1) * rp)], rs_sem)
            ag_done()
        else:
            pl.when(idx < p)(lambda: wait_for(cross_p.at[pl.ds(0, (p - 1) * rp)], rs_sem))
            pl.when(idx >= p)(lambda: wait_for(cross_p, rs_sem))
            pl.when(idx < p)(ag_done)


def put_out(*refs):
    n = len(refs) // 2
    ins, outs, sem = refs[:n], refs[n : 2 * n], refs[-1]
    copies = [pltpu.make_async_copy(ins[i], outs[i], sem.at[i]) for i in range(n)]
    for c in copies:
        c.start()
    for c in copies:
        c.wait()


def solution(mesh):
    leaves, across = mesh.shape["leaf"], mesh.shape["grid"]

    def shards(*args):
        levels = [args[8 * i : 8 * i + 8] for i in range(3)]
        root = args[24:30]
        (sl, bl, el, qs, pv, cl, rk, tg) = zip(*levels)
        src = list(sl) + [root[0]]
        blk = list(bl) + [root[1]]
        exp = list(el) + [root[2]]
        bas = list(qs) + [root[3]]
        piv = [v.reshape(1, -1) for v in list(pv) + [root[4]]]
        rnk = list(rk) + [root[5]]
        tgt = [t.reshape(1, -1) for t in tg]
        count = src[0].shape[0]
        ups = [t.shape[1] for t in tgt]
        fronts = [r.shape[0] for r in rnk]
        rnk = [r.T if r.shape[0] > 2 else r for r in rnk]
        size = [leaves * across // f for f in fronts]
        for v in src:
            assert v.shape[1] == LANES
        vm = lambda *s: pltpu.VMEM(s, F32)
        bits = lambda *s: pltpu.VMEM(s, BF16)
        total = leaves * across
        plane = size[1]
        planes = total // plane
        nch = [size[i + 1] // size[i] for i in range(3)]
        caps = [max(1, -(-ups[i] // size[i + 1])) for i in range(3)]
        group = size[:3] + [plane]
        spread = [size[0], size[2], size[3], plane]
        parts = [min(g, 16) for g in group]
        ft = (size[2] * 2 * LANES, LANES)
        bufs = {
            "f0": vm(size[0], count, LANES),
            "f1": vm(plane, count, LANES),
            "f2": vm(size[2], 3 * count, LANES),
            "f3a": vm(plane, 3 * count, LANES),
            "f3s": vm(planes, 3 * count, LANES),
            "f3b": vm(planes, 3 * count, LANES),
            ("f4", "a"): vm(plane, 2 * count, LANES),
            ("f4", "b"): vm(planes, 2 * count, LANES),
            "b1a": vm(plane, (nch[2] + 1) * count, LANES),
            "b1s": vm(planes, 2 * count, LANES),
            "b1b": vm(planes, 2 * count, LANES),
            "b2": vm(size[2], 3 * count, LANES),
            "b3": vm(size[1], count, LANES),
            "tgt_middle": vm(size[2], 1, LANES),
            "tgt_upper": vm(plane, 1, LANES),
            "tgt_layer": vm(planes, 1, LANES),
            "bot_middle": bits(2 * LANES, size[2] * LANES),
            "bot_upper": bits(planes * LANES, plane * LANES),
            "ft_middle": bits(*ft),
            "ft_upper": bits(plane * LANES, planes * LANES),
            "mask": vm(6 + 2 * sum(nch), count, LANES),
            "gram": vm(planes, RANK // parts[3], RANK),
        }
        arrays = {"src": src, "blk": blk, "exp": exp, "bas": bas, "piv": piv, "rnk": rnk, "cpl": cl, "tgt": tgt}
        for name, list_of in arrays.items():
            for i, v in enumerate(list_of):
                bufs[name, i] = pltpu.VMEM(v.shape, v.dtype)
        for i in range(1, 4):
            bufs["fwd", i, 0] = bits(LANES, 3 * RANK)
            bufs["fwd", i, 1] = bits(LANES, 3 * RANK)
        for i in range(4):
            bufs["cross_p", i] = vm(RANK, RANK)
            bufs["rs", i] = vm(group[i], RANK // parts[i], RANK)
            bufs["cross", i] = vm(spread[i] // group[i] * parts[i], RANK // parts[i], RANK)
        for i in range(3):
            wide = max(8, -(-caps[i] // 8) * 8)
            if caps[i] > 4:
                assert size[i] * wide <= LANES
                bufs["low_s", i] = vm(size[i + 1], 1, LANES)
                bufs["low", i] = vm(size[i + 1], 1, LANES)
            bufs["perm", i] = vm(size[i + 1], wide, LANES)
            bufs["couple", i] = vm(size[i + 1], wide, LANES)
            bufs["gt", i] = vm(nch[i] * RANK, LANES * (1 if i == 2 else 2))
            bufs["zp", i] = vm(size[i], count, LANES)
            bufs["piece", i] = vm(nch[i], count, LANES)
        scratch = list(bufs.values())
        scratch += [pltpu.SemaphoreType.DMA((40,)) for _ in range(3)]
        vspec = pl.BlockSpec(memory_space=pltpu.VMEM)
        aspec = pl.BlockSpec(memory_space=pl.ANY)
        answers = pl.pallas_call(
            functools.partial(kernel, (leaves, across, size, ups, count, caps, fronts), list(bufs)),
            out_shape=[pltpu.VMEM(v.shape, F32) for v in src],
            in_specs=[aspec] * 30,
            out_specs=[vspec] * 4,
            scratch_shapes=scratch,
            compiler_params=pltpu.CompilerParams(
                collective_id=0, has_side_effects=True, vmem_limit_bytes=56 * 1024 * 1024
            ),
        )(*src, *blk, *exp, *bas, *piv, *rnk, *cl, *tgt)
        return pl.pallas_call(
            put_out,
            out_shape=[jax.ShapeDtypeStruct(v.shape, F32) for v in src],
            in_specs=[vspec] * 4,
            out_specs=[aspec] * 4,
            scratch_shapes=[pltpu.SemaphoreType.DMA((4,))],
        )(*[pltpu.with_memory_space_constraint(v, pltpu.VMEM) for v in answers])

    spread_axes = ("leaf", "grid")
    level = (P(None, spread_axes), P(spread_axes, None), P(spread_axes, None), P(spread_axes, None), P(spread_axes))
    mid = level + (P(spread_axes, None), P(), P(spread_axes))
    return jax.shard_map(
        shards,
        mesh=mesh,
        in_specs=mid * 3 + level + (P(),),
        out_specs=(P(None, spread_axes),) * 4,
        check_vma=False,
    )
```

```python
import functools
import math

import jax
import jax.numpy as jnp
from jax import lax
from jax.experimental import pallas as pl
from jax.experimental.pallas import tpu as pltpu
from jax.sharding import PartitionSpec as P

RANK = 128
LANES = 128
MESH = pl.DeviceIdType.MESH
F32 = jnp.float32
BF16 = jnp.bfloat16

(
    N_SRC, N_BLK, N_EXP, N_BAS, N_PIV, N_RNK, N_CPL, N_TGT, N_RULER, N_COUPLE, N_MASK, N_OWN, N_KID,
    N_CROSS_P, N_LAST, N_NEAR, N_FWD, N_GT, N_CROSS, N_RS, N_GRAM, N_PERM, N_HIT, N_LOW_S, N_LOW, N_GTH,
    N_ROWS_S, N_ROWS_R, N_NAMED, N_G_P, N_G_RS, N_G_ZS, N_G_Z, N_G, N_GH, N_Z, N_XZ, N_BACK, N_TGT_MIDDLE,
    N_BOT_MIDDLE, N_TGT_UPPER, N_BOT_UPPER, N_FT_MIDDLE, N_TGT_LAYER, N_FT_UPPER, N_ZP, N_F0, N_F1, N_F2,
    N_F3B, N_F3A, N_F4A, N_HQ, N_F3S, N_F4S, N_F4B, N_B3, N_B2, N_PIECE,
) = range(59)


def once(a, b, ca, cb):
    return lax.dot_general(a, b, (((ca,), (cb,)), ((), ())), preferred_element_type=F32)


def halves(x):
    hi = x.astype(BF16)
    return hi, (x - hi.astype(F32)).astype(BF16)


def dot(a, b, ca, cb):
    ah, al = halves(a)
    bh, bl = halves(b)
    if ca == 0:
        return once(ah, bh, ca, cb) + (once(al, bh, ca, cb) + once(ah, bl, ca, cb))
    n = a.shape[0]
    both = once(jnp.concatenate([ah.astype(F32), al.astype(F32)], axis=0).astype(BF16), bh, ca, cb)
    return both[:n] + (both[n:] + once(ah, bl, ca, cb))


def mult(a, b):
    return dot(a, b, 1, 0)


def outer(a, b):
    return dot(a, b, 1, 1)


def inner(a, b):
    return dot(a, b, 0, 0)


def select(x, onehot, cb):
    hi = x.astype(BF16).astype(F32)
    out = once(jnp.concatenate([hi, x - hi], axis=0).astype(BF16), onehot, 1, cb)
    n = x.shape[0]
    return out[:n] + out[n:]


KINDS = (N_SRC, N_BLK, N_EXP, N_BAS, N_PIV, N_RNK)


def kernel(cfg, names, *refs):
    leaves, across, size, ups, count, caps, fronts = cfg
    total_devices = leaves * across
    hbm = [refs[4 * i : 4 * i + 4] for i in range(6)]
    cpl_in = refs[24:27]
    tgt_in = refs[27:30]
    outs = refs[30:34]
    m = dict(zip(names, refs[34:-4]))
    send_sem, recv_sem, load_sem, up_sem = refs[-4:]
    sems = {}
    src, blk, exp, bas, piv, rnk = [[m[k, i] for i in range(4)] for k in KINDS]
    cpl = [m[N_CPL, i] for i in range(3)]
    tgt = [m[N_TGT, i] for i in range(3)]

    me = lax.axis_index("leaf") * across + lax.axis_index("grid")
    plane = size[1]
    planes = total_devices // plane
    spot = me % plane
    layer = me // plane
    late = total_devices > 64
    pending = []

    shared_sends = total_devices <= 64
    sent_rows = []
    loaded = set()
    order = [[(N_SRC, 0), (N_BAS, 0)], [(N_EXP, 1), (N_BAS, 1)]]
    order += [[(N_CPL, 0), (N_TGT, 0)], [(N_BLK, 0), (N_EXP, 0), (N_PIV, 0)]]
    order += [[(N_RNK, i)] for i in range(4)]
    order += [[(N_BLK, 1), (N_SRC, 1), (N_PIV, 1), (N_CPL, 1), (N_TGT, 1), (N_TGT, 2), (N_CPL, 2)]]
    order += [[(k, i) for k in (N_EXP, N_BAS, N_BLK, N_SRC, N_PIV)] for i in (2, 3)]
    where_from = {(k, i): hbm[j][i] for j, k in enumerate(KINDS) for i in range(4)}
    for i in range(3):
        where_from[N_CPL, i] = cpl_in[i]
        where_from[N_TGT, i] = tgt_in[i]

    def load(some):
        for keys in some:
            for key in keys:
                pltpu.make_async_copy(where_from[key], m[key], load_sem.at[order.index(keys)]).start()

    def rows_in(ref):
        return math.prod(ref.shape) // LANES

    def wait_rows(rows, sem):
        wait_for(m[N_RULER].at[pl.ds(0, rows)], sem)

    def need(*wanted):
        for i, keys in enumerate(order):
            if any(key in keys for key in wanted) and i not in loaded:
                loaded.add(i)
                if len(keys) == 1:
                    wait_for(m[keys[0]], load_sem.at[i])
                else:
                    wait_rows(sum(rows_in(m[key]) for key in keys), load_sem.at[i])

    def where(peer):
        return (lax.div(peer, across), lax.rem(peer, across))

    def sem_of(name):
        return sems.setdefault(name, len(sems))

    def remote(a, b, sem, peer):
        return pltpu.make_async_remote_copy(
            src_ref=a,
            dst_ref=b,
            send_sem=send_sem.at[0 if shared_sends else sem],
            recv_sem=recv_sem.at[sem],
            device_id=where(peer),
            device_id_type=MESH,
        )

    def wait_for(part, sem):
        pltpu.make_async_copy(part, part, sem).wait()

    def send_each(source, dest, group, name, stride=1):
        idx = me // stride % group
        base = me - idx * stride
        sem = sem_of(name)

        def body(k, carry):
            q = lax.rem(idx + k, group)
            remote(source(q), dest(idx), sem, base + q * stride).start()
            return carry

        lax.fori_loop(1, group, body, 0)

    def send_all(name, group, stride=1):
        buf = m[name]
        idx = me // stride % group
        send_each(lambda q: buf.at[idx], lambda i: buf.at[i], group, name, stride)
        pending.append((buf.at[pl.ds(0, group - 1)], sem_of(name)))

    def arrive(name, group):
        wait_for(m[name].at[pl.ds(0, group - 1)], recv_sem.at[sem_of(name)])

    load(order[:3])
    m[N_COUPLE, 2][...] = jnp.zeros(m[N_COUPLE, 2].shape, F32)
    barrier = pltpu.get_barrier_semaphore()

    def greet_near(k, carry):
        peer = me - spot + lax.rem(spot + k, plane)
        pl.semaphore_signal(barrier, inc=1, device_id=where(peer), device_id_type=MESH)
        return carry

    def greet_far(peer, carry):
        pl.semaphore_signal(barrier, inc=1, device_id=where(peer), device_id_type=MESH)
        return carry

    def greet_back(k, carry):
        pl.semaphore_signal(up_sem, inc=1, device_id=where(k * plane + spot), device_id_type=MESH)
        return carry

    lax.fori_loop(1, plane, greet_near, 0)
    lax.fori_loop((layer + 1) * plane, total_devices, greet_far, 0)
    load(order[3:])

    col = lax.broadcasted_iota(jnp.int32, (count, RANK), 1).astype(F32)
    mask_slots = {}

    def fill_mask(name, level, front, which):
        ranks = rnk[level][...].astype(F32)
        if ranks.shape[0] == 2 and fronts[level] > 2:
            lane = lax.broadcasted_iota(jnp.int32, ranks.shape, 1)
            row = lax.broadcasted_iota(jnp.int32, ranks.shape, 0)
            hit = (lane == front) & (row == which)
        else:
            lane = lax.broadcasted_iota(jnp.int32, ranks.shape, 1)
            row = lax.broadcasted_iota(jnp.int32, ranks.shape, 0)
            hit = (lane == which) & (row == front)
        r = jnp.sum(jnp.where(hit, ranks, 0.0), axis=1, keepdims=True)
        r = jnp.sum(r, axis=0, keepdims=True)
        slot = mask_slots.setdefault(name, len(mask_slots))
        m[N_MASK][slot] = (col < r).astype(F32)

    def mask(*name):
        return m[N_MASK][mask_slots[name]]

    def fill_masks(level):
        need((N_RNK, level))
        fill_mask((N_OWN, level, 0), level, me // size[level], 0)
        if level == 3:
            return
        fill_mask((N_OWN, level, 1), level, me // size[level], 1)
        nch = size[level + 1] // size[level]
        for child in range(nch):
            front = me // size[level + 1] * nch + child
            fill_mask((N_KID, level, child, 1), level, front, 1)

    def build_forward(level):
        need((N_BLK, level), (N_BAS, level), (N_PIV, level), (N_EXP, level))
        parts = [blk[level][...], bas[level][:, :RANK]]
        if level == 3:
            pt = exp[3][...].T * piv[3][...]
            m[N_CROSS_P, 3][...] = mult(pt, exp[3][...])
            m[N_LAST, 3][...] = outer(blk[3][...], pt)
            m[N_NEAR][...] = outer(blk[3][...] * piv[3][...], blk[3][...])
            parts += [m[N_LAST, 3][...], m[N_NEAR][...]]
        else:
            m[N_LAST, level][...] = mult(blk[level][...], bas[level][:, RANK:])
        put_halves((N_FWD, level), 0, jnp.concatenate(parts, axis=1))

    def put_halves(name, start, value, first=0):
        hi, lo = halves(value)
        lanes = slice(start, start + value.shape[1])
        rows = slice(first, first + value.shape[0])
        m[name, 0][rows, lanes] = hi
        m[name, 1][rows, lanes] = lo

    def chain_forward(level):
        top = m[(N_FWD, level), 0][:LANES].astype(F32) + m[(N_FWD, level), 1][:LANES].astype(F32)
        put_halves((N_FWD, level), 0, -mult(m[N_GT, level - 1][:, :LANES], top), LANES)

    def add_cross(level):
        arrive_cross(level)
        heads = bas[level][:, :RANK] * mask(N_OWN, level, 0)[:1]
        yt = m[N_LAST, level][...] + mult(heads, m[N_CROSS, level][...].reshape(RANK, RANK))
        m[N_LAST, level][...] = yt
        if level > 0:
            put_halves((N_FWD, level), 2 * RANK, yt)

    def by_halves(a, name, cb, lanes=slice(None)):
        ah, al = halves(a)
        n = a.shape[0]
        wh = m[name, 0][:, lanes]
        two = once(jnp.concatenate([ah.astype(F32), al.astype(F32)], axis=0).astype(BF16), wh, 1, cb)
        return two[:n] + (two[n:] + once(ah, m[name, 1][:, lanes], 1, cb))

    def local_forward(level, b):
        out = by_halves(b, (N_FWD, level), 0)
        return [out[:, i : i + RANK] for i in range(0, out.shape[1], RANK)]

    def group_of(level):
        return size[level] if level < 3 else plane

    parts_of = [min(group_of(level), 16) for level in range(4)]

    def scatter_cross(level):
        g = group_of(level)
        p = parts_of[level]
        rp = RANK // p
        idx = me % g
        base = me - idx
        sem = sem_of((N_RS, level))
        cross_p, rs_buf = m[N_CROSS_P, level], m[N_RS, level]

        def body(k, carry):
            q = lax.rem(idx + k, p)

            def go():
                rows = pl.ds(pl.multiple_of(q * rp, 8), rp)
                remote(cross_p.at[rows], rs_buf.at[idx], sem, base + q).start()

            if g == p:
                go()
            else:
                pl.when(q != idx)(go)
            return carry

        lax.fori_loop(1 if g == p else 0, p, body, 0)
        sent_rows.append((p - 1) * rp)

        def keep():
            rows = pl.ds(pl.multiple_of(idx * rp, 8), rp)
            rs_buf[idx] = cross_p[rows, :]

        if g == p:
            keep()
        else:
            pl.when(idx < p)(keep)

    def spread_of(level):
        return group_of(level)

    def holds_part(level, go):
        if group_of(level) == parts_of[level]:
            go()
        else:
            pl.when(me % group_of(level) < parts_of[level])(go)

    def sum_parts(level):
        g = group_of(level)
        wait_for(m[N_RS, level].at[pl.ds(0, g - 1)], recv_sem.at[sem_of((N_RS, level))])
        return jnp.sum(m[N_RS, level][...], axis=0)

    def cross_planes():
        buf = m[N_GRAM]

        def go():
            buf[layer] = sum_parts(3)
            send_each(lambda q: buf.at[layer], lambda i: buf.at[i], planes, N_GRAM, plane)
            sent_rows.append((planes - 1) * rows_in(buf) // planes)

        holds_part(3, go)

    def gather_cross(level):
        g = group_of(level)
        gp = spread_of(level)
        p = parts_of[level]
        idx = me % g
        place = me % gp
        sem = sem_of((N_CROSS, level))
        slot = place // g * p + idx
        buf = m[N_CROSS, level]

        def go():
            if level == 3:
                arrive(N_GRAM, planes)
                buf[slot] = jnp.sum(m[N_GRAM][...], axis=0)
            else:
                buf[slot] = sum_parts(level)

            def body(k, carry):
                peer = me - place + lax.rem(place + k, gp)
                remote(buf.at[slot], buf.at[slot], sem, peer).start()
                return carry

            lax.fori_loop(1, gp, body, 0)
            sent_rows.append((gp - 1) * rows_in(buf) // p)

        holds_part(level, go)

    def rows_path(level):
        return size[level] * wide_of(level) <= LANES

    def tucked(level):
        return caps[level] < wide_of(level)

    def couple_rows(level):
        return caps[level] + 1 if rows_path(level) and tucked(level) else wide_of(level)

    def wide_of(level):
        return max(8, -(-caps[level] // 8) * 8)

    def make_couple(level):
        need((N_TGT, level), (N_CPL, level))
        g = size[level]
        gp = size[level + 1]
        u = ups[level]
        wide = wide_of(level)
        sep = gp * LANES
        t = tgt[level][...]
        upd = t >= sep
        rel = jnp.where(upd, t - sep, t)
        dst = rel // LANES
        low = rel % LANES + jnp.where(upd, LANES, 0)
        ri = lax.broadcasted_iota(jnp.int32, (u, u), 0)
        ci = lax.broadcasted_iota(jnp.int32, (u, u), 1)
        dst_f = dst.astype(F32)
        dst_c = jnp.sum(jnp.where(ri == ci, jnp.broadcast_to(dst_f, (u, u)), 0.0), axis=1, keepdims=True)
        same = dst_c == dst_f
        rank = jnp.sum(jnp.where(same & (ri < ci), 1.0, 0.0), axis=0, keepdims=True).astype(jnp.int32)
        pos = dst * wide + rank
        slots = gp * wide
        si = lax.broadcasted_iota(jnp.int32, (slots, u), 0)
        hit = (si == pos).astype(F32)
        hit16 = hit.astype(BF16)
        moved = sum(once(hit16, piece, 1, 0) for piece in halves(cpl[level][...]))
        perm_buf, recv_c = m[N_PERM, level], m[N_COUPLE, level]
        idx = me % gp
        if level == 2:
            m[N_HIT, 0][...] = hit16
            m[N_HIT, 1][...] = (si == pos + 4).astype(F32).astype(BF16)
        if rows_path(level):
            rank_c = jnp.sum(jnp.where(same & (ci < ri), 1.0, 0.0), axis=1, keepdims=True)
            first = (me % g * wide).astype(F32)
            lane = lax.broadcasted_iota(jnp.int32, (u, LANES), 1).astype(F32)
            place = (lane == rank_c + first).astype(F32).astype(BF16)
            low_f = low.astype(F32)
            if tucked(level):
                named = jnp.where(si == dst * wide + caps[level], low_f, 0.0).astype(BF16)
                moved = moved + once(named, place, 1, 0)
            else:
                qi = lax.broadcasted_iota(jnp.int32, (gp, u), 0)
                named = jnp.where(qi == dst, low_f, 0.0).astype(BF16)
                lows = once(named, place, 1, 0)
                lows_s, lows_r = m[N_LOW_S, level], m[N_LOW, level]
                for q in range(gp):
                    lows_s[q] = lows[q : q + 1, :]
                lows_r[idx] = lows_s[idx]
        else:
            shifted = (si == pos + 4).astype(F32)
            lowc = jnp.sum(shifted * low.astype(F32), axis=1, keepdims=True)
            moved = moved + jnp.broadcast_to(lowc, (slots, LANES))
        perm_buf[...] = moved.reshape(gp, wide, LANES)
        recv_c[idx] = perm_buf[idx]

    def send_couple(level):
        gp = size[level + 1]
        perm_buf, recv_c = m[N_PERM, level], m[N_COUPLE, level]
        if rows_path(level) and not tucked(level):
            lows_s, lows_r = m[N_LOW_S, level], m[N_LOW, level]
            send_each(lambda q: lows_s.at[q], lambda i: lows_r.at[i], gp, (N_LOW, level))
            pending.append((lows_s.at[pl.ds(0, gp - 1)], sem_of((N_LOW, level))))
        part = pl.ds(0, couple_rows(level))
        send_each(lambda q: perm_buf.at[q, part], lambda i: recv_c.at[i, part], gp, (N_COUPLE, level))
        pending.append((perm_buf.at[pl.ds(0, gp - 1), part], sem_of((N_COUPLE, level))))

    def ship_couple(level):
        make_couple(level)
        send_couple(level)

    def low_row(level, child):
        g = size[level]
        got = m[N_COUPLE, level] if tucked(level) else m[N_LOW, level]
        one = slice(caps[level], caps[level] + 1) if tucked(level) else slice(0, 1)
        return jnp.sum(got[child * g : (child + 1) * g, one, :], axis=0)[:, : g * wide_of(level)]

    def low_column(level, child):
        g = size[level]
        got = m[N_COUPLE, level][child * g : (child + 1) * g].reshape(g * wide_of(level), LANES)
        si = lax.broadcasted_iota(jnp.int32, (got.shape[0], 1), 0)
        up = jnp.concatenate([got[4:, :1], got[:4, :1]], axis=0)
        return jnp.where(si % 8 < 4, up, -1.0), jnp.where(si % 8 < 4, -1.0, got[:, :1])

    def build_gt(level):
        g = size[level]
        gp = size[level + 1]
        wide = wide_of(level)
        gt = m[N_GT, level]
        rows = gt.shape[1]
        if rows_path(level) and not tucked(level):
            arrive((N_LOW, level), gp)
        got_all = m[N_COUPLE, level]
        wait_for(
            got_all.at[pl.ds(0, gp - 1), pl.ds(0, couple_rows(level))],
            recv_sem.at[sem_of((N_COUPLE, level))],
        )
        slots = g * wide
        for child in range(gp // g):
            got = got_all[child * g : (child + 1) * g].reshape(slots, LANES)
            if rows_path(level):
                if tucked(level):
                    si = lax.broadcasted_iota(jnp.int32, (slots, LANES), 0)
                    got = jnp.where(si % wide < caps[level], got, 0.0)
                ri = lax.broadcasted_iota(jnp.int32, (rows, slots), 0).astype(F32)
                ot = (ri == low_row(level, child)).astype(F32).astype(BF16)
                full = sum(once(piece, ot, 0, 1) for piece in halves(got))
            else:
                lane = lax.broadcasted_iota(jnp.int32, (slots, rows), 1).astype(F32)
                ot = (lane == low_column(level, child)[0]).astype(F32).astype(BF16)
                full = sum(once(piece, ot, 0, 0) for piece in halves(got))
            gt[child * RANK : (child + 1) * RANK, :] = full
            if level < 2:
                put_halves((N_GTH, level), 0, full, child * RANK)

    def reply_rows():
        g = size[2]
        wide = wide_of(2)
        slots = g * wide
        heads = halves(bas[3][:, :RANK])
        tails = halves(m[N_LAST, 3][...])
        for child in range(size[3] // g):
            if rows_path(2):
                low = low_row(2, child)
                lane = lax.broadcasted_iota(jnp.int32, (1, slots), 1) % wide
                one = jnp.where(lane < 4, low, -1.0)
                two = jnp.where(lane < 4, -1.0, pltpu.roll(low, 4, 1))
                iota, by = lax.broadcasted_iota(jnp.int32, (LANES, slots), 0), 0
            else:
                one, two = low_column(2, child)
                iota, by = lax.broadcasted_iota(jnp.int32, (slots, LANES), 1), 1
            iota = iota.astype(F32)
            first = (iota == one).astype(F32).astype(BF16)
            second = (iota == two).astype(F32).astype(BF16)
            rows = once(first, heads[0], by, 0) + once(first, heads[1], by, 0)
            rows = rows + (once(second, tails[0], by, 0) + once(second, tails[1], by, 0))
            m[N_ROWS_S][child * g : (child + 1) * g] = rows.reshape(g, wide, LANES)
        m[N_ROWS_R][me] = m[N_ROWS_S][me]
        send_each(lambda q: m[N_ROWS_S].at[q], lambda i: m[N_ROWS_R].at[i], size[3], N_ROWS_R)
        pending.append((m[N_ROWS_S].at[pl.ds(0, size[3] - 1)], sem_of(N_ROWS_R)))

    def build_named():
        arrive(N_ROWS_R, size[3])
        got = m[N_ROWS_R][...].reshape(size[3] * wide_of(2), LANES)
        pieces = halves(got)
        out = [
            once(pieces[0], m[N_HIT, i][...], 0, 0) + once(pieces[1], m[N_HIT, i][...], 0, 0)
            for i in range(2)
        ]
        put_halves(N_NAMED, 0, jnp.concatenate(out, axis=0))

    g_p = min(plane, 16)
    g_rp = RANK // g_p

    def g_holds(go):
        if plane == g_p:
            go()
        else:
            pl.when(spot < g_p)(go)

    def g_scatter():
        both = jnp.concatenate([bas[3][:, :RANK], m[N_LAST, 3][...]], axis=1)
        full = mult(m[N_GT, 2][...], both)
        n = full.shape[0] // RANK
        for j in range(g_p):
            m[N_G_P][j] = jnp.concatenate(
                [full[c * RANK + j * g_rp : c * RANK + (j + 1) * g_rp] for c in range(n)], axis=0
            )
        sem = sem_of(N_G_RS)

        def body(k, carry):
            q = lax.rem(spot + k, g_p)

            def go():
                remote(m[N_G_P].at[q], m[N_G_RS].at[spot], sem, me - spot + q).start()

            if plane == g_p:
                go()
            else:
                pl.when(q != spot)(go)
            return carry

        lax.fori_loop(1 if plane == g_p else 0, g_p, body, 0)
        sent_rows.append((g_p - 1) * rows_in(m[N_G_P]) // g_p)

        def keep():
            m[N_G_RS][spot] = m[N_G_P][spot]

        g_holds(keep)

    def upper_of(q):
        return q * plane // size[2]

    def g_across():
        def go():
            arrive(N_G_RS, plane)
            total = jnp.sum(m[N_G_RS][...], axis=0)
            for c in range(total.shape[0] // g_rp):
                m[N_G_ZS][c] = total[c * g_rp : (c + 1) * g_rp]
            m[N_G_Z][layer] = m[N_G_ZS][upper_of(layer)]
            send_each(lambda q: m[N_G_ZS].at[upper_of(q)], lambda i: m[N_G_Z].at[i], planes, N_G_Z, plane)
            sent_rows.append((planes - 1) * rows_in(m[N_G_Z]) // planes)

        g_holds(go)

    def g_gather():
        def go():
            arrive(N_G_Z, planes)
            m[N_G][spot] = jnp.sum(m[N_G_Z][...], axis=0)
            send_each(lambda q: m[N_G].at[spot], lambda i: m[N_G].at[i], plane, N_G)
            sent_rows.append((plane - 1) * rows_in(m[N_G]) // g_p)

        g_holds(go)

    def g_arrive():
        sem = recv_sem.at[sem_of(N_G)]
        if plane == g_p:
            wait_for(m[N_G].at[pl.ds(0, g_p - 1)], sem)
        else:
            pl.when(spot < g_p)(lambda: wait_for(m[N_G].at[pl.ds(0, g_p - 1)], sem))
            pl.when(spot >= g_p)(lambda: wait_for(m[N_G].at[pl.ds(0, g_p)], sem))
        hi, lo = halves(m[N_G][...].reshape(RANK, 2 * RANK))
        m[N_GH, 0][...] = hi
        m[N_GH, 1][...] = lo

    def g_drain():
        if plane == g_p:
            wait_for(m[N_G_P].at[pl.ds(0, g_p - 1)], send_sem.at[sem_of(N_G_RS)])
        else:
            pl.when(spot < g_p)(lambda: wait_for(m[N_G_P].at[pl.ds(0, g_p - 1)], send_sem.at[sem_of(N_G_RS)]))
            pl.when(spot >= g_p)(lambda: wait_for(m[N_G_P], send_sem.at[sem_of(N_G_RS)]))

        def go():
            wait_for(m[N_G_Z].at[pl.ds(0, planes - 1)], send_sem.at[sem_of(N_G_Z)])
            n = plane - 1
            while n > 0:
                wait_for(m[N_G].at[pl.ds(0, min(n, g_p))], send_sem.at[sem_of(N_G)])
                n -= g_p

        g_holds(go)

    def prepare_back(level):
        z = m[N_Z, level][...]
        heads = bas[level][:, :RANK]
        own = mask(N_OWN, level, 0)
        xz = outer(z, blk[level][...]) + outer(shared(level) * own, heads)
        yt = m[N_LAST, level][...]
        if level > 0:
            sep = m[N_GT, level - 1][:, :LANES]
            xz = jnp.concatenate([xz, outer(xz, sep)], axis=1)
            yt = jnp.concatenate([yt, mult(sep, yt)], axis=0)
        m[N_XZ, level][...] = xz
        put_halves((N_BACK, level), 0, yt)

    def arrive_cross(level):
        g = group_of(level)
        p = parts_of[level]
        n = spread_of(level) // g * p
        sem = recv_sem.at[sem_of((N_CROSS, level))]
        buf = m[N_CROSS, level]
        if g == p:
            wait_for(buf.at[pl.ds(0, n - 1)], sem)
        else:
            idx = me % g
            pl.when(idx < p)(lambda: wait_for(buf.at[pl.ds(0, n - 1)], sem))
            pl.when(idx >= p)(lambda: wait_for(buf.at[pl.ds(0, n)], sem))

    def build_bot_middle():
        gp = size[2]
        place = me % gp
        rows = 2 * LANES
        ri = lax.broadcasted_iota(jnp.int32, (rows, LANES), 0)
        arrive(N_TGT_MIDDLE, gp)
        mine = jnp.where(ri < LANES, place * LANES + ri, (gp + place - 1) * LANES + ri).astype(F32)

        def fill(j, carry):
            t = m[N_TGT_MIDDLE][j]
            lanes = pl.ds(pl.multiple_of(j * LANES, LANES), LANES)
            m[N_BOT_MIDDLE][:, lanes] = (mine == t).astype(F32).astype(BF16)
            return carry

        lax.fori_loop(0, gp, fill, 0)

    def build_bot_upper():
        rows = planes * LANES
        ri = lax.broadcasted_iota(jnp.int32, (rows, LANES), 0)
        arrive(N_TGT_UPPER, plane)
        mine = ((ri // LANES * plane + spot) * LANES + ri % LANES).astype(F32)

        def fill(j, carry):
            t = m[N_TGT_UPPER][j]
            lanes = pl.ds(pl.multiple_of(j * LANES, LANES), LANES)
            m[N_BOT_UPPER][:, lanes] = (mine == t).astype(F32).astype(BF16)
            return carry

        lax.fori_loop(0, plane, fill, 0)

    def build_ft_middle():
        t = tgt[1][...]
        ri = lax.broadcasted_iota(jnp.int32, (LANES, LANES), 0)

        def fill(j, carry):
            rows = pl.ds(pl.multiple_of(j * LANES, LANES), LANES)
            m[N_FT_MIDDLE][rows, :] = (ri + j * LANES == t).astype(F32).astype(BF16)
            return carry

        lax.fori_loop(0, m[N_FT_MIDDLE].shape[0] // LANES, fill, 0)

    def build_ft_upper():
        arrive(N_TGT_LAYER, planes)
        t = jnp.concatenate([m[N_TGT_LAYER][j] for j in range(planes)], axis=1)
        ri = lax.broadcasted_iota(jnp.int32, (LANES, planes * LANES), 0)

        def fill(j, carry):
            rows = pl.ds(pl.multiple_of(j * LANES, LANES), LANES)
            here = ((ri + (layer * plane + j) * LANES).astype(F32) == t).astype(F32)
            m[N_FT_UPPER][rows, :] = here.astype(BF16)
            return carry

        lax.fori_loop(0, plane, fill, 0)

    def share(level, zp):
        m[N_ZP, level][me % size[level]] = zp
        send_all((N_ZP, level), size[level])

    def shared(level):
        arrive((N_ZP, level), size[level])
        return jnp.sum(m[N_ZP, level][...], axis=0)

    def make_cross(level):
        need((N_EXP, level), (N_BAS, level))
        m[N_CROSS_P, level][...] = inner(exp[level][...], bas[level][:, RANK:])

    def start_cross(level):
        make_cross(level)
        scatter_cross(level)

    need((N_SRC, 0), (N_BAS, 0))
    m[N_F0][me % size[0]] = mult(src[0][...], bas[0][:, :RANK])
    make_cross(1)
    pl.semaphore_wait(barrier, plane - 1 + layer * plane)
    send_all(N_F0, size[0])
    scatter_cross(1)
    lax.fori_loop(0, layer, greet_back, 0)
    ship_couple(0)
    need((N_BLK, 0), (N_EXP, 0), (N_PIV, 0))
    local = mult(src[0][...], blk[0][...])
    fill_masks(0)
    build_forward(1)
    make_cross(2)
    pl.when(layer < planes - 1)(lambda: pl.semaphore_wait(up_sem, planes - 1 - layer))
    scatter_cross(2)
    arrive(N_F0, size[0])
    hq = jnp.sum(m[N_F0][...], axis=0) * mask(N_OWN, 0, 0)
    y = local + outer(hq, exp[0][...])
    m[N_F1][spot] = mult(y, bas[0][:, RANK:])
    send_all(N_F1, plane)
    m[N_Z, 0][...] = y * piv[0][...]
    fill_masks(1)
    gather_cross(1)
    need((N_TGT, 1), (N_TGT, 2))
    m[N_TGT_MIDDLE][me % size[2]] = tgt[1][...].astype(F32)
    send_all(N_TGT_MIDDLE, size[2])
    mine_t = tgt[2][...].astype(F32)
    m[N_TGT_UPPER][spot] = mine_t
    send_all(N_TGT_UPPER, plane)
    m[N_TGT_LAYER][layer] = mine_t
    send_all(N_TGT_LAYER, planes, plane)
    ship_couple(1)
    ship_couple(2)
    gather_cross(2)
    build_gt(0)
    add_cross(1)

    for level in range(3):
        g = size[level]
        gp = size[level + 1]
        nch = gp // g
        child_me = me % gp // g
        need((N_SRC, level + 1))
        name = (N_F1, N_F2, N_F3B)[level]
        buf, step = m[name], g
        if level == 2:
            step = g // plane
        arrive(name, gp if level < 2 else planes)
        ws = [
            jnp.sum(buf[child * step : (child + 1) * step, :count, :], axis=0) * mask(N_KID, level, child, 1)
            for child in range(nch)
        ]
        ws = jnp.concatenate(ws, axis=1)
        bn = src[level + 1][...]
        upd = 0.0
        if level == 0:
            inc = by_halves(ws, (N_GTH, 0), 0)
            bn = bn - inc[:, :LANES]
            upd = -inc[:, LANES:]
        elif level == 1:
            rows = jnp.concatenate([buf[j, count : 2 * count, :] for j in range(gp)], axis=1)
            inc = select(rows, m[N_BOT_MIDDLE][...], 1)
            bn = jnp.concatenate([bn + inc[:, :LANES], ws], axis=1)
            upd = inc[:, LANES:] - by_halves(ws, (N_GTH, 1), 0, slice(LANES, 2 * LANES))
        else:
            bn = jnp.concatenate([bn + jnp.sum(buf[:, count : 2 * count, :], axis=0), ws], axis=1)
        local_n, bq, *sent = local_forward(level + 1, bn)
        if level < 2:
            sent.append(upd)
        else:
            sent = [bq] + sent[:1] + sent[2:] + sent[1:2]
        name = (N_F2, N_F3A, N_F4A)[level]
        group = size[2] if level == 0 else plane
        m[name][me % group] = jnp.concatenate(sent, axis=0)
        send_all(name, group)
        if level < 2:
            m[N_HQ, level + 1][me % gp] = bq
            send_all((N_HQ, level + 1), gp)
        if level > 0:
            arrive((N_HQ, level), g)
            hq = jnp.sum(m[N_HQ, level][...], axis=0) * mask(N_OWN, level, 0)
            z = (local + outer(hq, exp[level][...])) * piv[level][...]
            m[N_Z, level][...] = z
            share(level, mult(z, exp[level][...]))
        local = local_n
        if level == 0:
            build_forward(2)
            fill_masks(2)
            build_forward(3)
            scatter_cross(3)
            build_gt(1)
            build_bot_middle()
            add_cross(2)
            chain_forward(2)
        elif level == 1:
            build_gt(2)
            g_scatter()
            reply_rows()
            build_bot_upper()
            fill_masks(3)
            arrive(N_F3A, plane)
            sums = jnp.sum(m[N_F3A][:, :count, :], axis=0)
            rows = jnp.concatenate([m[N_F3A][j, count:, :] for j in range(plane)], axis=1)
            part = select(rows, m[N_BOT_UPPER][...], 1)
            for q in range(planes):
                m[N_F3S][q] = jnp.concatenate([sums, part[:, q * LANES : (q + 1) * LANES]], axis=0)
            m[N_F3B][layer] = m[N_F3S][layer]
            send_each(lambda q: m[N_F3S].at[q], lambda i: m[N_F3B].at[i], planes, N_F3B, plane)
            pending.append((m[N_F3S].at[pl.ds(0, planes - 1)], sem_of(N_F3B)))
            put_halves((N_FWD, 3), 4 * RANK, outer(m[N_NEAR][...], m[N_GT, 2][...]))
            chain_forward(3)
            share(0, mult(m[N_Z, 0][...], exp[0][...]))
            start_cross(0)
            m[N_LAST, 0][...] = mult(blk[0][...], bas[0][:, RANK:])
            build_ft_upper()
            if not late:
                build_ft_middle()
            cross_planes()
        else:
            g_across()

    gather_cross(3)
    gather_cross(0)
    arrive(N_F4A, plane)
    o = (2 + size[3] // size[2]) * count
    sums = jnp.sum(m[N_F4A][:, :o, :], axis=0)
    rows = jnp.concatenate([m[N_F4A][j, o:, :] for j in range(plane)], axis=1)
    part = select(rows, m[N_FT_UPPER][...], 0)
    for q in range(planes):
        c = 2 + q * plane // size[2]
        m[N_F4S][q] = jnp.concatenate(
            [sums[: 2 * count], sums[c * count : (c + 1) * count], part[:, q * LANES : (q + 1) * LANES]], axis=0
        )
    m[N_F4B][layer] = m[N_F4S][layer]
    send_each(lambda q: m[N_F4S].at[q], lambda i: m[N_F4B].at[i], planes, N_F4B, plane)
    pending.append((m[N_F4S].at[pl.ds(0, planes - 1)], sem_of(N_F4B)))
    g_gather()
    build_named()
    prepare_back(2)
    arrive_cross(3)
    arrive(N_F4B, planes)
    g_arrive()
    both = jnp.sum(m[N_F4B][...], axis=0)
    hq = both[:count] * mask(N_OWN, 3, 0)
    rp = (both[count : 2 * count] + mult(hq, m[N_CROSS, 3][...].reshape(RANK, RANK))) * mask(N_OWN, 3, 0)
    pair = jnp.concatenate([rp, hq], axis=1)
    s = both[2 * count : 3 * count] + by_halves(pair, N_GH, 1)
    xu = both[3 * count :] + by_halves(pair, N_NAMED, 0)

    for level in (2, 1, 0):
        s = s * mask(N_OWN, level, 1)
        xs = m[N_XZ, level][...] - by_halves(s, (N_BACK, level), 1)
        x = xs[:, :LANES]
        if level == 0:
            outs[0][...] = x
            break
        g = size[level - 1]
        gp = size[level]
        nch = gp // g
        place = me % gp
        child_me = place // g
        sp = xs[:, LANES:] + by_halves(xu, (N_GTH, level - 1), 1, slice(LANES, 2 * LANES))
        name = (N_B3, N_B2)[level - 1]
        buf, piece = m[name], m[N_PIECE, level - 1]
        for c in range(nch):
            piece[c] = sp[:, c * RANK : (c + 1) * RANK] if level == 1 else jnp.concatenate(
                [sp[:, c * RANK : (c + 1) * RANK], x, xu], axis=0
            )
        buf[place] = piece[child_me]
        send_each(lambda q: piece.at[lax.div(q, g)], lambda i: buf.at[i], gp, name)
        pending.append((buf.at[pl.ds(0, gp - 1)], sem_of(name)))
        outs[level][...] = x
        if level == 2:
            z = (local + outer(hq, exp[3][...])) * piv[3][...]
            outs[3][...] = outer(z, blk[3][...]) + outer(rp, bas[3][:, :RANK])
        else:
            add_cross(0)
        prepare_back(level - 1)
        arrive(name, gp)
        s = jnp.sum(buf[:, :count, :], axis=0)
        if level == 2:
            blocks = [buf[j, count : 2 * count, :] for j in range(gp)]
            blocks += [buf[j, 2 * count :, :] for j in range(gp)]
            if late:
                build_ft_middle()
            xu = select(jnp.concatenate(blocks, axis=1), m[N_FT_MIDDLE][...], 0)

    if shared_sends:
        assert all(group_of(level) == parts_of[level] for level in range(4))
        wait_rows(sum(sent_rows) + sum(rows_in(part) for part, _ in pending), send_sem.at[0])
    else:
        for part, sem in pending:
            wait_for(part, send_sem.at[sem])
        for level in range(4):
            g = group_of(level)
            p = parts_of[level]
            rp = RANK // p
            gp = spread_of(level)
            n = gp // g * p
            idx = me % g
            rs_sem = send_sem.at[sem_of((N_RS, level))]
            ag_sem = send_sem.at[sem_of((N_CROSS, level))]
            cross_p, buf = m[N_CROSS_P, level], m[N_CROSS, level]

            def ag_done():
                for _ in range((gp - 1) // n):
                    wait_for(buf.at[pl.ds(0, n)], ag_sem)
                if (gp - 1) % n:
                    wait_for(buf.at[pl.ds(0, (gp - 1) % n)], ag_sem)
                if level == 3:
                    wait_for(m[N_GRAM].at[pl.ds(0, planes - 1)], send_sem.at[sem_of(N_GRAM)])

            if g == p:
                wait_for(cross_p.at[pl.ds(0, (p - 1) * rp)], rs_sem)
                ag_done()
            else:
                pl.when(idx < p)(lambda: wait_for(cross_p.at[pl.ds(0, (p - 1) * rp)], rs_sem))
                pl.when(idx >= p)(lambda: wait_for(cross_p, rs_sem))
                pl.when(idx < p)(ag_done)
        g_drain()


def put_out(*refs):
    n = len(refs) // 2
    ins, outs, sem = refs[:n], refs[n : 2 * n], refs[-1]
    copies = [pltpu.make_async_copy(ins[i], outs[i], sem.at[i]) for i in range(n)]
    for c in copies:
        c.start()
    for c in copies:
        c.wait()


def solution(mesh):
    leaves, across = mesh.shape["leaf"], mesh.shape["grid"]

    def shards(*args):
        levels = [args[8 * i : 8 * i + 8] for i in range(3)]
        root = args[24:30]
        (sl, bl, el, qs, pv, cl, rk, tg) = zip(*levels)
        src = list(sl) + [root[0]]
        blk = list(bl) + [root[1]]
        exp = list(el) + [root[2]]
        bas = list(qs) + [root[3]]
        piv = [v.reshape(1, -1) for v in list(pv) + [root[4]]]
        rnk = list(rk) + [root[5]]
        tgt = [t.reshape(1, -1) for t in tg]
        count = src[0].shape[0]
        ups = [t.shape[1] for t in tgt]
        fronts = [r.shape[0] for r in rnk]
        rnk = [r.T if r.shape[0] > 2 else r for r in rnk]
        size = [leaves * across // f for f in fronts]
        for v in src:
            assert v.shape[1] == LANES
        vm = lambda *s: pltpu.VMEM(s, F32)
        bits = lambda *s: pltpu.VMEM(s, BF16)
        total = leaves * across
        plane = size[1]
        planes = total // plane
        nch = [size[i + 1] // size[i] for i in range(3)]
        caps = [max(1, -(-ups[i] // size[i + 1])) for i in range(3)]
        group = size[:3] + [plane]
        spread = group
        parts = [min(g, 16) for g in group]
        ft = (size[2] * 2 * LANES, LANES)
        bufs = {
            N_F0: vm(size[0], count, LANES),
            N_F1: vm(plane, count, LANES),
            N_F2: vm(size[2], 2 * count, LANES),
            N_F3A: vm(plane, 2 * count, LANES),
            N_F3S: vm(planes, 2 * count, LANES),
            N_F3B: vm(planes, 2 * count, LANES),
            (N_HQ, 1): vm(size[1], count, LANES),
            (N_HQ, 2): vm(size[2], count, LANES),
            N_F4A: vm(plane, (nch[2] + 3) * count, LANES),
            N_F4S: vm(planes, 4 * count, LANES),
            N_F4B: vm(planes, 4 * count, LANES),
            N_NEAR: vm(LANES, LANES),
            N_RULER: vm(8192 if total <= 64 else 1024, LANES),
            (N_HIT, 0): bits(total * 8, LANES),
            (N_HIT, 1): bits(total * 8, LANES),
            N_ROWS_S: vm(total, 8, LANES),
            N_ROWS_R: vm(total, 8, LANES),
            (N_NAMED, 0): bits(2 * RANK, LANES),
            (N_NAMED, 1): bits(2 * RANK, LANES),
            (N_GH, 0): bits(RANK, 2 * RANK),
            (N_GH, 1): bits(RANK, 2 * RANK),
            N_G_P: vm(parts[3], nch[2] * RANK // parts[3], 2 * RANK),
            N_G_RS: vm(plane, nch[2] * RANK // parts[3], 2 * RANK),
            N_G_ZS: vm(nch[2], RANK // parts[3], 2 * RANK),
            N_G_Z: vm(planes, RANK // parts[3], 2 * RANK),
            N_G: vm(parts[3], RANK // parts[3], 2 * RANK),
            N_B2: vm(size[2], 3 * count, LANES),
            N_B3: vm(size[1], count, LANES),
            N_TGT_MIDDLE: vm(size[2], 1, LANES),
            N_TGT_UPPER: vm(plane, 1, LANES),
            N_TGT_LAYER: vm(planes, 1, LANES),
            N_BOT_MIDDLE: bits(2 * LANES, size[2] * LANES),
            N_BOT_UPPER: bits(planes * LANES, plane * LANES),
            N_FT_MIDDLE: bits(*ft),
            N_FT_UPPER: bits(plane * LANES, planes * LANES),
            N_MASK: vm(6 + 2 * sum(nch), count, LANES),
            N_GRAM: vm(planes, RANK // parts[3], RANK),
        }
        arrays = {N_SRC: src, N_BLK: blk, N_EXP: exp, N_BAS: bas, N_PIV: piv, N_RNK: rnk, N_CPL: cl, N_TGT: tgt}
        for name, list_of in arrays.items():
            for i, v in enumerate(list_of):
                bufs[name, i] = pltpu.VMEM(v.shape, v.dtype)
        for i in range(4):
            bufs[N_LAST, i] = vm(LANES, RANK)
            for j in range(2):
                if i > 0:
                    bufs[(N_FWD, i), j] = bits(LANES + (nch[i - 1] * RANK if i > 1 else 0), (3 if i < 3 else 4 + nch[2]) * RANK)
                if i < 3:
                    bufs[(N_BACK, i), j] = bits((1 + (nch[i - 1] if i > 0 else 0)) * RANK, RANK)
        for i in range(2):
            for j in range(2):
                bufs[(N_GTH, i), j] = bits(nch[i] * RANK, 2 * LANES)
        for i in range(3):
            bufs[N_Z, i] = vm(count, LANES)
            bufs[N_XZ, i] = vm(count, (1 + (nch[i - 1] if i > 0 else 0)) * LANES)
        for i in range(4):
            bufs[N_CROSS_P, i] = vm(RANK, RANK)
            bufs[N_RS, i] = vm(group[i], RANK // parts[i], RANK)
            bufs[N_CROSS, i] = vm(spread[i] // group[i] * parts[i], RANK // parts[i], RANK)
        for i in range(3):
            wide = max(8, -(-caps[i] // 8) * 8)
            assert caps[i] <= 4 or size[i] * wide <= LANES
            if caps[i] == wide:
                bufs[N_LOW_S, i] = vm(size[i + 1], 1, LANES)
                bufs[N_LOW, i] = vm(size[i + 1], 1, LANES)
            bufs[N_PERM, i] = vm(size[i + 1], wide, LANES)
            bufs[N_COUPLE, i] = vm(size[i + 1], wide, LANES)
            bufs[N_GT, i] = vm(nch[i] * RANK, LANES * (1 if i == 2 else 2))
            bufs[N_ZP, i] = vm(size[i], count, LANES)
            bufs[N_PIECE, i] = vm(nch[i], (1 if i == 0 else 3) * count, LANES)
        scratch = list(bufs.values())
        scratch += [pltpu.SemaphoreType.DMA((n,)) for n in (1 if total <= 64 else 37, 37, 11)]
        scratch += [pltpu.SemaphoreType.REGULAR]
        vspec = pl.BlockSpec(memory_space=pltpu.VMEM)
        aspec = pl.BlockSpec(memory_space=pl.ANY)
        answers = pl.pallas_call(
            functools.partial(kernel, (leaves, across, size, ups, count, caps, fronts), list(bufs)),
            out_shape=[pltpu.VMEM(v.shape, F32) for v in src],
            in_specs=[aspec] * 30,
            out_specs=[vspec] * 4,
            scratch_shapes=scratch,
            compiler_params=pltpu.CompilerParams(
                collective_id=0, has_side_effects=True, vmem_limit_bytes=63 * 1024 * 1024
            ),
        )(*src, *blk, *exp, *bas, *piv, *rnk, *cl, *tgt)
        return pl.pallas_call(
            put_out,
            out_shape=[jax.ShapeDtypeStruct(v.shape, F32) for v in src],
            in_specs=[vspec] * 4,
            out_specs=[aspec] * 4,
            scratch_shapes=[pltpu.SemaphoreType.DMA((4,))],
        )(*[pltpu.with_memory_space_constraint(v, pltpu.VMEM) for v in answers])

    spread_axes = ("leaf", "grid")
    level = (P(None, spread_axes), P(spread_axes, None), P(spread_axes, None), P(spread_axes, None), P(spread_axes))
    mid = level + (P(spread_axes, None), P(), P(spread_axes))
    return jax.shard_map(
        shards,
        mesh=mesh,
        in_specs=mid * 3 + level + (P(),),
        out_specs=(P(None, spread_axes),) * 4,
        check_vma=False,
    )
```

```python
import functools
import math

import jax
import jax.numpy as jnp
from jax import lax
from jax.experimental import pallas as pl
from jax.experimental.pallas import tpu as pltpu
from jax.sharding import PartitionSpec as P

RANK = 128
LANES = 128
MESH = pl.DeviceIdType.MESH
F32 = jnp.float32
BF16 = jnp.bfloat16
F8 = jnp.float8_e4m3fn

(
    N_SRC, N_BLK, N_EXP, N_BAS, N_PIV, N_RNK, N_CPL, N_TGT, N_RULER, N_COUPLE, N_MASK, N_OWN, N_KID,
    N_CROSS_P, N_LAST, N_NEAR, N_FWD, N_GT, N_CROSS, N_RS, N_GRAM, N_PERM, N_TAKE_KEY, N_HIT, N_LOW_S, N_LOW,
    N_OT, N_GTH, N_ROWS_S, N_ROWS_R, N_NAMED, N_G_P, N_G_RS, N_G_ZS, N_G_Z, N_G, N_GH, N_Z, N_XZ, N_BACK,
    N_TGT_MIDDLE, N_BOT_MIDDLE, N_TGT_UPPER, N_BOT_UPPER, N_TAKE, N_FT_MIDDLE, N_TGT_LAYER, N_FT_UPPER, N_ZP,
    N_F0, N_F1, N_F2, N_F3B, N_F3A, N_F4A, N_HQ, N_F3S, N_F4S, N_F4B, N_B3, N_B2, N_PIECE,
) = range(62)


def once(a, b, ca, cb):
    return lax.dot_general(a, b, (((ca,), (cb,)), ((), ())), preferred_element_type=F32)


def halves(x):
    hi = x.astype(BF16)
    return hi, (x - hi.astype(F32)).astype(BF16)


def dot(a, b, ca, cb):
    ah, al = halves(a)
    bh, bl = halves(b)
    if ca == 0:
        return once(ah, bh, ca, cb) + (once(al, bh, ca, cb) + once(ah, bl, ca, cb))
    n = a.shape[0]
    both = once(jnp.concatenate([ah.astype(F32), al.astype(F32)], axis=0).astype(BF16), bh, ca, cb)
    return both[:n] + (both[n:] + once(ah, bl, ca, cb))


def mult(a, b):
    return dot(a, b, 1, 0)


def outer(a, b):
    return dot(a, b, 1, 1)


def inner(a, b):
    return dot(a, b, 0, 0)


def select(x, onehot, cb):
    hi = x.astype(BF16).astype(F32)
    out = once(jnp.concatenate([hi, x - hi], axis=0).astype(BF16), onehot, 1, cb)
    n = x.shape[0]
    return out[:n] + out[n:]


KINDS = (N_SRC, N_BLK, N_EXP, N_BAS, N_PIV, N_RNK)


def kernel(cfg, names, *refs):
    leaves, across, size, ups, count, caps, fronts = cfg
    total_devices = leaves * across
    hbm = [refs[4 * i : 4 * i + 4] for i in range(6)]
    cpl_in = refs[24:27]
    tgt_in = refs[27:30]
    outs = refs[30:34]
    m = dict(zip(names, refs[34:-4]))
    send_sem, recv_sem, load_sem, up_sem = refs[-4:]
    sems = {}
    src, blk, exp, bas, piv, rnk = [[m[k, i] for i in range(4)] for k in KINDS]
    cpl = [m[N_CPL, i] for i in range(3)]
    tgt = [m[N_TGT, i] for i in range(3)]

    me = lax.axis_index("leaf") * across + lax.axis_index("grid")
    plane = size[1]
    planes = total_devices // plane
    spot = me % plane
    layer = me // plane
    pending = []

    shared_sends = total_devices <= 64
    sent_rows = []
    loaded = set()
    order = [[(N_SRC, 0), (N_BAS, 0)], [(N_EXP, 1), (N_BAS, 1)]]
    order += [[(N_CPL, 0), (N_TGT, 0)], [(N_BLK, 0), (N_EXP, 0), (N_PIV, 0)]]
    order += [[(N_RNK, i)] for i in range(4)]
    order += [[(N_BLK, 1), (N_SRC, 1), (N_PIV, 1), (N_CPL, 1), (N_TGT, 1), (N_TGT, 2), (N_CPL, 2)]]
    order += [[(k, i) for k in (N_EXP, N_BAS, N_BLK, N_SRC, N_PIV)] for i in (2, 3)]
    where_from = {(k, i): hbm[j][i] for j, k in enumerate(KINDS) for i in range(4)}
    for i in range(3):
        where_from[N_CPL, i] = cpl_in[i]
        where_from[N_TGT, i] = tgt_in[i]

    def load(some):
        for keys in some:
            for key in keys:
                pltpu.make_async_copy(where_from[key], m[key], load_sem.at[order.index(keys)]).start()

    def rows_in(ref):
        return math.prod(ref.shape) // LANES

    def wait_rows(rows, sem):
        wait_for(m[N_RULER].at[pl.ds(0, rows)], sem)

    def need(*wanted):
        for i, keys in enumerate(order):
            if any(key in keys for key in wanted) and i not in loaded:
                loaded.add(i)
                if len(keys) == 1:
                    wait_for(m[keys[0]], load_sem.at[i])
                else:
                    wait_rows(sum(rows_in(m[key]) for key in keys), load_sem.at[i])

    def where(peer):
        return (lax.div(peer, across), lax.rem(peer, across))

    def sem_of(name):
        return sems.setdefault(name, len(sems))

    def remote(a, b, sem, peer):
        return pltpu.make_async_remote_copy(
            src_ref=a,
            dst_ref=b,
            send_sem=send_sem.at[0 if shared_sends else sem],
            recv_sem=recv_sem.at[sem],
            device_id=where(peer),
            device_id_type=MESH,
        )

    def wait_for(part, sem):
        pltpu.make_async_copy(part, part, sem).wait()

    def send_each(source, dest, group, name, stride=1):
        idx = me // stride % group
        base = me - idx * stride
        sem = sem_of(name)

        def body(k, carry):
            q = lax.rem(idx + k, group)
            remote(source(q), dest(idx), sem, base + q * stride).start()
            return carry

        lax.fori_loop(1, group, body, 0)

    def send_all(name, group, stride=1):
        buf = m[name]
        idx = me // stride % group
        send_each(lambda q: buf.at[idx], lambda i: buf.at[i], group, name, stride)
        pending.append((buf.at[pl.ds(0, group - 1)], sem_of(name)))

    def arrive(name, group):
        wait_for(m[name].at[pl.ds(0, group - 1)], recv_sem.at[sem_of(name)])

    load(order[:3])
    m[N_COUPLE, 2][...] = jnp.zeros(m[N_COUPLE, 2].shape, F32)
    barrier = pltpu.get_barrier_semaphore()

    def greet_near(k, carry):
        peer = me - spot + lax.rem(spot + k, plane)
        pl.semaphore_signal(barrier, inc=1, device_id=where(peer), device_id_type=MESH)
        return carry

    def greet_far(peer, carry):
        pl.semaphore_signal(barrier, inc=1, device_id=where(peer), device_id_type=MESH)
        return carry

    def greet_back(k, carry):
        pl.semaphore_signal(up_sem, inc=1, device_id=where(k * plane + spot), device_id_type=MESH)
        return carry

    lax.fori_loop(1, plane, greet_near, 0)
    lax.fori_loop((layer + 1) * plane, total_devices, greet_far, 0)
    load(order[3:])

    col = lax.broadcasted_iota(jnp.int32, (count, RANK), 1).astype(F32)
    mask_slots = {}

    def fill_mask(name, level, front, which):
        ranks = rnk[level][...].astype(F32)
        if ranks.shape[0] == 2 and fronts[level] > 2:
            lane = lax.broadcasted_iota(jnp.int32, ranks.shape, 1)
            row = lax.broadcasted_iota(jnp.int32, ranks.shape, 0)
            hit = (lane == front) & (row == which)
        else:
            lane = lax.broadcasted_iota(jnp.int32, ranks.shape, 1)
            row = lax.broadcasted_iota(jnp.int32, ranks.shape, 0)
            hit = (lane == which) & (row == front)
        r = jnp.sum(jnp.where(hit, ranks, 0.0), axis=1, keepdims=True)
        r = jnp.sum(r, axis=0, keepdims=True)
        slot = mask_slots.setdefault(name, len(mask_slots))
        m[N_MASK][slot] = (col < r).astype(F32)

    def mask(*name):
        return m[N_MASK][mask_slots[name]]

    def fill_masks(level):
        need((N_RNK, level))
        fill_mask((N_OWN, level, 0), level, me // size[level], 0)
        if level == 3:
            return
        fill_mask((N_OWN, level, 1), level, me // size[level], 1)
        nch = size[level + 1] // size[level]
        for child in range(nch):
            front = me // size[level + 1] * nch + child
            fill_mask((N_KID, level, child, 1), level, front, 1)

    def build_forward(level):
        need((N_BLK, level), (N_BAS, level), (N_PIV, level), (N_EXP, level))
        parts = [blk[level][...], bas[level][:, :RANK]]
        if level == 3:
            pt = exp[3][...].T * piv[3][...]
            m[N_CROSS_P, 3][...] = mult(pt, exp[3][...])
            m[N_LAST, 3][...] = outer(blk[3][...], pt)
            m[N_NEAR][...] = outer(blk[3][...] * piv[3][...], blk[3][...])
            parts += [m[N_LAST, 3][...], m[N_NEAR][...]]
        else:
            m[N_LAST, level][...] = mult(blk[level][...], bas[level][:, RANK:])
        put_halves((N_FWD, level), 0, jnp.concatenate(parts, axis=1))

    def put_halves(name, start, value, first=0):
        hi, lo = halves(value)
        lanes = slice(start, start + value.shape[1])
        rows = slice(first, first + value.shape[0])
        m[name, 0][rows, lanes] = hi
        m[name, 1][rows, lanes] = lo

    def chain_forward(level):
        top = m[(N_FWD, level), 0][:LANES].astype(F32) + m[(N_FWD, level), 1][:LANES].astype(F32)
        put_halves((N_FWD, level), 0, -mult(m[N_GT, level - 1][:, :LANES], top), LANES)

    def add_cross(level):
        arrive_cross(level)
        heads = bas[level][:, :RANK] * mask(N_OWN, level, 0)[:1]
        yt = m[N_LAST, level][...] + mult(heads, m[N_CROSS, level][...].reshape(RANK, RANK))
        m[N_LAST, level][...] = yt
        if level > 0:
            put_halves((N_FWD, level), 2 * RANK, yt)

    def by_halves(a, name, cb, lanes=slice(None)):
        ah, al = halves(a)
        n = a.shape[0]
        wh = m[name, 0][:, lanes]
        two = once(jnp.concatenate([ah.astype(F32), al.astype(F32)], axis=0).astype(BF16), wh, 1, cb)
        return two[:n] + (two[n:] + once(ah, m[name, 1][:, lanes], 1, cb))

    def local_forward(level, b):
        out = by_halves(b, (N_FWD, level), 0)
        return [out[:, i : i + RANK] for i in range(0, out.shape[1], RANK)]

    def group_of(level):
        return size[level] if level < 3 else plane

    parts_of = [min(group_of(level), 16) for level in range(4)]

    def scatter_cross(level):
        g = group_of(level)
        p = parts_of[level]
        rp = RANK // p
        idx = me % g
        base = me - idx
        sem = sem_of((N_RS, level))
        cross_p, rs_buf = m[N_CROSS_P, level], m[N_RS, level]

        def body(k, carry):
            q = lax.rem(idx + k, p)

            def go():
                rows = pl.ds(pl.multiple_of(q * rp, 8), rp)
                remote(cross_p.at[rows], rs_buf.at[idx], sem, base + q).start()

            if g == p:
                go()
            else:
                pl.when(q != idx)(go)
            return carry

        lax.fori_loop(1 if g == p else 0, p, body, 0)
        sent_rows.append((p - 1) * rp)

        def keep():
            rows = pl.ds(pl.multiple_of(idx * rp, 8), rp)
            rs_buf[idx] = cross_p[rows, :]

        if g == p:
            keep()
        else:
            pl.when(idx < p)(keep)

    def spread_of(level):
        return group_of(level)

    def holds_part(level, go):
        if group_of(level) == parts_of[level]:
            go()
        else:
            pl.when(me % group_of(level) < parts_of[level])(go)

    def sum_parts(level):
        g = group_of(level)
        wait_for(m[N_RS, level].at[pl.ds(0, g - 1)], recv_sem.at[sem_of((N_RS, level))])
        return jnp.sum(m[N_RS, level][...], axis=0)

    def cross_planes():
        buf = m[N_GRAM]

        def go():
            buf[layer] = sum_parts(3)
            send_each(lambda q: buf.at[layer], lambda i: buf.at[i], planes, N_GRAM, plane)
            sent_rows.append((planes - 1) * rows_in(buf) // planes)

        holds_part(3, go)

    def gather_cross(level):
        g = group_of(level)
        gp = spread_of(level)
        p = parts_of[level]
        idx = me % g
        place = me % gp
        sem = sem_of((N_CROSS, level))
        slot = place // g * p + idx
        buf = m[N_CROSS, level]

        def go():
            if level == 3:
                arrive(N_GRAM, planes)
                buf[slot] = jnp.sum(m[N_GRAM][...], axis=0)
            else:
                buf[slot] = sum_parts(level)

            def body(k, carry):
                peer = me - place + lax.rem(place + k, gp)
                remote(buf.at[slot], buf.at[slot], sem, peer).start()
                return carry

            lax.fori_loop(1, gp, body, 0)
            sent_rows.append((gp - 1) * rows_in(buf) // p)

        holds_part(level, go)

    def wide_of(level):
        return max(8, -(-caps[level] // 8) * 8)

    def rows_path(level):
        return size[level] * wide_of(level) <= LANES

    by_slots = size[2] * wide_of(1) <= LANES

    def tucked(level):
        return caps[level] < wide_of(level)

    def couple_rows(level):
        return caps[level] + 1 if rows_path(level) and tucked(level) else wide_of(level)

    def make_couple(level):
        need((N_TGT, level), (N_CPL, level))
        g = size[level]
        gp = size[level + 1]
        u = ups[level]
        wide = wide_of(level)
        sep = gp * LANES
        t = tgt[level][...]
        upd = t >= sep
        rel = jnp.where(upd, t - sep, t)
        dst = rel // LANES
        low = rel % LANES + jnp.where(upd, LANES, 0)
        ri = lax.broadcasted_iota(jnp.int32, (u, u), 0)
        ci = lax.broadcasted_iota(jnp.int32, (u, u), 1)
        dst_f = dst.astype(F32)
        dst_c = jnp.sum(jnp.where(ri == ci, jnp.broadcast_to(dst_f, (u, u)), 0.0), axis=1, keepdims=True)
        same = dst_c == dst_f
        rank = jnp.sum(jnp.where(same & (ri < ci), 1.0, 0.0), axis=0, keepdims=True).astype(jnp.int32)
        pos = dst * wide + rank
        slots = gp * wide
        si = lax.broadcasted_iota(jnp.int32, (slots, u), 0)
        hit = (si == pos).astype(F32)
        hit16 = hit.astype(BF16)
        moved = sum(once(hit16, piece, 1, 0) for piece in halves(cpl[level][...]))
        perm_buf, recv_c = m[N_PERM, level], m[N_COUPLE, level]
        idx = me % gp
        if level == 1 and by_slots:
            m[N_TAKE_KEY][...] = (dst * LANES + me % gp * wide + rank).astype(F32)
        if level == 2:
            m[N_HIT, 0][...] = hit16
            m[N_HIT, 1][...] = (si == pos + 4).astype(F32).astype(BF16)
        if rows_path(level):
            rank_c = jnp.sum(jnp.where(same & (ci < ri), 1.0, 0.0), axis=1, keepdims=True)
            first = (me % g * wide).astype(F32)
            lane = lax.broadcasted_iota(jnp.int32, (u, LANES), 1).astype(F32)
            place = (lane == rank_c + first).astype(F32).astype(BF16)
            low_f = low.astype(F32)
            if tucked(level):
                named = jnp.where(si == dst * wide + caps[level], low_f, 0.0).astype(BF16)
                moved = moved + once(named, place, 1, 0)
            else:
                qi = lax.broadcasted_iota(jnp.int32, (gp, u), 0)
                named = jnp.where(qi == dst, low_f, 0.0).astype(BF16)
                lows = once(named, place, 1, 0)
                lows_s, lows_r = m[N_LOW_S, level], m[N_LOW, level]
                for q in range(gp):
                    lows_s[q] = lows[q : q + 1, :]
                lows_r[idx] = lows_s[idx]
        else:
            shifted = (si == pos + 4).astype(F32)
            lowc = jnp.sum(shifted * low.astype(F32), axis=1, keepdims=True)
            moved = moved + jnp.broadcast_to(lowc, (slots, LANES))
        perm_buf[...] = moved.reshape(gp, wide, LANES)
        recv_c[idx] = perm_buf[idx]

    def send_couple(level):
        gp = size[level + 1]
        perm_buf, recv_c = m[N_PERM, level], m[N_COUPLE, level]
        if rows_path(level) and not tucked(level):
            lows_s, lows_r = m[N_LOW_S, level], m[N_LOW, level]
            send_each(lambda q: lows_s.at[q], lambda i: lows_r.at[i], gp, (N_LOW, level))
            pending.append((lows_s.at[pl.ds(0, gp - 1)], sem_of((N_LOW, level))))
        part = pl.ds(0, couple_rows(level))
        send_each(lambda q: perm_buf.at[q, part], lambda i: recv_c.at[i, part], gp, (N_COUPLE, level))
        pending.append((perm_buf.at[pl.ds(0, gp - 1), part], sem_of((N_COUPLE, level))))

    def ship_couple(level):
        make_couple(level)
        send_couple(level)

    def low_row(level, child):
        g = size[level]
        got = m[N_COUPLE, level] if tucked(level) else m[N_LOW, level]
        one = slice(caps[level], caps[level] + 1) if tucked(level) else slice(0, 1)
        return jnp.sum(got[child * g : (child + 1) * g, one, :], axis=0)[:, : g * wide_of(level)]

    def low_column(level, child):
        g = size[level]
        got = m[N_COUPLE, level][child * g : (child + 1) * g].reshape(g * wide_of(level), LANES)
        si = lax.broadcasted_iota(jnp.int32, (got.shape[0], 1), 0)
        up = jnp.concatenate([got[4:, :1], got[:4, :1]], axis=0)
        return jnp.where(si % 8 < 4, up, -1.0), jnp.where(si % 8 < 4, -1.0, got[:, :1])

    def build_gt(level):
        g = size[level]
        gp = size[level + 1]
        wide = wide_of(level)
        gt = m[N_GT, level]
        rows = gt.shape[1]
        if rows_path(level) and not tucked(level):
            arrive((N_LOW, level), gp)
        got_all = m[N_COUPLE, level]
        wait_for(
            got_all.at[pl.ds(0, gp - 1), pl.ds(0, couple_rows(level))],
            recv_sem.at[sem_of((N_COUPLE, level))],
        )
        slots = g * wide
        for child in range(gp // g):
            got = got_all[child * g : (child + 1) * g].reshape(slots, LANES)
            if rows_path(level):
                if tucked(level):
                    si = lax.broadcasted_iota(jnp.int32, (slots, LANES), 0)
                    got = jnp.where(si % wide < caps[level], got, 0.0)
                ri = lax.broadcasted_iota(jnp.int32, (rows, slots), 0).astype(F32)
                ot = (ri == low_row(level, child)).astype(F32).astype(BF16)
                full = sum(once(piece, ot, 0, 1) for piece in halves(got))
                if level == 1 and by_slots:
                    m[N_OT][:, child * slots : (child + 1) * slots] = ot.astype(F8)
            else:
                lane = lax.broadcasted_iota(jnp.int32, (slots, rows), 1).astype(F32)
                ot = (lane == low_column(level, child)[0]).astype(F32).astype(BF16)
                full = sum(once(piece, ot, 0, 0) for piece in halves(got))
            gt[child * RANK : (child + 1) * RANK, :] = full
            if level < 2:
                put_halves((N_GTH, level), 0, full, child * RANK)

    def reply_rows():
        g = size[2]
        wide = wide_of(2)
        slots = g * wide
        heads = halves(bas[3][:, :RANK])
        tails = halves(m[N_LAST, 3][...])
        for child in range(size[3] // g):
            if rows_path(2):
                low = low_row(2, child)
                lane = lax.broadcasted_iota(jnp.int32, (1, slots), 1) % wide
                one = jnp.where(lane < 4, low, -1.0)
                two = jnp.where(lane < 4, -1.0, pltpu.roll(low, 4, 1))
                iota, by = lax.broadcasted_iota(jnp.int32, (LANES, slots), 0), 0
            else:
                one, two = low_column(2, child)
                iota, by = lax.broadcasted_iota(jnp.int32, (slots, LANES), 1), 1
            iota = iota.astype(F32)
            first = (iota == one).astype(F32).astype(BF16)
            second = (iota == two).astype(F32).astype(BF16)
            rows = once(first, heads[0], by, 0) + once(first, heads[1], by, 0)
            rows = rows + (once(second, tails[0], by, 0) + once(second, tails[1], by, 0))
            m[N_ROWS_S][child * g : (child + 1) * g] = rows.reshape(g, wide, LANES)
        m[N_ROWS_R][me] = m[N_ROWS_S][me]
        send_each(lambda q: m[N_ROWS_S].at[q], lambda i: m[N_ROWS_R].at[i], size[3], N_ROWS_R)
        pending.append((m[N_ROWS_S].at[pl.ds(0, size[3] - 1)], sem_of(N_ROWS_R)))

    def build_named():
        arrive(N_ROWS_R, size[3])
        got = m[N_ROWS_R][...].reshape(size[3] * wide_of(2), LANES)
        pieces = halves(got)
        out = [
            once(pieces[0], m[N_HIT, i][...], 0, 0) + once(pieces[1], m[N_HIT, i][...], 0, 0)
            for i in range(2)
        ]
        put_halves(N_NAMED, 0, jnp.concatenate(out, axis=0))

    g_p = min(plane, 16)
    g_rp = RANK // g_p

    def g_holds(go):
        if plane == g_p:
            go()
        else:
            pl.when(spot < g_p)(go)

    def g_make():
        both = jnp.concatenate([bas[3][:, :RANK], m[N_LAST, 3][...]], axis=1)
        full = mult(m[N_GT, 2][...], both)
        n = full.shape[0] // RANK
        for j in range(g_p):
            m[N_G_P][j] = jnp.concatenate(
                [full[c * RANK + j * g_rp : c * RANK + (j + 1) * g_rp] for c in range(n)], axis=0
            )

    def g_scatter():
        sem = sem_of(N_G_RS)

        def body(k, carry):
            q = lax.rem(spot + k, g_p)

            def go():
                remote(m[N_G_P].at[q], m[N_G_RS].at[spot], sem, me - spot + q).start()

            if plane == g_p:
                go()
            else:
                pl.when(q != spot)(go)
            return carry

        lax.fori_loop(1 if plane == g_p else 0, g_p, body, 0)
        sent_rows.append((g_p - 1) * rows_in(m[N_G_P]) // g_p)

        def keep():
            m[N_G_RS][spot] = m[N_G_P][spot]

        g_holds(keep)

    def upper_of(q):
        return q * plane // size[2]

    def g_across():
        def go():
            arrive(N_G_RS, plane)
            total = jnp.sum(m[N_G_RS][...], axis=0)
            for c in range(total.shape[0] // g_rp):
                m[N_G_ZS][c] = total[c * g_rp : (c + 1) * g_rp]
            m[N_G_Z][layer] = m[N_G_ZS][upper_of(layer)]
            send_each(lambda q: m[N_G_ZS].at[upper_of(q)], lambda i: m[N_G_Z].at[i], planes, N_G_Z, plane)
            sent_rows.append((planes - 1) * rows_in(m[N_G_Z]) // planes)

        g_holds(go)

    def g_gather():
        def go():
            arrive(N_G_Z, planes)
            m[N_G][spot] = jnp.sum(m[N_G_Z][...], axis=0)
            send_each(lambda q: m[N_G].at[spot], lambda i: m[N_G].at[i], plane, N_G)
            sent_rows.append((plane - 1) * rows_in(m[N_G]) // g_p)

        g_holds(go)

    def g_arrive():
        sem = recv_sem.at[sem_of(N_G)]
        if plane == g_p:
            wait_for(m[N_G].at[pl.ds(0, g_p - 1)], sem)
        else:
            pl.when(spot < g_p)(lambda: wait_for(m[N_G].at[pl.ds(0, g_p - 1)], sem))
            pl.when(spot >= g_p)(lambda: wait_for(m[N_G].at[pl.ds(0, g_p)], sem))
        hi, lo = halves(m[N_G][...].reshape(RANK, 2 * RANK))
        m[N_GH, 0][...] = hi
        m[N_GH, 1][...] = lo

    def g_drain():
        if plane == g_p:
            wait_for(m[N_G_P].at[pl.ds(0, g_p - 1)], send_sem.at[sem_of(N_G_RS)])
        else:
            pl.when(spot < g_p)(lambda: wait_for(m[N_G_P].at[pl.ds(0, g_p - 1)], send_sem.at[sem_of(N_G_RS)]))
            pl.when(spot >= g_p)(lambda: wait_for(m[N_G_P], send_sem.at[sem_of(N_G_RS)]))

        def go():
            wait_for(m[N_G_Z].at[pl.ds(0, planes - 1)], send_sem.at[sem_of(N_G_Z)])
            n = plane - 1
            while n > 0:
                wait_for(m[N_G].at[pl.ds(0, min(n, g_p))], send_sem.at[sem_of(N_G)])
                n -= g_p

        g_holds(go)

    def prepare_back(level):
        z = m[N_Z, level][...]
        heads = bas[level][:, :RANK]
        own = mask(N_OWN, level, 0)
        xz = outer(z, blk[level][...]) + outer(shared(level) * own, heads)
        yt = m[N_LAST, level][...]
        if level > 0:
            sep = m[N_GT, level - 1][:, :LANES]
            xz = jnp.concatenate([xz, outer(xz, sep)], axis=1)
            yt = jnp.concatenate([yt, mult(sep, yt)], axis=0)
        m[N_XZ, level][...] = xz
        put_halves((N_BACK, level), 0, yt)

    def arrive_cross(level):
        g = group_of(level)
        p = parts_of[level]
        n = spread_of(level) // g * p
        sem = recv_sem.at[sem_of((N_CROSS, level))]
        buf = m[N_CROSS, level]
        if g == p:
            wait_for(buf.at[pl.ds(0, n - 1)], sem)
        else:
            idx = me % g
            pl.when(idx < p)(lambda: wait_for(buf.at[pl.ds(0, n - 1)], sem))
            pl.when(idx >= p)(lambda: wait_for(buf.at[pl.ds(0, n)], sem))

    def build_bot_middle():
        gp = size[2]
        place = me % gp
        rows = 2 * LANES
        ri = lax.broadcasted_iota(jnp.int32, (rows, LANES), 0)
        arrive(N_TGT_MIDDLE, gp)
        mine = jnp.where(ri < LANES, place * LANES + ri, (gp + place - 1) * LANES + ri).astype(F32)

        def fill(j, carry):
            t = m[N_TGT_MIDDLE][j]
            lanes = pl.ds(pl.multiple_of(j * LANES, LANES), LANES)
            m[N_BOT_MIDDLE][:, lanes] = (mine == t).astype(F32).astype(F8)
            return carry

        lax.fori_loop(0, gp, fill, 0)

    def build_bot_upper():
        rows = planes * LANES
        ri = lax.broadcasted_iota(jnp.int32, (rows, LANES), 0)
        arrive(N_TGT_UPPER, plane)
        mine = ((ri // LANES * plane + spot) * LANES + ri % LANES).astype(F32)

        def fill(j, carry):
            t = m[N_TGT_UPPER][j]
            lanes = pl.ds(pl.multiple_of(j * LANES, LANES), LANES)
            m[N_BOT_UPPER][:, lanes] = (mine == t).astype(F32).astype(F8)
            return carry

        lax.fori_loop(0, plane, fill, 0)

    def build_take():
        key = m[N_TAKE_KEY][...]
        ri = lax.broadcasted_iota(jnp.int32, (LANES, LANES), 0)

        def fill(j, carry):
            rows = pl.ds(pl.multiple_of(j * LANES, LANES), LANES)
            m[N_TAKE][rows, :] = ((ri + j * LANES).astype(F32) == key).astype(F32).astype(F8)
            return carry

        lax.fori_loop(0, size[2], fill, 0)

    def build_ft_middle():
        t = tgt[1][...]
        ri = lax.broadcasted_iota(jnp.int32, (LANES, LANES), 0)

        def fill(j, carry):
            rows = pl.ds(pl.multiple_of(j * LANES, LANES), LANES)
            m[N_FT_MIDDLE][rows, :] = (ri + j * LANES == t).astype(F32).astype(F8)
            return carry

        lax.fori_loop(0, m[N_FT_MIDDLE].shape[0] // LANES, fill, 0)

    def build_ft_upper():
        arrive(N_TGT_LAYER, planes)
        t = jnp.concatenate([m[N_TGT_LAYER][j] for j in range(planes)], axis=1)
        ri = lax.broadcasted_iota(jnp.int32, (LANES, planes * LANES), 0)

        def fill(j, carry):
            rows = pl.ds(pl.multiple_of(j * LANES, LANES), LANES)
            here = ((ri + (layer * plane + j) * LANES).astype(F32) == t).astype(F32)
            m[N_FT_UPPER][rows, :] = here.astype(F8)
            return carry

        lax.fori_loop(0, plane, fill, 0)

    def share(level, zp):
        m[N_ZP, level][me % size[level]] = zp
        send_all((N_ZP, level), size[level])

    def shared(level):
        arrive((N_ZP, level), size[level])
        return jnp.sum(m[N_ZP, level][...], axis=0)

    def make_cross(level):
        need((N_EXP, level), (N_BAS, level))
        m[N_CROSS_P, level][...] = inner(exp[level][...], bas[level][:, RANK:])

    def start_cross(level):
        make_cross(level)
        scatter_cross(level)

    need((N_SRC, 0), (N_BAS, 0))
    m[N_F0][me % size[0]] = mult(src[0][...], bas[0][:, :RANK])
    make_cross(1)
    pl.semaphore_wait(barrier, plane - 1 + layer * plane)
    send_all(N_F0, size[0])
    scatter_cross(1)
    lax.fori_loop(0, layer, greet_back, 0)
    ship_couple(0)
    need((N_BLK, 0), (N_EXP, 0), (N_PIV, 0))
    local = mult(src[0][...], blk[0][...])
    fill_masks(0)
    build_forward(1)
    make_cross(2)
    pl.when(layer < planes - 1)(lambda: pl.semaphore_wait(up_sem, planes - 1 - layer))
    scatter_cross(2)
    arrive(N_F0, size[0])
    hq = jnp.sum(m[N_F0][...], axis=0) * mask(N_OWN, 0, 0)
    y = local + outer(hq, exp[0][...])
    m[N_F1][spot] = mult(y, bas[0][:, RANK:])
    send_all(N_F1, plane)
    m[N_Z, 0][...] = y * piv[0][...]
    fill_masks(1)
    gather_cross(1)
    need((N_TGT, 1), (N_TGT, 2))
    m[N_TGT_MIDDLE][me % size[2]] = tgt[1][...].astype(F32)
    send_all(N_TGT_MIDDLE, size[2])
    mine_t = tgt[2][...].astype(F32)
    m[N_TGT_UPPER][spot] = mine_t
    send_all(N_TGT_UPPER, plane)
    m[N_TGT_LAYER][layer] = mine_t
    send_all(N_TGT_LAYER, planes, plane)
    ship_couple(1)
    ship_couple(2)
    gather_cross(2)
    build_gt(0)
    add_cross(1)

    for level in range(3):
        g = size[level]
        gp = size[level + 1]
        nch = gp // g
        child_me = me % gp // g
        need((N_SRC, level + 1))
        name = (N_F1, N_F2, N_F3B)[level]
        buf, step = m[name], g
        if level == 2:
            step = g // plane
        arrive(name, gp if level < 2 else planes)
        ws = [
            jnp.sum(buf[child * step : (child + 1) * step, :count, :], axis=0) * mask(N_KID, level, child, 1)
            for child in range(nch)
        ]
        ws = jnp.concatenate(ws, axis=1)
        bn = src[level + 1][...]
        upd = 0.0
        if level == 0:
            inc = by_halves(ws, (N_GTH, 0), 0)
            bn = bn - inc[:, :LANES]
            upd = -inc[:, LANES:]
        elif level == 1:
            rows = jnp.concatenate([buf[j, count : 2 * count, :] for j in range(gp)], axis=1)
            inc = select(rows, m[N_BOT_MIDDLE][...], 1)
            bn = jnp.concatenate([bn + inc[:, :LANES], ws], axis=1)
            upd = inc[:, LANES:] - by_halves(ws, (N_GTH, 1), 0, slice(LANES, 2 * LANES))
        else:
            bn = jnp.concatenate([bn + jnp.sum(buf[:, count : 2 * count, :], axis=0), ws], axis=1)
        local_n, bq, *sent = local_forward(level + 1, bn)
        if level < 2:
            sent.append(upd)
        else:
            sent = [bq] + sent[:1] + sent[2:] + sent[1:2]
        name = (N_F2, N_F3A, N_F4A)[level]
        group = size[2] if level == 0 else plane
        m[name][me % group] = jnp.concatenate(sent, axis=0)
        send_all(name, group)
        if level < 2:
            m[N_HQ, level + 1][me % gp] = bq
            send_all((N_HQ, level + 1), gp)
        if level == 1:
            g_scatter()
        if level == 2:
            g_across()
        if level > 0:
            arrive((N_HQ, level), g)
            hq = jnp.sum(m[N_HQ, level][...], axis=0) * mask(N_OWN, level, 0)
            z = (local + outer(hq, exp[level][...])) * piv[level][...]
            m[N_Z, level][...] = z
            share(level, mult(z, exp[level][...]))
        local = local_n
        if level == 0:
            build_forward(2)
            fill_masks(2)
            build_forward(3)
            scatter_cross(3)
            build_gt(1)
            build_bot_middle()
            add_cross(2)
            chain_forward(2)
            build_gt(2)
            g_make()
        elif level == 1:
            reply_rows()
            build_bot_upper()
            fill_masks(3)
            arrive(N_F3A, plane)
            sums = jnp.sum(m[N_F3A][:, :count, :], axis=0)
            rows = jnp.concatenate([m[N_F3A][j, count:, :] for j in range(plane)], axis=1)
            part = select(rows, m[N_BOT_UPPER][...], 1)
            for q in range(planes):
                m[N_F3S][q] = jnp.concatenate([sums, part[:, q * LANES : (q + 1) * LANES]], axis=0)
            m[N_F3B][layer] = m[N_F3S][layer]
            send_each(lambda q: m[N_F3S].at[q], lambda i: m[N_F3B].at[i], planes, N_F3B, plane)
            pending.append((m[N_F3S].at[pl.ds(0, planes - 1)], sem_of(N_F3B)))
            put_halves((N_FWD, 3), 4 * RANK, outer(m[N_NEAR][...], m[N_GT, 2][...]))
            chain_forward(3)
            share(0, mult(m[N_Z, 0][...], exp[0][...]))
            start_cross(0)
            m[N_LAST, 0][...] = mult(blk[0][...], bas[0][:, RANK:])
            build_ft_upper()
            if by_slots:
                build_take()
            cross_planes()
    gather_cross(3)
    gather_cross(0)
    g_gather()
    arrive(N_F4A, plane)
    o = (2 + size[3] // size[2]) * count
    sums = jnp.sum(m[N_F4A][:, :o, :], axis=0)
    rows = jnp.concatenate([m[N_F4A][j, o:, :] for j in range(plane)], axis=1)
    part = select(rows, m[N_FT_UPPER][...], 0)
    for q in range(planes):
        c = 2 + q * plane // size[2]
        m[N_F4S][q] = jnp.concatenate(
            [sums[: 2 * count], sums[c * count : (c + 1) * count], part[:, q * LANES : (q + 1) * LANES]], axis=0
        )
    m[N_F4B][layer] = m[N_F4S][layer]
    send_each(lambda q: m[N_F4S].at[q], lambda i: m[N_F4B].at[i], planes, N_F4B, plane)
    pending.append((m[N_F4S].at[pl.ds(0, planes - 1)], sem_of(N_F4B)))
    build_named()
    prepare_back(2)
    arrive_cross(3)
    arrive(N_F4B, planes)
    g_arrive()
    both = jnp.sum(m[N_F4B][...], axis=0)
    hq = both[:count] * mask(N_OWN, 3, 0)
    rp = (both[count : 2 * count] + mult(hq, m[N_CROSS, 3][...].reshape(RANK, RANK))) * mask(N_OWN, 3, 0)
    pair = jnp.concatenate([rp, hq], axis=1)
    s = both[2 * count : 3 * count] + by_halves(pair, N_GH, 1)
    xu = both[3 * count :] + by_halves(pair, N_NAMED, 0)

    for level in (2, 1, 0):
        s = s * mask(N_OWN, level, 1)
        xs = m[N_XZ, level][...] - by_halves(s, (N_BACK, level), 1)
        x = xs[:, :LANES]
        if level == 0:
            outs[0][...] = x
            break
        g = size[level - 1]
        gp = size[level]
        nch = gp // g
        place = me % gp
        child_me = place // g
        sp = xs[:, LANES:] + by_halves(xu, (N_GTH, level - 1), 1, slice(LANES, 2 * LANES))
        name = (N_B3, N_B2)[level - 1]
        buf, piece = m[name], m[N_PIECE, level - 1]
        for c in range(nch):
            rest = []
            if level == 2 and by_slots:
                rest = [select(jnp.concatenate([x, xu], axis=1), m[N_OT][...], 0)]
            elif level == 2:
                rest = [x, xu]
            piece[c] = jnp.concatenate([sp[:, c * RANK : (c + 1) * RANK]] + rest, axis=0)
        buf[place] = piece[child_me]
        send_each(lambda q: piece.at[lax.div(q, g)], lambda i: buf.at[i], gp, name)
        pending.append((buf.at[pl.ds(0, gp - 1)], sem_of(name)))
        outs[level][...] = x
        if level == 2:
            z = (local + outer(hq, exp[3][...])) * piv[3][...]
            outs[3][...] = outer(z, blk[3][...]) + outer(rp, bas[3][:, :RANK])
        else:
            add_cross(0)
        prepare_back(level - 1)
        arrive(name, gp)
        s = jnp.sum(buf[:, :count, :], axis=0)
        if level == 2:
            blocks = [buf[j, count : 2 * count, :] for j in range(gp)]
            if not by_slots:
                blocks += [buf[j, 2 * count :, :] for j in range(gp)]
                build_ft_middle()
            xu = select(jnp.concatenate(blocks, axis=1), m[N_TAKE if by_slots else N_FT_MIDDLE][...], 0)

    if shared_sends:
        assert all(group_of(level) == parts_of[level] for level in range(4))
        wait_rows(sum(sent_rows) + sum(rows_in(part) for part, _ in pending), send_sem.at[0])
    else:
        for part, sem in pending:
            wait_for(part, send_sem.at[sem])
        for level in range(4):
            g = group_of(level)
            p = parts_of[level]
            rp = RANK // p
            gp = spread_of(level)
            n = gp // g * p
            idx = me % g
            rs_sem = send_sem.at[sem_of((N_RS, level))]
            ag_sem = send_sem.at[sem_of((N_CROSS, level))]
            cross_p, buf = m[N_CROSS_P, level], m[N_CROSS, level]

            def ag_done():
                for _ in range((gp - 1) // n):
                    wait_for(buf.at[pl.ds(0, n)], ag_sem)
                if (gp - 1) % n:
                    wait_for(buf.at[pl.ds(0, (gp - 1) % n)], ag_sem)
                if level == 3:
                    wait_for(m[N_GRAM].at[pl.ds(0, planes - 1)], send_sem.at[sem_of(N_GRAM)])

            if g == p:
                wait_for(cross_p.at[pl.ds(0, (p - 1) * rp)], rs_sem)
                ag_done()
            else:
                pl.when(idx < p)(lambda: wait_for(cross_p.at[pl.ds(0, (p - 1) * rp)], rs_sem))
                pl.when(idx >= p)(lambda: wait_for(cross_p, rs_sem))
                pl.when(idx < p)(ag_done)
        g_drain()


def put_out(*refs):
    n = len(refs) // 2
    ins, outs, sem = refs[:n], refs[n : 2 * n], refs[-1]
    copies = [pltpu.make_async_copy(ins[i], outs[i], sem.at[i]) for i in range(n)]
    for c in copies:
        c.start()
    for c in copies:
        c.wait()


def solution(mesh):
    leaves, across = mesh.shape["leaf"], mesh.shape["grid"]

    def shards(*args):
        levels = [args[8 * i : 8 * i + 8] for i in range(3)]
        root = args[24:30]
        (sl, bl, el, qs, pv, cl, rk, tg) = zip(*levels)
        src = list(sl) + [root[0]]
        blk = list(bl) + [root[1]]
        exp = list(el) + [root[2]]
        bas = list(qs) + [root[3]]
        piv = [v.reshape(1, -1) for v in list(pv) + [root[4]]]
        rnk = list(rk) + [root[5]]
        tgt = [t.reshape(1, -1) for t in tg]
        count = src[0].shape[0]
        ups = [t.shape[1] for t in tgt]
        fronts = [r.shape[0] for r in rnk]
        rnk = [r.T if r.shape[0] > 2 else r for r in rnk]
        size = [leaves * across // f for f in fronts]
        for v in src:
            assert v.shape[1] == LANES
        vm = lambda *s: pltpu.VMEM(s, F32)
        bits = lambda *s: pltpu.VMEM(s, BF16)
        ones = lambda *s: pltpu.VMEM(s, F8)
        total = leaves * across
        plane = size[1]
        planes = total // plane
        nch = [size[i + 1] // size[i] for i in range(3)]
        caps = [max(1, -(-ups[i] // size[i + 1])) for i in range(3)]
        group = size[:3] + [plane]
        spread = group
        parts = [min(g, 16) for g in group]
        by_slots = size[2] * max(8, -(-caps[1] // 8) * 8) <= LANES
        bufs = {
            N_F0: vm(size[0], count, LANES),
            N_F1: vm(plane, count, LANES),
            N_F2: vm(size[2], 2 * count, LANES),
            N_F3A: vm(plane, 2 * count, LANES),
            N_F3S: vm(planes, 2 * count, LANES),
            N_F3B: vm(planes, 2 * count, LANES),
            (N_HQ, 1): vm(size[1], count, LANES),
            (N_HQ, 2): vm(size[2], count, LANES),
            N_F4A: vm(plane, (nch[2] + 3) * count, LANES),
            N_F4S: vm(planes, 4 * count, LANES),
            N_F4B: vm(planes, 4 * count, LANES),
            N_NEAR: vm(LANES, LANES),
            N_RULER: vm(8192 if total <= 64 else 1024, LANES),
            (N_HIT, 0): bits(total * 8, LANES),
            (N_HIT, 1): bits(total * 8, LANES),
            N_ROWS_S: vm(total, 8, LANES),
            N_ROWS_R: vm(total, 8, LANES),
            (N_NAMED, 0): bits(2 * RANK, LANES),
            (N_NAMED, 1): bits(2 * RANK, LANES),
            (N_GH, 0): bits(RANK, 2 * RANK),
            (N_GH, 1): bits(RANK, 2 * RANK),
            N_G_P: vm(parts[3], nch[2] * RANK // parts[3], 2 * RANK),
            N_G_RS: vm(plane, nch[2] * RANK // parts[3], 2 * RANK),
            N_G_ZS: vm(nch[2], RANK // parts[3], 2 * RANK),
            N_G_Z: vm(planes, RANK // parts[3], 2 * RANK),
            N_G: vm(parts[3], RANK // parts[3], 2 * RANK),
            N_B2: vm(size[2], (2 if by_slots else 3) * count, LANES),
            N_B3: vm(size[1], count, LANES),
            N_TGT_MIDDLE: vm(size[2], 1, LANES),
            N_TGT_UPPER: vm(plane, 1, LANES),
            N_TGT_LAYER: vm(planes, 1, LANES),
            N_BOT_MIDDLE: ones(2 * LANES, size[2] * LANES),
            N_BOT_UPPER: ones(planes * LANES, plane * LANES),
            N_FT_UPPER: ones(plane * LANES, planes * LANES),
            N_MASK: vm(6 + 2 * sum(nch), count, LANES),
            N_GRAM: vm(planes, RANK // parts[3], RANK),
        }
        arrays = {N_SRC: src, N_BLK: blk, N_EXP: exp, N_BAS: bas, N_PIV: piv, N_RNK: rnk, N_CPL: cl, N_TGT: tgt}
        for name, list_of in arrays.items():
            for i, v in enumerate(list_of):
                bufs[name, i] = pltpu.VMEM(v.shape, v.dtype)
        for i in range(4):
            bufs[N_LAST, i] = vm(LANES, RANK)
            for j in range(2):
                if i > 0:
                    bufs[(N_FWD, i), j] = bits(LANES + (nch[i - 1] * RANK if i > 1 else 0), (3 if i < 3 else 4 + nch[2]) * RANK)
                if i < 3:
                    bufs[(N_BACK, i), j] = bits((1 + (nch[i - 1] if i > 0 else 0)) * RANK, RANK)
        if by_slots:
            bufs[N_TAKE_KEY] = vm(1, LANES)
            bufs[N_TAKE] = ones(size[2] * LANES, LANES)
            bufs[N_OT] = ones(2 * LANES, LANES)
        else:
            bufs[N_FT_MIDDLE] = ones(size[2] * 2 * LANES, LANES)
        for i in range(2):
            for j in range(2):
                bufs[(N_GTH, i), j] = bits(nch[i] * RANK, 2 * LANES)
        for i in range(3):
            bufs[N_Z, i] = vm(count, LANES)
            bufs[N_XZ, i] = vm(count, (1 + (nch[i - 1] if i > 0 else 0)) * LANES)
        for i in range(4):
            bufs[N_CROSS_P, i] = vm(RANK, RANK)
            bufs[N_RS, i] = vm(group[i], RANK // parts[i], RANK)
            bufs[N_CROSS, i] = vm(spread[i] // group[i] * parts[i], RANK // parts[i], RANK)
        for i in range(3):
            wide = max(8, -(-caps[i] // 8) * 8)
            assert caps[i] <= 4 or size[i] * wide <= LANES
            if caps[i] == wide:
                bufs[N_LOW_S, i] = vm(size[i + 1], 1, LANES)
                bufs[N_LOW, i] = vm(size[i + 1], 1, LANES)
            bufs[N_PERM, i] = vm(size[i + 1], wide, LANES)
            bufs[N_COUPLE, i] = vm(size[i + 1], wide, LANES)
            bufs[N_GT, i] = vm(nch[i] * RANK, LANES * (1 if i == 2 else 2))
            bufs[N_ZP, i] = vm(size[i], count, LANES)
            bufs[N_PIECE, i] = vm(nch[i], (1 if i == 0 else 2 if by_slots else 3) * count, LANES)
        scratch = list(bufs.values())
        scratch += [pltpu.SemaphoreType.DMA((n,)) for n in (1 if total <= 64 else 37, 37, 11)]
        scratch += [pltpu.SemaphoreType.REGULAR]
        vspec = pl.BlockSpec(memory_space=pltpu.VMEM)
        aspec = pl.BlockSpec(memory_space=pl.ANY)
        answers = pl.pallas_call(
            functools.partial(kernel, (leaves, across, size, ups, count, caps, fronts), list(bufs)),
            out_shape=[pltpu.VMEM(v.shape, F32) for v in src],
            in_specs=[aspec] * 30,
            out_specs=[vspec] * 4,
            scratch_shapes=scratch,
            compiler_params=pltpu.CompilerParams(
                collective_id=0, has_side_effects=True, vmem_limit_bytes=63 * 1024 * 1024
            ),
        )(*src, *blk, *exp, *bas, *piv, *rnk, *cl, *tgt)
        return pl.pallas_call(
            put_out,
            out_shape=[jax.ShapeDtypeStruct(v.shape, F32) for v in src],
            in_specs=[vspec] * 4,
            out_specs=[aspec] * 4,
            scratch_shapes=[pltpu.SemaphoreType.DMA((4,))],
        )(*[pltpu.with_memory_space_constraint(v, pltpu.VMEM) for v in answers])

    spread_axes = ("leaf", "grid")
    level = (P(None, spread_axes), P(spread_axes, None), P(spread_axes, None), P(spread_axes, None), P(spread_axes))
    mid = level + (P(spread_axes, None), P(), P(spread_axes))
    return jax.shard_map(
        shards,
        mesh=mesh,
        in_specs=mid * 3 + level + (P(),),
        out_specs=(P(None, spread_axes),) * 4,
        check_vma=False,
    )
```

```python
import functools
import math

import jax
import jax.numpy as jnp
from jax import lax
from jax.experimental import pallas as pl
from jax.experimental.pallas import tpu as pltpu
from jax.sharding import PartitionSpec as P

RANK = 128
LANES = 128
MESH = pl.DeviceIdType.MESH
NSEM = 36
F32 = jnp.float32
BF16 = jnp.bfloat16
F8 = jnp.float8_e4m3fn

(
    N_SRC, N_BLK, N_EXP, N_BAS, N_PIV, N_RNK, N_CPL, N_TGT, N_RULER, N_COUPLE, N_MASK, N_OWN, N_KID,
    N_CROSS_P, N_LAST, N_NEAR, N_FWD, N_GT, N_CROSS, N_RS, N_GRAM, N_PERM, N_TAKE_KEY, N_HIT, N_LOW_S, N_LOW,
    N_OT, N_GTH, N_ROWS_S, N_ROWS_R, N_NAMED, N_G_P, N_G_RS, N_G_ZS, N_G_Z, N_G, N_GH, N_Z, N_XZ, N_BACK,
    N_TGT_MIDDLE, N_BOT_MIDDLE, N_TGT_UPPER, N_BOT_UPPER, N_TAKE, N_FT_MIDDLE, N_TGT_LAYER, N_FT_UPPER, N_ZP,
    N_F0, N_F1, N_F2, N_F3B, N_F2U, N_F3A, N_F4A, N_HQ, N_F3S, N_F4S, N_F4B, N_B3, N_B2, N_PIECE,
) = range(63)


def once(a, b, ca, cb):
    return lax.dot_general(a, b, (((ca,), (cb,)), ((), ())), preferred_element_type=F32)


def halves(x):
    hi = x.astype(BF16)
    return hi, (x - hi.astype(F32)).astype(BF16)


def dot(a, b, ca, cb):
    ah, al = halves(a)
    bh, bl = halves(b)
    if ca == 0:
        return once(ah, bh, ca, cb) + (once(al, bh, ca, cb) + once(ah, bl, ca, cb))
    n = a.shape[0]
    both = once(jnp.concatenate([ah.astype(F32), al.astype(F32)], axis=0).astype(BF16), bh, ca, cb)
    return both[:n] + (both[n:] + once(ah, bl, ca, cb))


def mult(a, b):
    return dot(a, b, 1, 0)


def outer(a, b):
    return dot(a, b, 1, 1)


def inner(a, b):
    return dot(a, b, 0, 0)


def select(x, onehot, cb):
    hi = x.astype(BF16).astype(F32)
    out = once(jnp.concatenate([hi, x - hi], axis=0).astype(BF16), onehot, 1, cb)
    n = x.shape[0]
    return out[:n] + out[n:]


KINDS = (N_SRC, N_BLK, N_EXP, N_BAS, N_PIV, N_RNK)


def kernel(cfg, names, *refs):
    leaves, across, size, ups, count, caps, fronts = cfg
    total_devices = leaves * across
    hbm = [refs[4 * i : 4 * i + 4] for i in range(6)]
    cpl_in = refs[24:27]
    tgt_in = refs[27:30]
    outs = refs[30:34]
    m = dict(zip(names, refs[34:-4]))
    send_sem, recv_sem, load_sem, up_sem = refs[-4:]
    sems = {}
    src, blk, exp, bas, piv, rnk = [[m[k, i] for i in range(4)] for k in KINDS]
    cpl = [m[N_CPL, i] for i in range(3)]
    tgt = [m[N_TGT, i] for i in range(3)]

    me = lax.axis_index("leaf") * across + lax.axis_index("grid")
    plane = size[1]
    planes = total_devices // plane
    spot = me % plane
    layer = me // plane
    pending = []

    shared_sends = total_devices <= 64
    sent_rows = []
    loaded = set()
    order = [[(N_SRC, 0), (N_BAS, 0)], [(N_EXP, 1), (N_BAS, 1)]]
    order += [[(N_CPL, 0), (N_TGT, 0)], [(N_BLK, 0), (N_EXP, 0), (N_PIV, 0)]]
    order += [[(N_RNK, i)] for i in range(4)]
    order += [[(N_BLK, 1), (N_SRC, 1), (N_PIV, 1), (N_CPL, 1), (N_TGT, 1), (N_TGT, 2), (N_CPL, 2)]]
    order += [[(k, i) for k in (N_EXP, N_BAS, N_BLK, N_SRC, N_PIV)] for i in (2, 3)]
    where_from = {(k, i): hbm[j][i] for j, k in enumerate(KINDS) for i in range(4)}
    for i in range(3):
        where_from[N_CPL, i] = cpl_in[i]
        where_from[N_TGT, i] = tgt_in[i]

    def load(some):
        for keys in some:
            for key in keys:
                pltpu.make_async_copy(where_from[key], m[key], load_sem.at[order.index(keys)]).start()

    def rows_in(ref):
        return math.prod(ref.shape) // LANES

    def wait_rows(rows, sem):
        wait_for(m[N_RULER].at[pl.ds(0, rows)], sem)

    def need(*wanted):
        for i, keys in enumerate(order):
            if any(key in keys for key in wanted) and i not in loaded:
                loaded.add(i)
                if len(keys) == 1:
                    wait_for(m[keys[0]], load_sem.at[i])
                else:
                    wait_rows(sum(rows_in(m[key]) for key in keys), load_sem.at[i])

    def where(peer):
        return (lax.div(peer, across), lax.rem(peer, across))

    def sem_of(name):
        return sems.setdefault(name, len(sems))

    def remote(a, b, sem, peer):
        return pltpu.make_async_remote_copy(
            src_ref=a,
            dst_ref=b,
            send_sem=send_sem.at[0 if shared_sends else sem],
            recv_sem=recv_sem.at[sem],
            device_id=where(peer),
            device_id_type=MESH,
        )

    def wait_for(part, sem):
        pltpu.make_async_copy(part, part, sem).wait()

    def send_each(source, dest, group, name, stride=1):
        idx = me // stride % group
        base = me - idx * stride
        sem = sem_of(name)

        def body(k, carry):
            q = lax.rem(idx + k, group)
            remote(source(q), dest(idx), sem, base + q * stride).start()
            return carry

        lax.fori_loop(1, group, body, 0)

    def send_all(name, group, stride=1):
        buf = m[name]
        idx = me // stride % group
        send_each(lambda q: buf.at[idx], lambda i: buf.at[i], group, name, stride)
        pending.append((buf.at[pl.ds(0, group - 1)], sem_of(name)))

    def arrive(name, group):
        wait_for(m[name].at[pl.ds(0, group - 1)], recv_sem.at[sem_of(name)])

    load(order[:3])
    m[N_COUPLE, 2][...] = jnp.zeros(m[N_COUPLE, 2].shape, F32)
    barrier = pltpu.get_barrier_semaphore()

    def greet_near(k, carry):
        peer = me - spot + lax.rem(spot + k, plane)
        pl.semaphore_signal(barrier, inc=1, device_id=where(peer), device_id_type=MESH)
        return carry

    def greet_far(peer, carry):
        pl.semaphore_signal(barrier, inc=1, device_id=where(peer), device_id_type=MESH)
        return carry

    def greet_back(k, carry):
        pl.semaphore_signal(up_sem, inc=1, device_id=where(k * plane + spot), device_id_type=MESH)
        return carry

    lax.fori_loop(1, plane, greet_near, 0)
    lax.fori_loop((layer + 1) * plane, total_devices, greet_far, 0)
    load(order[3:])

    col = lax.broadcasted_iota(jnp.int32, (count, RANK), 1).astype(F32)
    mask_slots = {}

    def fill_mask(name, level, front, which):
        ranks = rnk[level][...].astype(F32)
        if ranks.shape[0] == 2 and fronts[level] > 2:
            lane = lax.broadcasted_iota(jnp.int32, ranks.shape, 1)
            row = lax.broadcasted_iota(jnp.int32, ranks.shape, 0)
            hit = (lane == front) & (row == which)
        else:
            lane = lax.broadcasted_iota(jnp.int32, ranks.shape, 1)
            row = lax.broadcasted_iota(jnp.int32, ranks.shape, 0)
            hit = (lane == which) & (row == front)
        r = jnp.sum(jnp.where(hit, ranks, 0.0), axis=1, keepdims=True)
        r = jnp.sum(r, axis=0, keepdims=True)
        slot = mask_slots.setdefault(name, len(mask_slots))
        m[N_MASK][slot] = (col < r).astype(F32)

    def mask(*name):
        return m[N_MASK][mask_slots[name]]

    def fill_masks(level):
        need((N_RNK, level))
        fill_mask((N_OWN, level, 0), level, me // size[level], 0)
        if level == 3:
            return
        fill_mask((N_OWN, level, 1), level, me // size[level], 1)
        nch = size[level + 1] // size[level]
        for child in range(nch):
            front = me // size[level + 1] * nch + child
            fill_mask((N_KID, level, child, 1), level, front, 1)

    def build_forward(level):
        need((N_BLK, level), (N_BAS, level), (N_PIV, level), (N_EXP, level))
        parts = [blk[level][...], bas[level][:, :RANK]]
        if level == 3:
            pt = exp[3][...].T * piv[3][...]
            m[N_CROSS_P, 3][...] = mult(pt, exp[3][...])
            m[N_LAST, 3][...] = outer(blk[3][...], pt)
            m[N_NEAR][...] = outer(blk[3][...] * piv[3][...], blk[3][...])
            parts += [m[N_LAST, 3][...], m[N_NEAR][...]]
        else:
            m[N_LAST, level][...] = mult(blk[level][...], bas[level][:, RANK:])
            parts += [m[N_LAST, level][...]]
        put_halves((N_FWD, level), 0, jnp.concatenate(parts, axis=1))

    def put_halves(name, start, value, first=0):
        hi, lo = halves(value)
        lanes = slice(start, start + value.shape[1])
        rows = slice(first, first + value.shape[0])
        m[name, 0][rows, lanes] = hi
        m[name, 1][rows, lanes] = lo

    def chain_forward(level):
        top = m[(N_FWD, level), 0][:LANES].astype(F32) + m[(N_FWD, level), 1][:LANES].astype(F32)
        put_halves((N_FWD, level), 0, -mult(m[N_GT, level - 1][:, :LANES], top), LANES)

    def add_cross(level):
        if level == 0:
            arrive_cross(0)
        heads = bas[level][:, :RANK] * mask(N_OWN, level, 0)[:1]
        yt = m[N_LAST, level][...] + mult(heads, m[N_CROSS, level][...].reshape(RANK, RANK))
        m[N_LAST, level][...] = yt

    def by_halves(a, name, cb, lanes=slice(None)):
        ah, al = halves(a)
        n = a.shape[0]
        wh = m[name, 0][:, lanes]
        two = once(jnp.concatenate([ah.astype(F32), al.astype(F32)], axis=0).astype(BF16), wh, 1, cb)
        return two[:n] + (two[n:] + once(ah, m[name, 1][:, lanes], 1, cb))

    def local_forward(level, b):
        out = by_halves(b, (N_FWD, level), 0)
        return [out[:, i : i + RANK] for i in range(0, out.shape[1], RANK)]

    def group_of(level):
        return size[level] if level < 3 else plane

    parts_of = [min(group_of(level), 16) for level in range(4)]

    def scatter_cross(level):
        g = group_of(level)
        p = parts_of[level]
        rp = RANK // p
        idx = me % g
        base = me - idx
        sem = sem_of((N_RS, level))
        cross_p, rs_buf = m[N_CROSS_P, level], m[N_RS, level]

        def body(k, carry):
            q = lax.rem(idx + k, p)

            def go():
                rows = pl.ds(pl.multiple_of(q * rp, 8), rp)
                remote(cross_p.at[rows], rs_buf.at[idx], sem, base + q).start()

            if g == p:
                go()
            else:
                pl.when(q != idx)(go)
            return carry

        lax.fori_loop(1 if g == p else 0, p, body, 0)
        sent_rows.append((p - 1) * rp)

        def keep():
            rows = pl.ds(pl.multiple_of(idx * rp, 8), rp)
            rs_buf[idx] = cross_p[rows, :]

        if g == p:
            keep()
        else:
            pl.when(idx < p)(keep)

    def spread_of(level):
        return group_of(level)

    def holds_part(level, go):
        if group_of(level) == parts_of[level]:
            go()
        else:
            pl.when(me % group_of(level) < parts_of[level])(go)

    def sum_parts(level):
        g = group_of(level)
        wait_for(m[N_RS, level].at[pl.ds(0, g - 1)], recv_sem.at[sem_of((N_RS, level))])
        return jnp.sum(m[N_RS, level][...], axis=0)

    def cross_planes():
        buf = m[N_GRAM]

        def go():
            buf[layer] = sum_parts(3)
            send_each(lambda q: buf.at[layer], lambda i: buf.at[i], planes, N_GRAM, plane)
            sent_rows.append((planes - 1) * rows_in(buf) // planes)

        holds_part(3, go)

    def gather_cross(level):
        g = group_of(level)
        gp = spread_of(level)
        p = parts_of[level]
        idx = me % g
        place = me % gp
        sem = sem_of((N_CROSS, level))
        slot = place // g * p + idx
        buf = m[N_CROSS, level]

        def go():
            if level == 3:
                arrive(N_GRAM, planes)
                buf[slot] = jnp.sum(m[N_GRAM][...], axis=0)
            else:
                buf[slot] = sum_parts(level)

            def body(k, carry):
                peer = me - place + lax.rem(place + k, gp)
                remote(buf.at[slot], buf.at[slot], sem, peer).start()
                return carry

            lax.fori_loop(1, gp, body, 0)
            sent_rows.append((gp - 1) * rows_in(buf) // p)

        holds_part(level, go)

    def wide_of(level):
        return max(8, -(-caps[level] // 8) * 8)

    def rows_path(level):
        return size[level] * wide_of(level) <= LANES

    by_slots = size[2] * wide_of(1) <= LANES

    def tucked(level):
        return caps[level] < wide_of(level)

    def couple_rows(level):
        return caps[level] + 1 if rows_path(level) and tucked(level) else wide_of(level)

    def make_couple(level):
        need((N_TGT, level), (N_CPL, level))
        g = size[level]
        gp = size[level + 1]
        u = ups[level]
        wide = wide_of(level)
        sep = gp * LANES
        t = tgt[level][...]
        upd = t >= sep
        rel = jnp.where(upd, t - sep, t)
        dst = rel // LANES
        low = rel % LANES + jnp.where(upd, LANES, 0)
        ri = lax.broadcasted_iota(jnp.int32, (u, u), 0)
        ci = lax.broadcasted_iota(jnp.int32, (u, u), 1)
        dst_f = dst.astype(F32)
        dst_c = jnp.sum(jnp.where(ri == ci, jnp.broadcast_to(dst_f, (u, u)), 0.0), axis=1, keepdims=True)
        same = dst_c == dst_f
        rank = jnp.sum(jnp.where(same & (ri < ci), 1.0, 0.0), axis=0, keepdims=True).astype(jnp.int32)
        pos = dst * wide + rank
        slots = gp * wide
        si = lax.broadcasted_iota(jnp.int32, (slots, u), 0)
        hit = (si == pos).astype(F32)
        hit16 = hit.astype(BF16)
        moved = sum(once(hit16, piece, 1, 0) for piece in halves(cpl[level][...]))
        perm_buf, recv_c = m[N_PERM, level], m[N_COUPLE, level]
        idx = me % gp
        if level == 1 and by_slots:
            m[N_TAKE_KEY][...] = (dst * LANES + me % gp * wide + rank).astype(F32)
        if level == 2:
            m[N_HIT, 0][...] = hit16
            m[N_HIT, 1][...] = (si == pos + 4).astype(F32).astype(BF16)
        if rows_path(level):
            rank_c = jnp.sum(jnp.where(same & (ci < ri), 1.0, 0.0), axis=1, keepdims=True)
            first = (me % g * wide).astype(F32)
            lane = lax.broadcasted_iota(jnp.int32, (u, LANES), 1).astype(F32)
            place = (lane == rank_c + first).astype(F32).astype(BF16)
            low_f = low.astype(F32)
            if tucked(level):
                named = jnp.where(si == dst * wide + caps[level], low_f, 0.0).astype(BF16)
                moved = moved + once(named, place, 1, 0)
            else:
                qi = lax.broadcasted_iota(jnp.int32, (gp, u), 0)
                named = jnp.where(qi == dst, low_f, 0.0).astype(BF16)
                lows = once(named, place, 1, 0)
                lows_s, lows_r = m[N_LOW_S, level], m[N_LOW, level]
                for q in range(gp):
                    lows_s[q] = lows[q : q + 1, :]
                lows_r[idx] = lows_s[idx]
        else:
            shifted = (si == pos + 4).astype(F32)
            lowc = jnp.sum(shifted * low.astype(F32), axis=1, keepdims=True)
            moved = moved + jnp.broadcast_to(lowc, (slots, LANES))
        perm_buf[...] = moved.reshape(gp, wide, LANES)
        recv_c[idx] = perm_buf[idx]

    def send_couple(level):
        gp = size[level + 1]
        perm_buf, recv_c = m[N_PERM, level], m[N_COUPLE, level]
        if rows_path(level) and not tucked(level):
            lows_s, lows_r = m[N_LOW_S, level], m[N_LOW, level]
            send_each(lambda q: lows_s.at[q], lambda i: lows_r.at[i], gp, (N_LOW, level))
            pending.append((lows_s.at[pl.ds(0, gp - 1)], sem_of((N_LOW, level))))
        part = pl.ds(0, couple_rows(level))
        send_each(lambda q: perm_buf.at[q, part], lambda i: recv_c.at[i, part], gp, (N_COUPLE, level))
        pending.append((perm_buf.at[pl.ds(0, gp - 1), part], sem_of((N_COUPLE, level))))

    def ship_couple(level):
        make_couple(level)
        send_couple(level)

    def low_row(level, child):
        g = size[level]
        got = m[N_COUPLE, level] if tucked(level) else m[N_LOW, level]
        one = slice(caps[level], caps[level] + 1) if tucked(level) else slice(0, 1)
        return jnp.sum(got[child * g : (child + 1) * g, one, :], axis=0)[:, : g * wide_of(level)]

    def low_column(level, child):
        g = size[level]
        got = m[N_COUPLE, level][child * g : (child + 1) * g].reshape(g * wide_of(level), LANES)
        si = lax.broadcasted_iota(jnp.int32, (got.shape[0], 1), 0)
        up = jnp.concatenate([got[4:, :1], got[:4, :1]], axis=0)
        return jnp.where(si % 8 < 4, up, -1.0), jnp.where(si % 8 < 4, -1.0, got[:, :1])

    def build_gt(level):
        g = size[level]
        gp = size[level + 1]
        wide = wide_of(level)
        gt = m[N_GT, level]
        rows = gt.shape[1]
        if rows_path(level) and not tucked(level):
            arrive((N_LOW, level), gp)
        got_all = m[N_COUPLE, level]
        wait_for(
            got_all.at[pl.ds(0, gp - 1), pl.ds(0, couple_rows(level))],
            recv_sem.at[sem_of((N_COUPLE, level))],
        )
        slots = g * wide
        for child in range(gp // g):
            got = got_all[child * g : (child + 1) * g].reshape(slots, LANES)
            if rows_path(level):
                if tucked(level):
                    si = lax.broadcasted_iota(jnp.int32, (slots, LANES), 0)
                    got = jnp.where(si % wide < caps[level], got, 0.0)
                ri = lax.broadcasted_iota(jnp.int32, (rows, slots), 0).astype(F32)
                ot = (ri == low_row(level, child)).astype(F32).astype(BF16)
                full = sum(once(piece, ot, 0, 1) for piece in halves(got))
                if level == 1 and by_slots:
                    m[N_OT][:, child * slots : (child + 1) * slots] = ot.astype(F8)
            else:
                lane = lax.broadcasted_iota(jnp.int32, (slots, rows), 1).astype(F32)
                ot = (lane == low_column(level, child)[0]).astype(F32).astype(BF16)
                full = sum(once(piece, ot, 0, 0) for piece in halves(got))
            gt[child * RANK : (child + 1) * RANK, :] = full
            if level < 2:
                put_halves((N_GTH, level), 0, full, child * RANK)

    def reply_rows():
        g = size[2]
        wide = wide_of(2)
        slots = g * wide
        heads = halves(bas[3][:, :RANK])
        tails = halves(m[N_LAST, 3][...])
        for child in range(size[3] // g):
            if rows_path(2):
                low = low_row(2, child)
                lane = lax.broadcasted_iota(jnp.int32, (1, slots), 1) % wide
                one = jnp.where(lane < 4, low, -1.0)
                two = jnp.where(lane < 4, -1.0, pltpu.roll(low, 4, 1))
                iota, by = lax.broadcasted_iota(jnp.int32, (LANES, slots), 0), 0
            else:
                one, two = low_column(2, child)
                iota, by = lax.broadcasted_iota(jnp.int32, (slots, LANES), 1), 1
            iota = iota.astype(F32)
            first = (iota == one).astype(F32).astype(BF16)
            second = (iota == two).astype(F32).astype(BF16)
            rows = once(first, heads[0], by, 0) + once(first, heads[1], by, 0)
            rows = rows + (once(second, tails[0], by, 0) + once(second, tails[1], by, 0))
            m[N_ROWS_S][child * g : (child + 1) * g] = rows.reshape(g, wide, LANES)
        m[N_ROWS_R][me] = m[N_ROWS_S][me]
        send_each(lambda q: m[N_ROWS_S].at[q], lambda i: m[N_ROWS_R].at[i], size[3], N_ROWS_R)
        pending.append((m[N_ROWS_S].at[pl.ds(0, size[3] - 1)], sem_of(N_ROWS_R)))

    def build_named():
        arrive(N_ROWS_R, size[3])
        got = m[N_ROWS_R][...].reshape(size[3] * wide_of(2), LANES)
        pieces = halves(got)
        out = [
            once(pieces[0], m[N_HIT, i][...], 0, 0) + once(pieces[1], m[N_HIT, i][...], 0, 0)
            for i in range(2)
        ]
        put_halves(N_NAMED, 0, jnp.concatenate(out, axis=0))

    g_p = min(plane, 16)
    g_rp = RANK // g_p

    def g_holds(go):
        if plane == g_p:
            go()
        else:
            pl.when(spot < g_p)(go)

    def g_make():
        both = jnp.concatenate([bas[3][:, :RANK], m[N_LAST, 3][...]], axis=1)
        full = mult(m[N_GT, 2][...], both)
        n = full.shape[0] // RANK
        for j in range(g_p):
            m[N_G_P][j] = jnp.concatenate(
                [full[c * RANK + j * g_rp : c * RANK + (j + 1) * g_rp] for c in range(n)], axis=0
            )

    def g_scatter():
        sem = sem_of(N_G_RS)

        def body(k, carry):
            q = lax.rem(spot + k, g_p)

            def go():
                remote(m[N_G_P].at[q], m[N_G_RS].at[spot], sem, me - spot + q).start()

            if plane == g_p:
                go()
            else:
                pl.when(q != spot)(go)
            return carry

        lax.fori_loop(1 if plane == g_p else 0, g_p, body, 0)
        sent_rows.append((g_p - 1) * rows_in(m[N_G_P]) // g_p)

        def keep():
            m[N_G_RS][spot] = m[N_G_P][spot]

        g_holds(keep)

    def upper_of(q):
        return q * plane // size[2]

    def g_across():
        def go():
            arrive(N_G_RS, plane)
            total = jnp.sum(m[N_G_RS][...], axis=0)
            for c in range(total.shape[0] // g_rp):
                m[N_G_ZS][c] = total[c * g_rp : (c + 1) * g_rp]
            m[N_G_Z][layer] = m[N_G_ZS][upper_of(layer)]
            send_each(lambda q: m[N_G_ZS].at[upper_of(q)], lambda i: m[N_G_Z].at[i], planes, N_G_Z, plane)
            sent_rows.append((planes - 1) * rows_in(m[N_G_Z]) // planes)

        g_holds(go)

    def g_gather():
        def go():
            arrive(N_G_Z, planes)
            m[N_G][spot] = jnp.sum(m[N_G_Z][...], axis=0)
            send_each(lambda q: m[N_G].at[spot], lambda i: m[N_G].at[i], plane, N_G)
            sent_rows.append((plane - 1) * rows_in(m[N_G]) // g_p)

        g_holds(go)

    def g_arrive():
        sem = recv_sem.at[sem_of(N_G)]
        if plane == g_p:
            wait_for(m[N_G].at[pl.ds(0, g_p - 1)], sem)
        else:
            pl.when(spot < g_p)(lambda: wait_for(m[N_G].at[pl.ds(0, g_p - 1)], sem))
            pl.when(spot >= g_p)(lambda: wait_for(m[N_G].at[pl.ds(0, g_p)], sem))
        hi, lo = halves(m[N_G][...].reshape(RANK, 2 * RANK))
        m[N_GH, 0][...] = hi
        m[N_GH, 1][...] = lo

    def g_drain():
        if plane == g_p:
            wait_for(m[N_G_P].at[pl.ds(0, g_p - 1)], send_sem.at[sem_of(N_G_RS)])
        else:
            pl.when(spot < g_p)(lambda: wait_for(m[N_G_P].at[pl.ds(0, g_p - 1)], send_sem.at[sem_of(N_G_RS)]))
            pl.when(spot >= g_p)(lambda: wait_for(m[N_G_P], send_sem.at[sem_of(N_G_RS)]))

        def go():
            wait_for(m[N_G_Z].at[pl.ds(0, planes - 1)], send_sem.at[sem_of(N_G_Z)])
            n = plane - 1
            while n > 0:
                wait_for(m[N_G].at[pl.ds(0, min(n, g_p))], send_sem.at[sem_of(N_G)])
                n -= g_p

        g_holds(go)

    def prepare_back(level):
        z = m[N_Z, level][...]
        heads = bas[level][:, :RANK]
        own = mask(N_OWN, level, 0)
        xz = outer(z, blk[level][...]) + outer(shared(level) * own, heads)
        yt = m[N_LAST, level][...]
        if level > 0:
            sep = m[N_GT, level - 1][:, :LANES]
            xz = jnp.concatenate([xz, outer(xz, sep)], axis=1)
            yt = jnp.concatenate([yt, mult(sep, yt)], axis=0)
        m[N_XZ, level][...] = xz
        put_halves((N_BACK, level), 0, yt)

    def arrive_cross(level):
        g = group_of(level)
        p = parts_of[level]
        n = spread_of(level) // g * p
        sem = recv_sem.at[sem_of((N_CROSS, level))]
        buf = m[N_CROSS, level]
        if g == p:
            wait_for(buf.at[pl.ds(0, n - 1)], sem)
        else:
            idx = me % g
            pl.when(idx < p)(lambda: wait_for(buf.at[pl.ds(0, n - 1)], sem))
            pl.when(idx >= p)(lambda: wait_for(buf.at[pl.ds(0, n)], sem))

    def build_bot_middle():
        gp = size[2]
        place = me % gp
        rows = 2 * LANES
        ri = lax.broadcasted_iota(jnp.int32, (rows, LANES), 0)
        arrive(N_TGT_MIDDLE, gp)
        mine = jnp.where(ri < LANES, place * LANES + ri, (gp + place - 1) * LANES + ri).astype(F32)

        def fill(j, carry):
            t = m[N_TGT_MIDDLE][j]
            lanes = pl.ds(pl.multiple_of(j * LANES, LANES), LANES)
            m[N_BOT_MIDDLE][:, lanes] = (mine == t).astype(F32).astype(F8)
            return carry

        lax.fori_loop(0, gp, fill, 0)

    def build_bot_upper():
        rows = planes * LANES
        ri = lax.broadcasted_iota(jnp.int32, (rows, LANES), 0)
        arrive(N_TGT_UPPER, plane)
        mine = ((ri // LANES * plane + spot) * LANES + ri % LANES).astype(F32)

        def fill(j, carry):
            t = m[N_TGT_UPPER][j]
            lanes = pl.ds(pl.multiple_of(j * LANES, LANES), LANES)
            m[N_BOT_UPPER][:, lanes] = (mine == t).astype(F32).astype(F8)
            return carry

        lax.fori_loop(0, plane, fill, 0)

    def build_take():
        key = m[N_TAKE_KEY][...]
        ri = lax.broadcasted_iota(jnp.int32, (LANES, LANES), 0)

        def fill(j, carry):
            rows = pl.ds(pl.multiple_of(j * LANES, LANES), LANES)
            m[N_TAKE][rows, :] = ((ri + j * LANES).astype(F32) == key).astype(F32).astype(F8)
            return carry

        lax.fori_loop(0, size[2], fill, 0)

    def build_ft_middle():
        t = tgt[1][...]
        ri = lax.broadcasted_iota(jnp.int32, (LANES, LANES), 0)

        def fill(j, carry):
            rows = pl.ds(pl.multiple_of(j * LANES, LANES), LANES)
            m[N_FT_MIDDLE][rows, :] = (ri + j * LANES == t).astype(F32).astype(F8)
            return carry

        lax.fori_loop(0, m[N_FT_MIDDLE].shape[0] // LANES, fill, 0)

    def build_ft_upper():
        arrive(N_TGT_LAYER, planes)
        t = jnp.concatenate([m[N_TGT_LAYER][j] for j in range(planes)], axis=1)
        ri = lax.broadcasted_iota(jnp.int32, (LANES, planes * LANES), 0)

        def fill(j, carry):
            rows = pl.ds(pl.multiple_of(j * LANES, LANES), LANES)
            here = ((ri + (layer * plane + j) * LANES).astype(F32) == t).astype(F32)
            m[N_FT_UPPER][rows, :] = here.astype(F8)
            return carry

        lax.fori_loop(0, plane, fill, 0)

    def share(level, zp):
        m[N_ZP, level][me % size[level]] = zp
        send_all((N_ZP, level), size[level])

    def shared(level):
        arrive((N_ZP, level), size[level])
        return jnp.sum(m[N_ZP, level][...], axis=0)

    def make_cross(level):
        need((N_EXP, level), (N_BAS, level))
        m[N_CROSS_P, level][...] = inner(exp[level][...], bas[level][:, RANK:])

    def start_cross(level):
        make_cross(level)
        scatter_cross(level)

    need((N_SRC, 0), (N_BAS, 0))
    m[N_F0][me % size[0]] = mult(src[0][...], bas[0][:, :RANK])
    make_cross(1)
    pl.semaphore_wait(barrier, plane - 1 + layer * plane)
    send_all(N_F0, size[0])
    scatter_cross(1)
    lax.fori_loop(0, layer, greet_back, 0)
    ship_couple(0)
    need((N_BLK, 0), (N_EXP, 0), (N_PIV, 0))
    local = mult(src[0][...], blk[0][...])
    fill_masks(0)
    build_forward(1)
    make_cross(2)
    pl.when(layer < planes - 1)(lambda: pl.semaphore_wait(up_sem, planes - 1 - layer))
    scatter_cross(2)
    arrive(N_F0, size[0])
    hq = jnp.sum(m[N_F0][...], axis=0) * mask(N_OWN, 0, 0)
    y = local + outer(hq, exp[0][...])
    m[N_F1][spot] = mult(y, bas[0][:, RANK:])
    send_all(N_F1, plane)
    m[N_Z, 0][...] = y * piv[0][...]
    fill_masks(1)
    gather_cross(1)
    need((N_TGT, 1), (N_TGT, 2))
    m[N_TGT_MIDDLE][me % size[2]] = tgt[1][...].astype(F32)
    send_all(N_TGT_MIDDLE, size[2])
    mine_t = tgt[2][...].astype(F32)
    m[N_TGT_UPPER][spot] = mine_t
    send_all(N_TGT_UPPER, plane)
    m[N_TGT_LAYER][layer] = mine_t
    send_all(N_TGT_LAYER, planes, plane)
    ship_couple(1)
    ship_couple(2)
    gather_cross(2)
    build_gt(0)

    for level in range(3):
        g = size[level]
        gp = size[level + 1]
        nch = gp // g
        child_me = me % gp // g
        need((N_SRC, level + 1))
        name = (N_F1, N_F2, N_F3B)[level]
        buf, step = m[name], g
        if level == 2:
            step = g // plane
        if level == 1:
            arrive(N_F2U, gp)
            rows = jnp.concatenate([m[N_F2U][j] for j in range(gp)], axis=1)
            inc = select(rows, m[N_BOT_MIDDLE][...], 1)
        arrive(name, gp if level < 2 else planes)
        ws = [
            jnp.sum(buf[child * step : (child + 1) * step, :count, :], axis=0) * mask(N_KID, level, child, 1)
            for child in range(nch)
        ]
        ws = jnp.concatenate(ws, axis=1)
        bn = src[level + 1][...]
        if level == 0:
            inc = by_halves(ws, (N_GTH, 0), 0)
            m[N_F2U][me % size[2]] = -inc[:, LANES:]
            send_all(N_F2U, size[2])
            local_n, bq, w = local_forward(1, bn - inc[:, :LANES])
            arrive_cross(1)
            sent = [w + mult(bq * mask(N_OWN, 1, 0), m[N_CROSS, 1][...].reshape(RANK, RANK))]
        elif level == 1:
            bn = jnp.concatenate([bn + inc[:, :LANES], ws], axis=1)
            upd = inc[:, LANES:] - by_halves(ws, (N_GTH, 1), 0, slice(LANES, 2 * LANES))
            local_n, bq, w = local_forward(2, bn)
            arrive_cross(2)
            sent = [w + mult(bq * mask(N_OWN, 2, 0), m[N_CROSS, 2][...].reshape(RANK, RANK)), upd]
        else:
            bn = jnp.concatenate([bn + jnp.sum(buf[:, count : 2 * count, :], axis=0), ws], axis=1)
            local_n, bq, *sent = local_forward(3, bn)
            sent = [bq] + sent[:1] + sent[2:] + sent[1:2]
        name = (N_F2, N_F3A, N_F4A)[level]
        group = size[2] if level == 0 else plane
        m[name][me % group] = jnp.concatenate(sent, axis=0)
        send_all(name, group)
        if level < 2:
            m[N_HQ, level + 1][me % gp] = bq
            send_all((N_HQ, level + 1), gp)
        if level == 1:
            g_scatter()
        if level == 2:
            g_across()
        if level > 0:
            arrive((N_HQ, level), g)
            hq = jnp.sum(m[N_HQ, level][...], axis=0) * mask(N_OWN, level, 0)
            z = (local + outer(hq, exp[level][...])) * piv[level][...]
            m[N_Z, level][...] = z
            share(level, mult(z, exp[level][...]))
        local = local_n
        if level == 0:
            add_cross(1)
            build_forward(2)
            fill_masks(2)
            build_forward(3)
            scatter_cross(3)
            build_gt(1)
            build_bot_middle()
            chain_forward(2)
            build_gt(2)
            g_make()
        elif level == 1:
            reply_rows()
            add_cross(2)
            build_bot_upper()
            fill_masks(3)
            arrive(N_F3A, plane)
            sums = jnp.sum(m[N_F3A][:, :count, :], axis=0)
            rows = jnp.concatenate([m[N_F3A][j, count:, :] for j in range(plane)], axis=1)
            part = select(rows, m[N_BOT_UPPER][...], 1)
            for q in range(planes):
                m[N_F3S][q] = jnp.concatenate([sums, part[:, q * LANES : (q + 1) * LANES]], axis=0)
            m[N_F3B][layer] = m[N_F3S][layer]
            send_each(lambda q: m[N_F3S].at[q], lambda i: m[N_F3B].at[i], planes, N_F3B, plane)
            pending.append((m[N_F3S].at[pl.ds(0, planes - 1)], sem_of(N_F3B)))
            put_halves((N_FWD, 3), 4 * RANK, outer(m[N_NEAR][...], m[N_GT, 2][...]))
            chain_forward(3)
            share(0, mult(m[N_Z, 0][...], exp[0][...]))
            start_cross(0)
            m[N_LAST, 0][...] = mult(blk[0][...], bas[0][:, RANK:])
            build_ft_upper()
            if by_slots:
                build_take()
            cross_planes()
    gather_cross(3)
    gather_cross(0)
    g_gather()
    arrive(N_F4A, plane)
    o = (2 + size[3] // size[2]) * count
    sums = jnp.sum(m[N_F4A][:, :o, :], axis=0)
    rows = jnp.concatenate([m[N_F4A][j, o:, :] for j in range(plane)], axis=1)
    part = select(rows, m[N_FT_UPPER][...], 0)
    for q in range(planes):
        c = 2 + q * plane // size[2]
        m[N_F4S][q] = jnp.concatenate(
            [sums[: 2 * count], sums[c * count : (c + 1) * count], part[:, q * LANES : (q + 1) * LANES]], axis=0
        )
    m[N_F4B][layer] = m[N_F4S][layer]
    send_each(lambda q: m[N_F4S].at[q], lambda i: m[N_F4B].at[i], planes, N_F4B, plane)
    pending.append((m[N_F4S].at[pl.ds(0, planes - 1)], sem_of(N_F4B)))
    build_named()
    prepare_back(2)
    arrive_cross(3)
    arrive(N_F4B, planes)
    g_arrive()
    both = jnp.sum(m[N_F4B][...], axis=0)
    hq = both[:count] * mask(N_OWN, 3, 0)
    rp = (both[count : 2 * count] + mult(hq, m[N_CROSS, 3][...].reshape(RANK, RANK))) * mask(N_OWN, 3, 0)
    pair = jnp.concatenate([rp, hq], axis=1)
    s = both[2 * count : 3 * count] + by_halves(pair, N_GH, 1)
    xu = both[3 * count :] + by_halves(pair, N_NAMED, 0)

    for level in (2, 1, 0):
        s = s * mask(N_OWN, level, 1)
        xs = m[N_XZ, level][...] - by_halves(s, (N_BACK, level), 1)
        x = xs[:, :LANES]
        if level == 0:
            outs[0][...] = x
            break
        g = size[level - 1]
        gp = size[level]
        nch = gp // g
        place = me % gp
        child_me = place // g
        sp = xs[:, LANES:] + by_halves(xu, (N_GTH, level - 1), 1, slice(LANES, 2 * LANES))
        name = (N_B3, N_B2)[level - 1]
        buf, piece = m[name], m[N_PIECE, level - 1]
        for c in range(nch):
            rest = []
            if level == 2 and by_slots:
                rest = [select(jnp.concatenate([x, xu], axis=1), m[N_OT][...], 0)]
            elif level == 2:
                rest = [x, xu]
            piece[c] = jnp.concatenate([sp[:, c * RANK : (c + 1) * RANK]] + rest, axis=0)
        buf[place] = piece[child_me]
        send_each(lambda q: piece.at[lax.div(q, g)], lambda i: buf.at[i], gp, name)
        pending.append((buf.at[pl.ds(0, gp - 1)], sem_of(name)))
        outs[level][...] = x
        if level == 2:
            z = (local + outer(hq, exp[3][...])) * piv[3][...]
            outs[3][...] = outer(z, blk[3][...]) + outer(rp, bas[3][:, :RANK])
        else:
            add_cross(0)
        prepare_back(level - 1)
        arrive(name, gp)
        s = jnp.sum(buf[:, :count, :], axis=0)
        if level == 2:
            blocks = [buf[j, count : 2 * count, :] for j in range(gp)]
            if not by_slots:
                blocks += [buf[j, 2 * count :, :] for j in range(gp)]
                build_ft_middle()
            xu = select(jnp.concatenate(blocks, axis=1), m[N_TAKE if by_slots else N_FT_MIDDLE][...], 0)

    if shared_sends:
        assert all(group_of(level) == parts_of[level] for level in range(4))
        wait_rows(sum(sent_rows) + sum(rows_in(part) for part, _ in pending), send_sem.at[0])
    else:
        for part, sem in pending:
            wait_for(part, send_sem.at[sem])
        for level in range(4):
            g = group_of(level)
            p = parts_of[level]
            rp = RANK // p
            gp = spread_of(level)
            n = gp // g * p
            idx = me % g
            rs_sem = send_sem.at[sem_of((N_RS, level))]
            ag_sem = send_sem.at[sem_of((N_CROSS, level))]
            cross_p, buf = m[N_CROSS_P, level], m[N_CROSS, level]

            def ag_done():
                for _ in range((gp - 1) // n):
                    wait_for(buf.at[pl.ds(0, n)], ag_sem)
                if (gp - 1) % n:
                    wait_for(buf.at[pl.ds(0, (gp - 1) % n)], ag_sem)
                if level == 3:
                    wait_for(m[N_GRAM].at[pl.ds(0, planes - 1)], send_sem.at[sem_of(N_GRAM)])

            if g == p:
                wait_for(cross_p.at[pl.ds(0, (p - 1) * rp)], rs_sem)
                ag_done()
            else:
                pl.when(idx < p)(lambda: wait_for(cross_p.at[pl.ds(0, (p - 1) * rp)], rs_sem))
                pl.when(idx >= p)(lambda: wait_for(cross_p, rs_sem))
                pl.when(idx < p)(ag_done)
        g_drain()
    assert len(sems) <= NSEM


def put_out(*refs):
    n = len(refs) // 2
    ins, outs, sem = refs[:n], refs[n : 2 * n], refs[-1]
    copies = [pltpu.make_async_copy(ins[i], outs[i], sem.at[i]) for i in range(n)]
    for c in copies:
        c.start()
    for c in copies:
        c.wait()


def solution(mesh):
    leaves, across = mesh.shape["leaf"], mesh.shape["grid"]

    def shards(*args):
        levels = [args[8 * i : 8 * i + 8] for i in range(3)]
        root = args[24:30]
        (sl, bl, el, qs, pv, cl, rk, tg) = zip(*levels)
        src = list(sl) + [root[0]]
        blk = list(bl) + [root[1]]
        exp = list(el) + [root[2]]
        bas = list(qs) + [root[3]]
        piv = [v.reshape(1, -1) for v in list(pv) + [root[4]]]
        rnk = list(rk) + [root[5]]
        tgt = [t.reshape(1, -1) for t in tg]
        count = src[0].shape[0]
        ups = [t.shape[1] for t in tgt]
        fronts = [r.shape[0] for r in rnk]
        rnk = [r.T if r.shape[0] > 2 else r for r in rnk]
        size = [leaves * across // f for f in fronts]
        for v in src:
            assert v.shape[1] == LANES
        vm = lambda *s: pltpu.VMEM(s, F32)
        bits = lambda *s: pltpu.VMEM(s, BF16)
        ones = lambda *s: pltpu.VMEM(s, F8)
        total = leaves * across
        plane = size[1]
        planes = total // plane
        nch = [size[i + 1] // size[i] for i in range(3)]
        caps = [max(1, -(-ups[i] // size[i + 1])) for i in range(3)]
        group = size[:3] + [plane]
        spread = group
        parts = [min(g, 16) for g in group]
        by_slots = size[2] * max(8, -(-caps[1] // 8) * 8) <= LANES
        bufs = {
            N_F0: vm(size[0], count, LANES),
            N_F1: vm(plane, count, LANES),
            N_F2: vm(size[2], count, LANES),
            N_F2U: vm(size[2], count, LANES),
            N_F3A: vm(plane, 2 * count, LANES),
            N_F3S: vm(planes, 2 * count, LANES),
            N_F3B: vm(planes, 2 * count, LANES),
            (N_HQ, 1): vm(size[1], count, LANES),
            (N_HQ, 2): vm(size[2], count, LANES),
            N_F4A: vm(plane, (nch[2] + 3) * count, LANES),
            N_F4S: vm(planes, 4 * count, LANES),
            N_F4B: vm(planes, 4 * count, LANES),
            N_NEAR: vm(LANES, LANES),
            N_RULER: vm(8192 if total <= 64 else 1024, LANES),
            (N_HIT, 0): bits(total * 8, LANES),
            (N_HIT, 1): bits(total * 8, LANES),
            N_ROWS_S: vm(total, 8, LANES),
            N_ROWS_R: vm(total, 8, LANES),
            (N_NAMED, 0): bits(2 * RANK, LANES),
            (N_NAMED, 1): bits(2 * RANK, LANES),
            (N_GH, 0): bits(RANK, 2 * RANK),
            (N_GH, 1): bits(RANK, 2 * RANK),
            N_G_P: vm(parts[3], nch[2] * RANK // parts[3], 2 * RANK),
            N_G_RS: vm(plane, nch[2] * RANK // parts[3], 2 * RANK),
            N_G_ZS: vm(nch[2], RANK // parts[3], 2 * RANK),
            N_G_Z: vm(planes, RANK // parts[3], 2 * RANK),
            N_G: vm(parts[3], RANK // parts[3], 2 * RANK),
            N_B2: vm(size[2], (2 if by_slots else 3) * count, LANES),
            N_B3: vm(size[1], count, LANES),
            N_TGT_MIDDLE: vm(size[2], 1, LANES),
            N_TGT_UPPER: vm(plane, 1, LANES),
            N_TGT_LAYER: vm(planes, 1, LANES),
            N_BOT_MIDDLE: ones(2 * LANES, size[2] * LANES),
            N_BOT_UPPER: ones(planes * LANES, plane * LANES),
            N_FT_UPPER: ones(plane * LANES, planes * LANES),
            N_MASK: vm(6 + 2 * sum(nch), count, LANES),
            N_GRAM: vm(planes, RANK // parts[3], RANK),
        }
        arrays = {N_SRC: src, N_BLK: blk, N_EXP: exp, N_BAS: bas, N_PIV: piv, N_RNK: rnk, N_CPL: cl, N_TGT: tgt}
        for name, list_of in arrays.items():
            for i, v in enumerate(list_of):
                bufs[name, i] = pltpu.VMEM(v.shape, v.dtype)
        for i in range(4):
            bufs[N_LAST, i] = vm(LANES, RANK)
            for j in range(2):
                if i > 0:
                    bufs[(N_FWD, i), j] = bits(LANES + (nch[i - 1] * RANK if i > 1 else 0), (3 if i < 3 else 4 + nch[2]) * RANK)
                if i < 3:
                    bufs[(N_BACK, i), j] = bits((1 + (nch[i - 1] if i > 0 else 0)) * RANK, RANK)
        if by_slots:
            bufs[N_TAKE_KEY] = vm(1, LANES)
            bufs[N_TAKE] = ones(size[2] * LANES, LANES)
            bufs[N_OT] = ones(2 * LANES, LANES)
        else:
            bufs[N_FT_MIDDLE] = ones(size[2] * 2 * LANES, LANES)
        for i in range(2):
            for j in range(2):
                bufs[(N_GTH, i), j] = bits(nch[i] * RANK, 2 * LANES)
        for i in range(3):
            bufs[N_Z, i] = vm(count, LANES)
            bufs[N_XZ, i] = vm(count, (1 + (nch[i - 1] if i > 0 else 0)) * LANES)
        for i in range(4):
            bufs[N_CROSS_P, i] = vm(RANK, RANK)
            bufs[N_RS, i] = vm(group[i], RANK // parts[i], RANK)
            bufs[N_CROSS, i] = vm(spread[i] // group[i] * parts[i], RANK // parts[i], RANK)
        for i in range(3):
            wide = max(8, -(-caps[i] // 8) * 8)
            assert caps[i] <= 4 or size[i] * wide <= LANES
            if caps[i] == wide:
                bufs[N_LOW_S, i] = vm(size[i + 1], 1, LANES)
                bufs[N_LOW, i] = vm(size[i + 1], 1, LANES)
            bufs[N_PERM, i] = vm(size[i + 1], wide, LANES)
            bufs[N_COUPLE, i] = vm(size[i + 1], wide, LANES)
            bufs[N_GT, i] = vm(nch[i] * RANK, LANES * (1 if i == 2 else 2))
            bufs[N_ZP, i] = vm(size[i], count, LANES)
            bufs[N_PIECE, i] = vm(nch[i], (1 if i == 0 else 2 if by_slots else 3) * count, LANES)
        scratch = list(bufs.values())
        scratch += [pltpu.SemaphoreType.DMA((n,)) for n in (1 if total <= 64 else NSEM, NSEM, 11)]
        scratch += [pltpu.SemaphoreType.REGULAR]
        vspec = pl.BlockSpec(memory_space=pltpu.VMEM)
        aspec = pl.BlockSpec(memory_space=pl.ANY)
        answers = pl.pallas_call(
            functools.partial(kernel, (leaves, across, size, ups, count, caps, fronts), list(bufs)),
            out_shape=[pltpu.VMEM(v.shape, F32) for v in src],
            in_specs=[aspec] * 30,
            out_specs=[vspec] * 4,
            scratch_shapes=scratch,
            compiler_params=pltpu.CompilerParams(
                collective_id=0, has_side_effects=True, vmem_limit_bytes=63 * 1024 * 1024
            ),
        )(*src, *blk, *exp, *bas, *piv, *rnk, *cl, *tgt)
        return pl.pallas_call(
            put_out,
            out_shape=[jax.ShapeDtypeStruct(v.shape, F32) for v in src],
            in_specs=[vspec] * 4,
            out_specs=[aspec] * 4,
            scratch_shapes=[pltpu.SemaphoreType.DMA((4,))],
        )(*[pltpu.with_memory_space_constraint(v, pltpu.VMEM) for v in answers])

    spread_axes = ("leaf", "grid")
    level = (P(None, spread_axes), P(spread_axes, None), P(spread_axes, None), P(spread_axes, None), P(spread_axes))
    mid = level + (P(spread_axes, None), P(), P(spread_axes))
    return jax.shard_map(
        shards,
        mesh=mesh,
        in_specs=mid * 3 + level + (P(),),
        out_specs=(P(None, spread_axes),) * 4,
        check_vma=False,
    )
```

```python
import functools
import math

import jax
import jax.numpy as jnp
from jax import lax
from jax.experimental import pallas as pl
from jax.experimental.pallas import tpu as pltpu
from jax.sharding import PartitionSpec as P

RANK = 128
LANES = 128
MESH = pl.DeviceIdType.MESH
NSEM = 34
F32 = jnp.float32
BF16 = jnp.bfloat16
F8 = jnp.float8_e4m3fn

(
    N_SRC, N_BLK, N_EXP, N_BAS, N_PIV, N_RNK, N_CPL, N_TGT, N_RULER, N_TGT_MIDDLE, N_TGT_UPPER, N_TGT_LAYER,
    N_COUPLE, N_MASK, N_OWN, N_KID, N_CROSS_P, N_LAST, N_NEAR, N_FWD, N_GT, N_CROSS, N_RS, N_GRAM, N_PERM,
    N_TAKE_KEY, N_HIT, N_LOW_S, N_LOW, N_OT, N_GTH, N_ROWS_S, N_ROWS_R, N_NAMED, N_G_P, N_G_RS, N_G_ZS,
    N_G_Z, N_G, N_GH, N_Z, N_XZ, N_BACK, N_BOT_MIDDLE, N_BOT_UPPER, N_TAKE, N_FT_MIDDLE, N_FT_UPPER, N_ZP,
    N_F0, N_F1, N_F2, N_F3B, N_F2U, N_F3A, N_F4A, N_HQ, N_F3S, N_F4S, N_F4B, N_B3, N_B2, N_PIECE,
) = range(63)


def once(a, b, ca, cb):
    return lax.dot_general(a, b, (((ca,), (cb,)), ((), ())), preferred_element_type=F32)


def halves(x):
    hi = x.astype(BF16)
    return hi, (x - hi.astype(F32)).astype(BF16)


def dot(a, b, ca, cb):
    ah, al = halves(a)
    bh, bl = halves(b)
    if ca == 0:
        return once(ah, bh, ca, cb) + (once(al, bh, ca, cb) + once(ah, bl, ca, cb))
    n = a.shape[0]
    both = once(jnp.concatenate([ah.astype(F32), al.astype(F32)], axis=0).astype(BF16), bh, ca, cb)
    return both[:n] + (both[n:] + once(ah, bl, ca, cb))


def mult(a, b):
    return dot(a, b, 1, 0)


def outer(a, b):
    return dot(a, b, 1, 1)


def inner(a, b):
    return dot(a, b, 0, 0)


def select(x, onehot, cb):
    hi = x.astype(BF16).astype(F32)
    out = once(jnp.concatenate([hi, x - hi], axis=0).astype(BF16), onehot, 1, cb)
    n = x.shape[0]
    return out[:n] + out[n:]


KINDS = (N_SRC, N_BLK, N_EXP, N_BAS, N_PIV, N_RNK)


def kernel(cfg, names, *refs):
    leaves, across, size, ups, count, caps, fronts = cfg
    total_devices = leaves * across
    hbm = [refs[4 * i : 4 * i + 4] for i in range(6)]
    cpl_in = refs[24:27]
    tgt_in = refs[27:30]
    outs = refs[30:34]
    m = dict(zip(names, refs[34:-4]))
    send_sem, recv_sem, load_sem, up_sem = refs[-4:]
    sems = {}
    src, blk, exp, bas, piv, rnk = [[m[k, i] for i in range(4)] for k in KINDS]
    cpl = [m[N_CPL, i] for i in range(3)]
    tgt = [m[N_TGT, i] for i in range(3)]

    me = lax.axis_index("leaf") * across + lax.axis_index("grid")
    plane = size[1]
    planes = total_devices // plane
    spot = me % plane
    layer = me // plane
    pending = []

    shared_sends = total_devices <= 64
    sent_rows = []
    loaded = set()
    order = [[(N_SRC, 0), (N_BAS, 0)], [(N_EXP, 1), (N_BAS, 1)]]
    order += [[(N_CPL, 0), (N_TGT, 0), (N_BLK, 0), (N_EXP, 0), (N_PIV, 0)]]
    order += [[(N_RNK, i)] for i in range(4)]
    order += [[(N_BLK, 1), (N_SRC, 1), (N_PIV, 1), (N_CPL, 1), (N_TGT, 1), (N_TGT, 2), (N_CPL, 2)]]
    order += [[(k, i) for i in (2, 3) for k in (N_EXP, N_BAS, N_BLK, N_SRC, N_PIV)]]
    where_from = {(k, i): hbm[j][i] for j, k in enumerate(KINDS) for i in range(4)}
    for i in range(3):
        where_from[N_CPL, i] = cpl_in[i]
        where_from[N_TGT, i] = tgt_in[i]

    def load(some):
        for keys in some:
            for key in keys:
                pltpu.make_async_copy(where_from[key], m[key], load_sem.at[order.index(keys)]).start()

    def rows_in(ref):
        return math.prod(ref.shape) // LANES

    def wait_rows(rows, sem):
        wait_for(m[N_RULER].at[pl.ds(0, rows)], sem)

    def need(*wanted):
        for i, keys in enumerate(order):
            if any(key in keys for key in wanted) and i not in loaded:
                loaded.add(i)
                if len(keys) == 1:
                    wait_for(m[keys[0]], load_sem.at[i])
                else:
                    wait_rows(sum(rows_in(m[key]) for key in keys), load_sem.at[i])

    def where(peer):
        return (lax.div(peer, across), lax.rem(peer, across))

    def sem_of(name):
        name = N_TGT_MIDDLE if name in (N_TGT_UPPER, N_TGT_LAYER) else name
        return sems.setdefault(name, len(sems))

    def remote(a, b, sem, peer):
        return pltpu.make_async_remote_copy(
            src_ref=a,
            dst_ref=b,
            send_sem=send_sem.at[0 if shared_sends else sem],
            recv_sem=recv_sem.at[sem],
            device_id=where(peer),
            device_id_type=MESH,
        )

    def wait_for(part, sem):
        pltpu.make_async_copy(part, part, sem).wait()

    def send_each(source, dest, group, name, stride=1):
        idx = me // stride % group
        base = me - idx * stride
        sem = sem_of(name)

        def body(k, carry):
            q = lax.rem(idx + k, group)
            remote(source(q), dest(idx), sem, base + q * stride).start()
            return carry

        lax.fori_loop(1, group, body, 0)

    def send_all(name, group, stride=1):
        buf = m[name]
        idx = me // stride % group
        send_each(lambda q: buf.at[idx], lambda i: buf.at[i], group, name, stride)
        pending.append((buf.at[pl.ds(0, group - 1)], sem_of(name)))

    def arrive(name, group):
        wait_for(m[name].at[pl.ds(0, group - 1)], recv_sem.at[sem_of(name)])

    load(order[:3])
    m[N_COUPLE, 2][...] = jnp.zeros(m[N_COUPLE, 2].shape, F32)
    barrier = pltpu.get_barrier_semaphore()

    def greet_near(k, carry):
        peer = me - spot + lax.rem(spot + k, plane)
        pl.semaphore_signal(barrier, inc=1, device_id=where(peer), device_id_type=MESH)
        return carry

    def greet_far(peer, carry):
        pl.semaphore_signal(barrier, inc=1, device_id=where(peer), device_id_type=MESH)
        return carry

    def greet_back(k, carry):
        pl.semaphore_signal(up_sem, inc=1, device_id=where(k * plane + spot), device_id_type=MESH)
        return carry

    lax.fori_loop(1, plane, greet_near, 0)
    lax.fori_loop((layer + 1) * plane, total_devices, greet_far, 0)
    load(order[3:])

    col = lax.broadcasted_iota(jnp.int32, (count, RANK), 1).astype(F32)
    mask_slots = {}

    def fill_mask(name, level, front, which):
        ranks = rnk[level][...].astype(F32)
        if ranks.shape[0] == 2 and fronts[level] > 2:
            lane = lax.broadcasted_iota(jnp.int32, ranks.shape, 1)
            row = lax.broadcasted_iota(jnp.int32, ranks.shape, 0)
            hit = (lane == front) & (row == which)
        else:
            lane = lax.broadcasted_iota(jnp.int32, ranks.shape, 1)
            row = lax.broadcasted_iota(jnp.int32, ranks.shape, 0)
            hit = (lane == which) & (row == front)
        r = jnp.sum(jnp.where(hit, ranks, 0.0), axis=1, keepdims=True)
        r = jnp.sum(r, axis=0, keepdims=True)
        slot = mask_slots.setdefault(name, len(mask_slots))
        m[N_MASK][slot] = (col < r).astype(F32)

    def mask(*name):
        return m[N_MASK][mask_slots[name]]

    def fill_masks(level):
        need((N_RNK, level))
        fill_mask((N_OWN, level, 0), level, me // size[level], 0)
        if level == 3:
            return
        fill_mask((N_OWN, level, 1), level, me // size[level], 1)
        nch = size[level + 1] // size[level]
        for child in range(nch):
            front = me // size[level + 1] * nch + child
            fill_mask((N_KID, level, child, 1), level, front, 1)

    def build_forward(level):
        need((N_BLK, level), (N_BAS, level), (N_PIV, level), (N_EXP, level))
        parts = [blk[level][...], bas[level][:, :RANK]]
        if level == 3:
            pt = exp[3][...].T * piv[3][...]
            m[N_CROSS_P, 3][...] = mult(pt, exp[3][...])
            m[N_LAST, 3][...] = outer(blk[3][...], pt)
            m[N_NEAR][...] = outer(blk[3][...] * piv[3][...], blk[3][...])
            parts += [m[N_LAST, 3][...], m[N_NEAR][...]]
        else:
            m[N_LAST, level][...] = mult(blk[level][...], bas[level][:, RANK:])
            parts += [m[N_LAST, level][...]]
        put_halves((N_FWD, level), 0, jnp.concatenate(parts, axis=1))

    def put_halves(name, start, value, first=0):
        hi, lo = halves(value)
        lanes = slice(start, start + value.shape[1])
        rows = slice(first, first + value.shape[0])
        m[name, 0][rows, lanes] = hi
        m[name, 1][rows, lanes] = lo

    def chain_forward(level):
        top = m[(N_FWD, level), 0][:LANES].astype(F32) + m[(N_FWD, level), 1][:LANES].astype(F32)
        put_halves((N_FWD, level), 0, -mult(m[N_GT, level - 1][:, :LANES], top), LANES)

    def add_cross(level):
        if level == 0:
            arrive_cross(0)
        heads = bas[level][:, :RANK] * mask(N_OWN, level, 0)[:1]
        yt = m[N_LAST, level][...] + mult(heads, m[N_CROSS, level][...].reshape(RANK, RANK))
        m[N_LAST, level][...] = yt

    def by_halves(a, name, cb, lanes=slice(None)):
        ah, al = halves(a)
        n = a.shape[0]
        wh = m[name, 0][:, lanes]
        two = once(jnp.concatenate([ah.astype(F32), al.astype(F32)], axis=0).astype(BF16), wh, 1, cb)
        return two[:n] + (two[n:] + once(ah, m[name, 1][:, lanes], 1, cb))

    def local_forward(level, b):
        out = by_halves(b, (N_FWD, level), 0)
        return [out[:, i : i + RANK] for i in range(0, out.shape[1], RANK)]

    def group_of(level):
        return size[level] if level < 3 else plane

    parts_of = [min(group_of(level), 16) for level in range(4)]

    def scatter_cross(level):
        g = group_of(level)
        p = parts_of[level]
        rp = RANK // p
        idx = me % g
        base = me - idx
        sem = sem_of((N_RS, level))
        cross_p, rs_buf = m[N_CROSS_P, level], m[N_RS, level]

        def body(k, carry):
            q = lax.rem(idx + k, p)

            def go():
                rows = pl.ds(pl.multiple_of(q * rp, 8), rp)
                remote(cross_p.at[rows], rs_buf.at[idx], sem, base + q).start()

            if g == p:
                go()
            else:
                pl.when(q != idx)(go)
            return carry

        lax.fori_loop(1 if g == p else 0, p, body, 0)
        sent_rows.append((p - 1) * rp)

        def keep():
            rows = pl.ds(pl.multiple_of(idx * rp, 8), rp)
            rs_buf[idx] = cross_p[rows, :]

        if g == p:
            keep()
        else:
            pl.when(idx < p)(keep)

    def spread_of(level):
        return group_of(level)

    def holds_part(level, go):
        if group_of(level) == parts_of[level]:
            go()
        else:
            pl.when(me % group_of(level) < parts_of[level])(go)

    def sum_parts(level):
        g = group_of(level)
        wait_for(m[N_RS, level].at[pl.ds(0, g - 1)], recv_sem.at[sem_of((N_RS, level))])
        return jnp.sum(m[N_RS, level][...], axis=0)

    def cross_planes():
        buf = m[N_GRAM]

        def go():
            buf[layer] = sum_parts(3)
            send_each(lambda q: buf.at[layer], lambda i: buf.at[i], planes, N_GRAM, plane)
            sent_rows.append((planes - 1) * rows_in(buf) // planes)

        holds_part(3, go)

    def gather_cross(level):
        g = group_of(level)
        gp = spread_of(level)
        p = parts_of[level]
        idx = me % g
        place = me % gp
        sem = sem_of((N_CROSS, level))
        slot = place // g * p + idx
        buf = m[N_CROSS, level]

        def go():
            if level == 3:
                arrive(N_GRAM, planes)
                buf[slot] = jnp.sum(m[N_GRAM][...], axis=0)
            else:
                buf[slot] = sum_parts(level)

            def body(k, carry):
                peer = me - place + lax.rem(place + k, gp)
                remote(buf.at[slot], buf.at[slot], sem, peer).start()
                return carry

            lax.fori_loop(1, gp, body, 0)
            sent_rows.append((gp - 1) * rows_in(buf) // p)

        holds_part(level, go)

    def wide_of(level):
        return max(8, -(-caps[level] // 8) * 8)

    def rows_path(level):
        return size[level] * wide_of(level) <= LANES

    by_slots = size[2] * wide_of(1) <= LANES

    def tucked(level):
        return caps[level] < wide_of(level)

    def couple_rows(level):
        return caps[level] + 1 if rows_path(level) and tucked(level) else wide_of(level)

    def make_couple(level):
        need((N_TGT, level), (N_CPL, level))
        g = size[level]
        gp = size[level + 1]
        u = ups[level]
        wide = wide_of(level)
        sep = gp * LANES
        t = tgt[level][...]
        upd = t >= sep
        rel = jnp.where(upd, t - sep, t)
        dst = rel // LANES
        low = rel % LANES + jnp.where(upd, LANES, 0)
        ri = lax.broadcasted_iota(jnp.int32, (u, u), 0)
        ci = lax.broadcasted_iota(jnp.int32, (u, u), 1)
        dst_f = dst.astype(F32)
        dst_c = jnp.sum(jnp.where(ri == ci, jnp.broadcast_to(dst_f, (u, u)), 0.0), axis=1, keepdims=True)
        same = dst_c == dst_f
        rank = jnp.sum(jnp.where(same & (ri < ci), 1.0, 0.0), axis=0, keepdims=True).astype(jnp.int32)
        pos = dst * wide + rank
        slots = gp * wide
        si = lax.broadcasted_iota(jnp.int32, (slots, u), 0)
        hit = (si == pos).astype(F32)
        hit16 = hit.astype(BF16)
        moved = sum(once(hit16, piece, 1, 0) for piece in halves(cpl[level][...]))
        perm_buf, recv_c = m[N_PERM, level], m[N_COUPLE, level]
        idx = me % gp
        if level == 1 and by_slots:
            m[N_TAKE_KEY][...] = (dst * LANES + me % gp * wide + rank).astype(F32)
        if level == 2:
            m[N_HIT, 0][...] = hit16
            m[N_HIT, 1][...] = (si == pos + 4).astype(F32).astype(BF16)
        if rows_path(level):
            rank_c = jnp.sum(jnp.where(same & (ci < ri), 1.0, 0.0), axis=1, keepdims=True)
            first = (me % g * wide).astype(F32)
            lane = lax.broadcasted_iota(jnp.int32, (u, LANES), 1).astype(F32)
            place = (lane == rank_c + first).astype(F32).astype(BF16)
            low_f = low.astype(F32)
            if tucked(level):
                named = jnp.where(si == dst * wide + caps[level], low_f, 0.0).astype(BF16)
                moved = moved + once(named, place, 1, 0)
            else:
                qi = lax.broadcasted_iota(jnp.int32, (gp, u), 0)
                named = jnp.where(qi == dst, low_f, 0.0).astype(BF16)
                lows = once(named, place, 1, 0)
                lows_s, lows_r = m[N_LOW_S, level], m[N_LOW, level]
                for q in range(gp):
                    lows_s[q] = lows[q : q + 1, :]
                lows_r[idx] = lows_s[idx]
        else:
            shifted = (si == pos + 4).astype(F32)
            lowc = jnp.sum(shifted * low.astype(F32), axis=1, keepdims=True)
            moved = moved + jnp.broadcast_to(lowc, (slots, LANES))
        perm_buf[...] = moved.reshape(gp, wide, LANES)
        recv_c[idx] = perm_buf[idx]

    def send_couple(level):
        gp = size[level + 1]
        perm_buf, recv_c = m[N_PERM, level], m[N_COUPLE, level]
        if rows_path(level) and not tucked(level):
            lows_s, lows_r = m[N_LOW_S, level], m[N_LOW, level]
            send_each(lambda q: lows_s.at[q], lambda i: lows_r.at[i], gp, (N_LOW, level))
            pending.append((lows_s.at[pl.ds(0, gp - 1)], sem_of((N_LOW, level))))
        part = pl.ds(0, couple_rows(level))
        send_each(lambda q: perm_buf.at[q, part], lambda i: recv_c.at[i, part], gp, (N_COUPLE, level))
        pending.append((perm_buf.at[pl.ds(0, gp - 1), part], sem_of((N_COUPLE, level))))

    def ship_couple(level):
        make_couple(level)
        send_couple(level)

    def low_row(level, child):
        g = size[level]
        got = m[N_COUPLE, level] if tucked(level) else m[N_LOW, level]
        one = slice(caps[level], caps[level] + 1) if tucked(level) else slice(0, 1)
        return jnp.sum(got[child * g : (child + 1) * g, one, :], axis=0)[:, : g * wide_of(level)]

    def low_column(level, child):
        g = size[level]
        got = m[N_COUPLE, level][child * g : (child + 1) * g].reshape(g * wide_of(level), LANES)
        si = lax.broadcasted_iota(jnp.int32, (got.shape[0], 1), 0)
        up = jnp.concatenate([got[4:, :1], got[:4, :1]], axis=0)
        return jnp.where(si % 8 < 4, up, -1.0), jnp.where(si % 8 < 4, -1.0, got[:, :1])

    def build_gt(level):
        g = size[level]
        gp = size[level + 1]
        wide = wide_of(level)
        gt = m[N_GT, level]
        rows = gt.shape[1]
        if rows_path(level) and not tucked(level):
            arrive((N_LOW, level), gp)
        got_all = m[N_COUPLE, level]
        wait_for(
            got_all.at[pl.ds(0, gp - 1), pl.ds(0, couple_rows(level))],
            recv_sem.at[sem_of((N_COUPLE, level))],
        )
        slots = g * wide
        for child in range(gp // g):
            got = got_all[child * g : (child + 1) * g].reshape(slots, LANES)
            if rows_path(level):
                if tucked(level):
                    si = lax.broadcasted_iota(jnp.int32, (slots, LANES), 0)
                    got = jnp.where(si % wide < caps[level], got, 0.0)
                ri = lax.broadcasted_iota(jnp.int32, (rows, slots), 0).astype(F32)
                ot = (ri == low_row(level, child)).astype(F32).astype(BF16)
                full = sum(once(piece, ot, 0, 1) for piece in halves(got))
                if level == 1 and by_slots:
                    m[N_OT][:, child * slots : (child + 1) * slots] = ot.astype(F8)
            else:
                lane = lax.broadcasted_iota(jnp.int32, (slots, rows), 1).astype(F32)
                ot = (lane == low_column(level, child)[0]).astype(F32).astype(BF16)
                full = sum(once(piece, ot, 0, 0) for piece in halves(got))
            gt[child * RANK : (child + 1) * RANK, :] = full
            if level < 2:
                put_halves((N_GTH, level), 0, full, child * RANK)

    def reply_rows():
        g = size[2]
        wide = wide_of(2)
        slots = g * wide
        heads = halves(bas[3][:, :RANK])
        tails = halves(m[N_LAST, 3][...])
        for child in range(size[3] // g):
            if rows_path(2):
                low = low_row(2, child)
                lane = lax.broadcasted_iota(jnp.int32, (1, slots), 1) % wide
                one = jnp.where(lane < 4, low, -1.0)
                two = jnp.where(lane < 4, -1.0, pltpu.roll(low, 4, 1))
                iota, by = lax.broadcasted_iota(jnp.int32, (LANES, slots), 0), 0
            else:
                one, two = low_column(2, child)
                iota, by = lax.broadcasted_iota(jnp.int32, (slots, LANES), 1), 1
            iota = iota.astype(F32)
            first = (iota == one).astype(F32).astype(BF16)
            second = (iota == two).astype(F32).astype(BF16)
            rows = once(first, heads[0], by, 0) + once(first, heads[1], by, 0)
            rows = rows + (once(second, tails[0], by, 0) + once(second, tails[1], by, 0))
            m[N_ROWS_S][child * g : (child + 1) * g] = rows.reshape(g, wide, LANES)
        m[N_ROWS_R][me] = m[N_ROWS_S][me]
        send_each(lambda q: m[N_ROWS_S].at[q], lambda i: m[N_ROWS_R].at[i], size[3], N_ROWS_R)
        pending.append((m[N_ROWS_S].at[pl.ds(0, size[3] - 1)], sem_of(N_ROWS_R)))

    def build_named():
        arrive(N_ROWS_R, size[3])
        got = m[N_ROWS_R][...].reshape(size[3] * wide_of(2), LANES)
        pieces = halves(got)
        out = [
            once(pieces[0], m[N_HIT, i][...], 0, 0) + once(pieces[1], m[N_HIT, i][...], 0, 0)
            for i in range(2)
        ]
        put_halves(N_NAMED, 0, jnp.concatenate(out, axis=0))

    g_p = min(plane, 16)
    g_rp = RANK // g_p

    def g_holds(go):
        if plane == g_p:
            go()
        else:
            pl.when(spot < g_p)(go)

    def g_make():
        both = jnp.concatenate([bas[3][:, :RANK], m[N_LAST, 3][...]], axis=1)
        full = mult(m[N_GT, 2][...], both)
        n = full.shape[0] // RANK
        for j in range(g_p):
            m[N_G_P][j] = jnp.concatenate(
                [full[c * RANK + j * g_rp : c * RANK + (j + 1) * g_rp] for c in range(n)], axis=0
            )

    def g_scatter():
        sem = sem_of(N_G_RS)

        def body(k, carry):
            q = lax.rem(spot + k, g_p)

            def go():
                remote(m[N_G_P].at[q], m[N_G_RS].at[spot], sem, me - spot + q).start()

            if plane == g_p:
                go()
            else:
                pl.when(q != spot)(go)
            return carry

        lax.fori_loop(1 if plane == g_p else 0, g_p, body, 0)
        sent_rows.append((g_p - 1) * rows_in(m[N_G_P]) // g_p)

        def keep():
            m[N_G_RS][spot] = m[N_G_P][spot]

        g_holds(keep)

    def upper_of(q):
        return q * plane // size[2]

    def g_across():
        def go():
            arrive(N_G_RS, plane)
            total = jnp.sum(m[N_G_RS][...], axis=0)
            for c in range(total.shape[0] // g_rp):
                m[N_G_ZS][c] = total[c * g_rp : (c + 1) * g_rp]
            m[N_G_Z][layer] = m[N_G_ZS][upper_of(layer)]
            send_each(lambda q: m[N_G_ZS].at[upper_of(q)], lambda i: m[N_G_Z].at[i], planes, N_G_Z, plane)
            sent_rows.append((planes - 1) * rows_in(m[N_G_Z]) // planes)

        g_holds(go)

    def g_gather():
        def go():
            arrive(N_G_Z, planes)
            m[N_G][spot] = jnp.sum(m[N_G_Z][...], axis=0)
            send_each(lambda q: m[N_G].at[spot], lambda i: m[N_G].at[i], plane, N_G)
            sent_rows.append((plane - 1) * rows_in(m[N_G]) // g_p)

        g_holds(go)

    def g_arrive():
        sem = recv_sem.at[sem_of(N_G)]
        if plane == g_p:
            wait_for(m[N_G].at[pl.ds(0, g_p - 1)], sem)
        else:
            pl.when(spot < g_p)(lambda: wait_for(m[N_G].at[pl.ds(0, g_p - 1)], sem))
            pl.when(spot >= g_p)(lambda: wait_for(m[N_G].at[pl.ds(0, g_p)], sem))
        hi, lo = halves(m[N_G][...].reshape(RANK, 2 * RANK))
        m[N_GH, 0][...] = hi
        m[N_GH, 1][...] = lo

    def g_drain():
        if plane == g_p:
            wait_for(m[N_G_P].at[pl.ds(0, g_p - 1)], send_sem.at[sem_of(N_G_RS)])
        else:
            pl.when(spot < g_p)(lambda: wait_for(m[N_G_P].at[pl.ds(0, g_p - 1)], send_sem.at[sem_of(N_G_RS)]))
            pl.when(spot >= g_p)(lambda: wait_for(m[N_G_P], send_sem.at[sem_of(N_G_RS)]))

        def go():
            wait_for(m[N_G_Z].at[pl.ds(0, planes - 1)], send_sem.at[sem_of(N_G_Z)])
            n = plane - 1
            while n > 0:
                wait_for(m[N_G].at[pl.ds(0, min(n, g_p))], send_sem.at[sem_of(N_G)])
                n -= g_p

        g_holds(go)

    def prepare_back(level):
        z = m[N_Z, level][...]
        heads = bas[level][:, :RANK]
        own = mask(N_OWN, level, 0)
        xz = outer(z, blk[level][...]) + outer(shared(level) * own, heads)
        yt = m[N_LAST, level][...]
        if level > 0:
            sep = m[N_GT, level - 1][:, :LANES]
            xz = jnp.concatenate([xz, outer(xz, sep)], axis=1)
            yt = jnp.concatenate([yt, mult(sep, yt)], axis=0)
        m[N_XZ, level][...] = xz
        put_halves((N_BACK, level), 0, yt)

    def arrive_cross(level):
        g = group_of(level)
        p = parts_of[level]
        n = spread_of(level) // g * p
        sem = recv_sem.at[sem_of((N_CROSS, level))]
        buf = m[N_CROSS, level]
        if g == p:
            wait_for(buf.at[pl.ds(0, n - 1)], sem)
        else:
            idx = me % g
            pl.when(idx < p)(lambda: wait_for(buf.at[pl.ds(0, n - 1)], sem))
            pl.when(idx >= p)(lambda: wait_for(buf.at[pl.ds(0, n)], sem))

    def build_bot_middle():
        gp = size[2]
        place = me % gp
        rows = 2 * LANES
        ri = lax.broadcasted_iota(jnp.int32, (rows, LANES), 0)
        wait_rows(gp + plane + planes - 3, recv_sem.at[sem_of(N_TGT_MIDDLE)])
        mine = jnp.where(ri < LANES, place * LANES + ri, (gp + place - 1) * LANES + ri).astype(F32)

        def fill(j, carry):
            t = m[N_TGT_MIDDLE][j]
            lanes = pl.ds(pl.multiple_of(j * LANES, LANES), LANES)
            m[N_BOT_MIDDLE][:, lanes] = (mine == t).astype(F32).astype(F8)
            return carry

        lax.fori_loop(0, gp, fill, 0)

    def build_bot_upper():
        rows = planes * LANES
        ri = lax.broadcasted_iota(jnp.int32, (rows, LANES), 0)
        mine = ((ri // LANES * plane + spot) * LANES + ri % LANES).astype(F32)

        def fill(j, carry):
            t = m[N_TGT_UPPER][j]
            lanes = pl.ds(pl.multiple_of(j * LANES, LANES), LANES)
            m[N_BOT_UPPER][:, lanes] = (mine == t).astype(F32).astype(F8)
            return carry

        lax.fori_loop(0, plane, fill, 0)

    def build_take():
        key = m[N_TAKE_KEY][...]
        ri = lax.broadcasted_iota(jnp.int32, (LANES, LANES), 0)

        def fill(j, carry):
            rows = pl.ds(pl.multiple_of(j * LANES, LANES), LANES)
            m[N_TAKE][rows, :] = ((ri + j * LANES).astype(F32) == key).astype(F32).astype(F8)
            return carry

        lax.fori_loop(0, size[2], fill, 0)

    def build_ft_middle():
        t = tgt[1][...]
        ri = lax.broadcasted_iota(jnp.int32, (LANES, LANES), 0)

        def fill(j, carry):
            rows = pl.ds(pl.multiple_of(j * LANES, LANES), LANES)
            m[N_FT_MIDDLE][rows, :] = (ri + j * LANES == t).astype(F32).astype(F8)
            return carry

        lax.fori_loop(0, m[N_FT_MIDDLE].shape[0] // LANES, fill, 0)

    def build_ft_upper():
        t = jnp.concatenate([m[N_TGT_LAYER][j] for j in range(planes)], axis=1)
        ri = lax.broadcasted_iota(jnp.int32, (LANES, planes * LANES), 0)

        def fill(j, carry):
            rows = pl.ds(pl.multiple_of(j * LANES, LANES), LANES)
            here = ((ri + (layer * plane + j) * LANES).astype(F32) == t).astype(F32)
            m[N_FT_UPPER][rows, :] = here.astype(F8)
            return carry

        lax.fori_loop(0, plane, fill, 0)

    def share(level, zp):
        m[N_ZP, level][me % size[level]] = zp
        send_all((N_ZP, level), size[level])

    def shared(level):
        arrive((N_ZP, level), size[level])
        return jnp.sum(m[N_ZP, level][...], axis=0)

    def make_cross(level):
        need((N_EXP, level), (N_BAS, level))
        m[N_CROSS_P, level][...] = inner(exp[level][...], bas[level][:, RANK:])

    def start_cross(level):
        make_cross(level)
        scatter_cross(level)

    need((N_SRC, 0), (N_BAS, 0))
    m[N_F0][me % size[0]] = mult(src[0][...], bas[0][:, :RANK])
    make_cross(1)
    pl.semaphore_wait(barrier, plane - 1 + layer * plane)
    send_all(N_F0, size[0])
    scatter_cross(1)
    lax.fori_loop(0, layer, greet_back, 0)
    ship_couple(0)
    need((N_BLK, 0), (N_EXP, 0), (N_PIV, 0))
    local = mult(src[0][...], blk[0][...])
    fill_masks(0)
    build_forward(1)
    make_cross(2)
    pl.when(layer < planes - 1)(lambda: pl.semaphore_wait(up_sem, planes - 1 - layer))
    scatter_cross(2)
    arrive(N_F0, size[0])
    hq = jnp.sum(m[N_F0][...], axis=0) * mask(N_OWN, 0, 0)
    y = local + outer(hq, exp[0][...])
    m[N_F1][spot] = mult(y, bas[0][:, RANK:])
    send_all(N_F1, plane)
    m[N_Z, 0][...] = y * piv[0][...]
    fill_masks(1)
    gather_cross(1)
    need((N_TGT, 1), (N_TGT, 2))
    m[N_TGT_MIDDLE][me % size[2]] = tgt[1][...].astype(F32)
    send_all(N_TGT_MIDDLE, size[2])
    mine_t = tgt[2][...].astype(F32)
    m[N_TGT_UPPER][spot] = mine_t
    send_all(N_TGT_UPPER, plane)
    m[N_TGT_LAYER][layer] = mine_t
    send_all(N_TGT_LAYER, planes, plane)
    ship_couple(1)
    ship_couple(2)
    gather_cross(2)
    build_gt(0)

    for level in range(3):
        g = size[level]
        gp = size[level + 1]
        nch = gp // g
        child_me = me % gp // g
        need((N_SRC, level + 1))
        name = (N_F1, N_F2, N_F3B)[level]
        buf, step = m[name], g
        if level == 2:
            step = g // plane
        if level == 1:
            arrive(N_F2U, gp)
            rows = jnp.concatenate([m[N_F2U][j] for j in range(gp)], axis=1)
            inc = select(rows, m[N_BOT_MIDDLE][...], 1)
        arrive(name, gp if level < 2 else planes)
        ws = [
            jnp.sum(buf[child * step : (child + 1) * step, :count, :], axis=0) * mask(N_KID, level, child, 1)
            for child in range(nch)
        ]
        ws = jnp.concatenate(ws, axis=1)
        bn = src[level + 1][...]
        if level == 0:
            inc = by_halves(ws, (N_GTH, 0), 0)
            m[N_F2U][me % size[2]] = -inc[:, LANES:]
            send_all(N_F2U, size[2])
            local_n, bq, w = local_forward(1, bn - inc[:, :LANES])
            arrive_cross(1)
            sent = [w + mult(bq * mask(N_OWN, 1, 0), m[N_CROSS, 1][...].reshape(RANK, RANK))]
        elif level == 1:
            bn = jnp.concatenate([bn + inc[:, :LANES], ws], axis=1)
            upd = inc[:, LANES:] - by_halves(ws, (N_GTH, 1), 0, slice(LANES, 2 * LANES))
            local_n, bq, w = local_forward(2, bn)
            arrive_cross(2)
            sent = [w + mult(bq * mask(N_OWN, 2, 0), m[N_CROSS, 2][...].reshape(RANK, RANK)), upd]
        else:
            bn = jnp.concatenate([bn + jnp.sum(buf[:, count : 2 * count, :], axis=0), ws], axis=1)
            local_n, bq, *sent = local_forward(3, bn)
            sent = [bq] + sent[:1] + sent[2:] + sent[1:2]
        name = (N_F2, N_F3A, N_F4A)[level]
        group = size[2] if level == 0 else plane
        m[name][me % group] = jnp.concatenate(sent, axis=0)
        send_all(name, group)
        if level < 2:
            m[N_HQ, level + 1][me % gp] = bq
            send_all((N_HQ, level + 1), gp)
        if level == 1:
            g_scatter()
        if level == 2:
            g_across()
        if level > 0:
            arrive((N_HQ, level), g)
            hq = jnp.sum(m[N_HQ, level][...], axis=0) * mask(N_OWN, level, 0)
            z = (local + outer(hq, exp[level][...])) * piv[level][...]
            m[N_Z, level][...] = z
            share(level, mult(z, exp[level][...]))
        local = local_n
        if level == 0:
            add_cross(1)
            build_forward(2)
            fill_masks(2)
            build_forward(3)
            scatter_cross(3)
            build_gt(1)
            build_bot_middle()
            chain_forward(2)
            build_gt(2)
            g_make()
        elif level == 1:
            reply_rows()
            add_cross(2)
            build_bot_upper()
            fill_masks(3)
            arrive(N_F3A, plane)
            sums = jnp.sum(m[N_F3A][:, :count, :], axis=0)
            rows = jnp.concatenate([m[N_F3A][j, count:, :] for j in range(plane)], axis=1)
            part = select(rows, m[N_BOT_UPPER][...], 1)
            for q in range(planes):
                m[N_F3S][q] = jnp.concatenate([sums, part[:, q * LANES : (q + 1) * LANES]], axis=0)
            m[N_F3B][layer] = m[N_F3S][layer]
            send_each(lambda q: m[N_F3S].at[q], lambda i: m[N_F3B].at[i], planes, N_F3B, plane)
            pending.append((m[N_F3S].at[pl.ds(0, planes - 1)], sem_of(N_F3B)))
            put_halves((N_FWD, 3), 4 * RANK, outer(m[N_NEAR][...], m[N_GT, 2][...]))
            chain_forward(3)
            share(0, mult(m[N_Z, 0][...], exp[0][...]))
            start_cross(0)
            m[N_LAST, 0][...] = mult(blk[0][...], bas[0][:, RANK:])
            build_ft_upper()
            if by_slots:
                build_take()
            cross_planes()
    gather_cross(3)
    gather_cross(0)
    g_gather()
    arrive(N_F4A, plane)
    o = (2 + size[3] // size[2]) * count
    sums = jnp.sum(m[N_F4A][:, :o, :], axis=0)
    rows = jnp.concatenate([m[N_F4A][j, o:, :] for j in range(plane)], axis=1)
    part = select(rows, m[N_FT_UPPER][...], 0)
    for q in range(planes):
        c = 2 + q * plane // size[2]
        m[N_F4S][q] = jnp.concatenate(
            [sums[: 2 * count], sums[c * count : (c + 1) * count], part[:, q * LANES : (q + 1) * LANES]], axis=0
        )
    m[N_F4B][layer] = m[N_F4S][layer]
    send_each(lambda q: m[N_F4S].at[q], lambda i: m[N_F4B].at[i], planes, N_F4B, plane)
    pending.append((m[N_F4S].at[pl.ds(0, planes - 1)], sem_of(N_F4B)))
    build_named()
    prepare_back(2)
    arrive_cross(3)
    arrive(N_F4B, planes)
    g_arrive()
    both = jnp.sum(m[N_F4B][...], axis=0)
    hq = both[:count] * mask(N_OWN, 3, 0)
    rp = (both[count : 2 * count] + mult(hq, m[N_CROSS, 3][...].reshape(RANK, RANK))) * mask(N_OWN, 3, 0)
    pair = jnp.concatenate([rp, hq], axis=1)
    s = both[2 * count : 3 * count] + by_halves(pair, N_GH, 1)
    xu = both[3 * count :] + by_halves(pair, N_NAMED, 0)

    for level in (2, 1, 0):
        s = s * mask(N_OWN, level, 1)
        xs = m[N_XZ, level][...] - by_halves(s, (N_BACK, level), 1)
        x = xs[:, :LANES]
        if level == 0:
            outs[0][...] = x
            break
        g = size[level - 1]
        gp = size[level]
        nch = gp // g
        place = me % gp
        child_me = place // g
        sp = xs[:, LANES:] + by_halves(xu, (N_GTH, level - 1), 1, slice(LANES, 2 * LANES))
        name = (N_B3, N_B2)[level - 1]
        buf, piece = m[name], m[N_PIECE, level - 1]
        for c in range(nch):
            rest = []
            if level == 2 and by_slots:
                rest = [select(jnp.concatenate([x, xu], axis=1), m[N_OT][...], 0)]
            elif level == 2:
                rest = [x, xu]
            piece[c] = jnp.concatenate([sp[:, c * RANK : (c + 1) * RANK]] + rest, axis=0)
        buf[place] = piece[child_me]
        send_each(lambda q: piece.at[lax.div(q, g)], lambda i: buf.at[i], gp, name)
        pending.append((buf.at[pl.ds(0, gp - 1)], sem_of(name)))
        outs[level][...] = x
        if level == 2:
            z = (local + outer(hq, exp[3][...])) * piv[3][...]
            outs[3][...] = outer(z, blk[3][...]) + outer(rp, bas[3][:, :RANK])
        else:
            add_cross(0)
        prepare_back(level - 1)
        arrive(name, gp)
        s = jnp.sum(buf[:, :count, :], axis=0)
        if level == 2:
            blocks = [buf[j, count : 2 * count, :] for j in range(gp)]
            if not by_slots:
                blocks += [buf[j, 2 * count :, :] for j in range(gp)]
                build_ft_middle()
            xu = select(jnp.concatenate(blocks, axis=1), m[N_TAKE if by_slots else N_FT_MIDDLE][...], 0)

    if shared_sends:
        assert all(group_of(level) == parts_of[level] for level in range(4))
        wait_rows(sum(sent_rows) + sum(rows_in(part) for part, _ in pending), send_sem.at[0])
    else:
        for part, sem in pending:
            wait_for(part, send_sem.at[sem])
        for level in range(4):
            g = group_of(level)
            p = parts_of[level]
            rp = RANK // p
            gp = spread_of(level)
            n = gp // g * p
            idx = me % g
            rs_sem = send_sem.at[sem_of((N_RS, level))]
            ag_sem = send_sem.at[sem_of((N_CROSS, level))]
            cross_p, buf = m[N_CROSS_P, level], m[N_CROSS, level]

            def ag_done():
                for _ in range((gp - 1) // n):
                    wait_for(buf.at[pl.ds(0, n)], ag_sem)
                if (gp - 1) % n:
                    wait_for(buf.at[pl.ds(0, (gp - 1) % n)], ag_sem)
                if level == 3:
                    wait_for(m[N_GRAM].at[pl.ds(0, planes - 1)], send_sem.at[sem_of(N_GRAM)])

            if g == p:
                wait_for(cross_p.at[pl.ds(0, (p - 1) * rp)], rs_sem)
                ag_done()
            else:
                pl.when(idx < p)(lambda: wait_for(cross_p.at[pl.ds(0, (p - 1) * rp)], rs_sem))
                pl.when(idx >= p)(lambda: wait_for(cross_p, rs_sem))
                pl.when(idx < p)(ag_done)
        g_drain()
    assert len(sems) <= NSEM


def put_out(*refs):
    n = len(refs) // 2
    ins, outs, sem = refs[:n], refs[n : 2 * n], refs[-1]
    copies = [pltpu.make_async_copy(ins[i], outs[i], sem.at[i]) for i in range(n)]
    for c in copies:
        c.start()
    for c in copies:
        c.wait()


def solution(mesh):
    leaves, across = mesh.shape["leaf"], mesh.shape["grid"]

    def shards(*args):
        levels = [args[8 * i : 8 * i + 8] for i in range(3)]
        root = args[24:30]
        (sl, bl, el, qs, pv, cl, rk, tg) = zip(*levels)
        src = list(sl) + [root[0]]
        blk = list(bl) + [root[1]]
        exp = list(el) + [root[2]]
        bas = list(qs) + [root[3]]
        piv = [v.reshape(1, -1) for v in list(pv) + [root[4]]]
        rnk = list(rk) + [root[5]]
        tgt = [t.reshape(1, -1) for t in tg]
        count = src[0].shape[0]
        ups = [t.shape[1] for t in tgt]
        fronts = [r.shape[0] for r in rnk]
        rnk = [r.T if r.shape[0] > 2 else r for r in rnk]
        size = [leaves * across // f for f in fronts]
        for v in src:
            assert v.shape[1] == LANES
        vm = lambda *s: pltpu.VMEM(s, F32)
        bits = lambda *s: pltpu.VMEM(s, BF16)
        ones = lambda *s: pltpu.VMEM(s, F8)
        total = leaves * across
        plane = size[1]
        planes = total // plane
        nch = [size[i + 1] // size[i] for i in range(3)]
        caps = [max(1, -(-ups[i] // size[i + 1])) for i in range(3)]
        group = size[:3] + [plane]
        spread = group
        parts = [min(g, 16) for g in group]
        by_slots = size[2] * max(8, -(-caps[1] // 8) * 8) <= LANES
        bufs = {
            N_F0: vm(size[0], count, LANES),
            N_F1: vm(plane, count, LANES),
            N_F2: vm(size[2], count, LANES),
            N_F2U: vm(size[2], count, LANES),
            N_F3A: vm(plane, 2 * count, LANES),
            N_F3S: vm(planes, 2 * count, LANES),
            N_F3B: vm(planes, 2 * count, LANES),
            (N_HQ, 1): vm(size[1], count, LANES),
            (N_HQ, 2): vm(size[2], count, LANES),
            N_F4A: vm(plane, (nch[2] + 3) * count, LANES),
            N_F4S: vm(planes, 4 * count, LANES),
            N_F4B: vm(planes, 4 * count, LANES),
            N_NEAR: vm(LANES, LANES),
            N_RULER: vm(8192 if total <= 64 else 1280, LANES),
            (N_HIT, 0): bits(total * 8, LANES),
            (N_HIT, 1): bits(total * 8, LANES),
            N_ROWS_S: vm(total, 8, LANES),
            N_ROWS_R: vm(total, 8, LANES),
            (N_NAMED, 0): bits(2 * RANK, LANES),
            (N_NAMED, 1): bits(2 * RANK, LANES),
            (N_GH, 0): bits(RANK, 2 * RANK),
            (N_GH, 1): bits(RANK, 2 * RANK),
            N_G_P: vm(parts[3], nch[2] * RANK // parts[3], 2 * RANK),
            N_G_RS: vm(plane, nch[2] * RANK // parts[3], 2 * RANK),
            N_G_ZS: vm(nch[2], RANK // parts[3], 2 * RANK),
            N_G_Z: vm(planes, RANK // parts[3], 2 * RANK),
            N_G: vm(parts[3], RANK // parts[3], 2 * RANK),
            N_B2: vm(size[2], (2 if by_slots else 3) * count, LANES),
            N_B3: vm(size[1], count, LANES),
            N_TGT_MIDDLE: vm(size[2], 1, LANES),
            N_TGT_UPPER: vm(plane, 1, LANES),
            N_TGT_LAYER: vm(planes, 1, LANES),
            N_BOT_MIDDLE: ones(2 * LANES, size[2] * LANES),
            N_BOT_UPPER: ones(planes * LANES, plane * LANES),
            N_FT_UPPER: ones(plane * LANES, planes * LANES),
            N_MASK: vm(6 + 2 * sum(nch), count, LANES),
            N_GRAM: vm(planes, RANK // parts[3], RANK),
        }
        arrays = {N_SRC: src, N_BLK: blk, N_EXP: exp, N_BAS: bas, N_PIV: piv, N_RNK: rnk, N_CPL: cl, N_TGT: tgt}
        for name, list_of in arrays.items():
            for i, v in enumerate(list_of):
                bufs[name, i] = pltpu.VMEM(v.shape, v.dtype)
        for i in range(4):
            bufs[N_LAST, i] = vm(LANES, RANK)
            for j in range(2):
                if i > 0:
                    bufs[(N_FWD, i), j] = bits(LANES + (nch[i - 1] * RANK if i > 1 else 0), (3 if i < 3 else 4 + nch[2]) * RANK)
                if i < 3:
                    bufs[(N_BACK, i), j] = bits((1 + (nch[i - 1] if i > 0 else 0)) * RANK, RANK)
        if by_slots:
            bufs[N_TAKE_KEY] = vm(1, LANES)
            bufs[N_TAKE] = ones(size[2] * LANES, LANES)
            bufs[N_OT] = ones(2 * LANES, LANES)
        else:
            bufs[N_FT_MIDDLE] = ones(size[2] * 2 * LANES, LANES)
        for i in range(2):
            for j in range(2):
                bufs[(N_GTH, i), j] = bits(nch[i] * RANK, 2 * LANES)
        for i in range(3):
            bufs[N_Z, i] = vm(count, LANES)
            bufs[N_XZ, i] = vm(count, (1 + (nch[i - 1] if i > 0 else 0)) * LANES)
        for i in range(4):
            bufs[N_CROSS_P, i] = vm(RANK, RANK)
            bufs[N_RS, i] = vm(group[i], RANK // parts[i], RANK)
            bufs[N_CROSS, i] = vm(spread[i] // group[i] * parts[i], RANK // parts[i], RANK)
        for i in range(3):
            wide = max(8, -(-caps[i] // 8) * 8)
            assert caps[i] <= 4 or size[i] * wide <= LANES
            if caps[i] == wide:
                bufs[N_LOW_S, i] = vm(size[i + 1], 1, LANES)
                bufs[N_LOW, i] = vm(size[i + 1], 1, LANES)
            bufs[N_PERM, i] = vm(size[i + 1], wide, LANES)
            bufs[N_COUPLE, i] = vm(size[i + 1], wide, LANES)
            bufs[N_GT, i] = vm(nch[i] * RANK, LANES * (1 if i == 2 else 2))
            bufs[N_ZP, i] = vm(size[i], count, LANES)
            bufs[N_PIECE, i] = vm(nch[i], (1 if i == 0 else 2 if by_slots else 3) * count, LANES)
        scratch = list(bufs.values())
        scratch += [pltpu.SemaphoreType.DMA((n,)) for n in (1 if total <= 64 else NSEM, NSEM, 9)]
        scratch += [pltpu.SemaphoreType.REGULAR]
        vspec = pl.BlockSpec(memory_space=pltpu.VMEM)
        aspec = pl.BlockSpec(memory_space=pl.ANY)
        answers = pl.pallas_call(
            functools.partial(kernel, (leaves, across, size, ups, count, caps, fronts), list(bufs)),
            out_shape=[pltpu.VMEM(v.shape, F32) for v in src],
            in_specs=[aspec] * 30,
            out_specs=[vspec] * 4,
            scratch_shapes=scratch,
            compiler_params=pltpu.CompilerParams(
                collective_id=0, has_side_effects=True, vmem_limit_bytes=63 * 1024 * 1024
            ),
        )(*src, *blk, *exp, *bas, *piv, *rnk, *cl, *tgt)
        return pl.pallas_call(
            put_out,
            out_shape=[jax.ShapeDtypeStruct(v.shape, F32) for v in src],
            in_specs=[vspec] * 4,
            out_specs=[aspec] * 4,
            scratch_shapes=[pltpu.SemaphoreType.DMA((4,))],
        )(*[pltpu.with_memory_space_constraint(v, pltpu.VMEM) for v in answers])

    spread_axes = ("leaf", "grid")
    level = (P(None, spread_axes), P(spread_axes, None), P(spread_axes, None), P(spread_axes, None), P(spread_axes))
    mid = level + (P(spread_axes, None), P(), P(spread_axes))
    return jax.shard_map(
        shards,
        mesh=mesh,
        in_specs=mid * 3 + level + (P(),),
        out_specs=(P(None, spread_axes),) * 4,
        check_vma=False,
    )
```
